32 devices in a mesh: scan: 16 (over z, x, core), tile: 2 (over y).
Axes of the slice: x: 2, y: 2, z: 4, core: 2. Of those that a mesh axis runs over, the one named last changes fastest.
Arguments:
- probe_modes: float32 [12, 2, 128, 128], replicated, may hold values from -5 to 5
- patterns: float32 [128, 128, 128], P(('scan', 'tile')), may hold values from 0.005 to 300
- specimen: float32 [2, 2048, 512], P(None, 'scan', 'tile'), may hold values from -17.5 to 17.5
- offsets: int32 [128, 2], P(('scan', 'tile')), may hold values from -128 to 2048, as said below
Outputs:
- new_probe: float32 [12, 2, 128, 128], replicated
- new_specimen: float32 [2, 2048, 512], P(None, 'scan', 'tile')
The draws below stay inside these ranges and needn't reach their ends.
Inputs may be any that keep to these rules, and one draw needn't show every extreme that they name: `offsets`: position p lies in aligned block b = p // 4, held by the device of scan index s = b // (the number of tile devices) and tile index t = b % (the number of tile devices); its row offset lies in s * 128 - 128 to s * 128 + 128, its column offset in t * 256 - 128 to t * 256 + 256, both ends included; in every block one position has its row offset at the lower end and its column offset at the upper end, and one has its row offset at the upper end.
All inputs are finite; a program needn't handle non-finite values.
Results may differ from the reference program's by a relative error of at most 0.0001.
Values sent between devices are 32-bit elements; how exact they have to be, the bound alone decides.
A program may use at most 64 MiB of HBM per device.

```python
import math
import jax
import jax.numpy as jnp
from jax import lax

DET = 128
MODES = 12
P_DEV = 4
ROWS_DEV = 128
COLS_DEV = 256
NS_STEPS = 8
POSITIONS = 128
OBJ_ROWS = 2048
OBJ_COLS = 512


def draw_probe_modes(key, part):
    key_base, key_weight = jax.random.split(key, 2)
    shape_all = (MODES, 2, DET, DET)
    base_field = jnp.clip(jax.random.normal(key_base, shape_all, jnp.float32), -5.0, 5.0)
    weights = jnp.exp(jax.random.uniform(key_weight, (MODES,), jnp.float32, math.log(0.1), math.log(0.4)))
    mixing = 0.6
    weights = weights.at[0].set(1.0)
    mixed = base_field + mixing * base_field[0:1]
    mixed = mixed.at[0].set(base_field[0])
    return (mixed * weights[:, None, None, None]).astype(jnp.float32)


def draw_patterns(key, part):
    key_flux, key_pixel, key_speckle = jax.random.split(key, 3)
    block_count = POSITIONS // P_DEV
    along = (jnp.arange(POSITIONS, dtype=jnp.int32) // P_DEV).astype(jnp.float32) / max(block_count - 1, 1)
    flux_low, flux_high, growth, speck_low, speck_high = (1.0, 6.0, 3.0, 0.2, 1.8)
    flux = jnp.exp(jax.random.uniform(key_flux, (POSITIONS,), jnp.float32, math.log(flux_low), math.log(flux_high))) * growth ** along
    pixel_gain = jnp.exp(jax.random.uniform(key_pixel, (DET, DET), jnp.float32, math.log(0.3), math.log(3.0)))
    speckle = jax.random.uniform(key_speckle, (POSITIONS, DET, DET), jnp.float32, speck_low, speck_high)
    return (flux[:, None, None] * pixel_gain[None] * speckle).astype(jnp.float32)


def draw_specimen(key, part):
    key_values, key_rows, key_cols = jax.random.split(key, 3)
    values = 0.4 * jnp.clip(jax.random.normal(key_values, (2, OBJ_ROWS, OBJ_COLS), jnp.float32), -4.0, 4.0)
    mean_part = 1.0
    row_scale = jnp.exp(jax.random.uniform(key_rows, (OBJ_ROWS,), jnp.float32, math.log(0.5), math.log(2.0)))
    col_scale = jnp.exp(jax.random.uniform(key_cols, (OBJ_COLS,), jnp.float32, math.log(0.5), math.log(2.0)))
    rough = values * row_scale[None, :, None] * col_scale[None, None, :]
    shift = jnp.array([mean_part, 0.0], jnp.float32)[:, None, None]
    return (rough + shift).astype(jnp.float32)


def draw_offsets(key, part):
    key_rows, key_cols = jax.random.split(key, 2)
    tile_count = OBJ_COLS // COLS_DEV
    position = jnp.arange(POSITIONS, dtype=jnp.int32)
    group_index = position // P_DEV
    within = position % P_DEV
    scan_index = group_index // tile_count
    tile_index = group_index % tile_count
    local_row = jax.random.randint(key_rows, (POSITIONS,), 0, ROWS_DEV + DET + 1, dtype=jnp.int32)
    local_col = jax.random.randint(key_cols, (POSITIONS,), 0, COLS_DEV + DET + 1, dtype=jnp.int32)
    local_row = jnp.where(within == 0, 0, jnp.where(within == 1, ROWS_DEV + DET, local_row))
    local_col = jnp.where(within == 0, COLS_DEV + DET, local_col)
    row_offsets = scan_index * ROWS_DEV - DET + local_row
    col_offsets = tile_index * COLS_DEV - DET + local_col
    return jnp.stack([row_offsets, col_offsets], axis=1).astype(jnp.int32)


def setup_inputs(seed: int = 0) -> dict:
    splits = jax.random.split(jax.random.key(seed), 5)
    return {
        "probe_modes": draw_probe_modes(jax.random.fold_in(splits[4], 71), 0),
        "patterns": draw_patterns(jax.random.fold_in(splits[4], 71), 0),
        "specimen": draw_specimen(jax.random.fold_in(splits[4], 71), 0),
        "offsets": draw_offsets(jax.random.fold_in(splits[4], 71), 0),
    }


highest = lax.Precision.HIGHEST
light_floor = 0.05
object_reg = 0.5
probe_reg = 1.0
total_eps = 1e-06

def newton_steps(gram_re, gram_im):
    mode_count = gram_re.shape[0]
    upper = jnp.concatenate([gram_re, -gram_im], axis=1)
    lower = jnp.concatenate([gram_im, gram_re], axis=1)
    embedded = jnp.concatenate([upper, lower], axis=0)
    frobenius = jnp.sqrt(jnp.sum(embedded * embedded))
    identity = jnp.eye(2 * mode_count, dtype=jnp.float32)
    current = embedded / frobenius
    inverse = identity
    for repeat in range(NS_STEPS):
        factor = 1.5 * identity - 0.5 * jnp.dot(inverse, current, precision=highest, preferred_element_type=jnp.float32)
        current = jnp.dot(current, factor, precision=highest, preferred_element_type=jnp.float32)
        inverse = jnp.dot(factor, inverse, precision=highest, preferred_element_type=jnp.float32)
    inverse = inverse / jnp.sqrt(frobenius)
    return (inverse[:mode_count, :mode_count], inverse[mode_count:, :mode_count])

def gram_parts(mode_rows):
    real_rows = mode_rows[0::2]
    imag_rows = mode_rows[1::2]
    gram_re = jnp.dot(real_rows, real_rows.T, precision=highest, preferred_element_type=jnp.float32) + jnp.dot(imag_rows, imag_rows.T, precision=highest, preferred_element_type=jnp.float32)
    gram_im = jnp.dot(real_rows, imag_rows.T, precision=highest, preferred_element_type=jnp.float32) - jnp.dot(imag_rows, real_rows.T, precision=highest, preferred_element_type=jnp.float32)
    return (gram_re, gram_im)

def orthonormal_rows(mode_rows, gram_re, gram_im, power_ratio):
    real_rows = mode_rows[0::2]
    imag_rows = mode_rows[1::2]
    mix_re, mix_im = newton_steps(gram_re, gram_im)
    ortho_re = jnp.dot(mix_re.T, real_rows, precision=highest, preferred_element_type=jnp.float32) - jnp.dot(mix_im.T, imag_rows, precision=highest, preferred_element_type=jnp.float32)
    ortho_im = jnp.dot(mix_im.T, real_rows, precision=highest, preferred_element_type=jnp.float32) + jnp.dot(mix_re.T, imag_rows, precision=highest, preferred_element_type=jnp.float32)
    weight = jnp.sqrt(power_ratio * jnp.diagonal(gram_re))
    joined = jnp.stack([ortho_re, ortho_im], axis=1) * weight[:, None, None]
    return joined.reshape(mode_rows.shape)

def reference(probe_modes, patterns, specimen, offsets):
    detector = probe_modes.shape[-1]
    mode_count = probe_modes.shape[0]
    probe_field = lax.complex(probe_modes[:, 0], probe_modes[:, 1])
    probe_power = lax.optimization_barrier(jnp.sum(probe_modes[:, 0] ** 2 + probe_modes[:, 1] ** 2, axis=0))
    padded = jnp.pad(lax.complex(specimen[0], specimen[1]), ((detector, detector), (detector, detector)))
    frame_zeros = jnp.zeros(padded.shape, jnp.float32)
    mode_zeros = jnp.zeros((mode_count, detector, detector), jnp.float32)

    def one_position(position, running):
        grad_sum, light_sum, frame_num, frame_light, model_sum = running
        row_at = (offsets[position, 0] + detector).astype(jnp.int32)
        col_at = (offsets[position, 1] + detector).astype(jnp.int32)
        patch_now = lax.dynamic_slice(padded, (row_at, col_at), (detector, detector))
        exit_wave = probe_field * patch_now[None]
        model_sum = model_sum + jnp.sum(jnp.real(exit_wave) ** 2 + jnp.imag(exit_wave) ** 2)
        far_field = jnp.fft.fft2(exit_wave, norm='ortho')
        model_light = lax.optimization_barrier(jnp.sum(jnp.real(far_field) ** 2 + jnp.imag(far_field) ** 2, axis=0))
        factor = jnp.sqrt(patterns[position]) / jnp.sqrt(jnp.maximum(model_light, light_floor)) - 1.0
        change = jnp.fft.ifft2(far_field * factor[None], norm='ortho')
        grad_sum = grad_sum + jnp.conj(patch_now)[None] * change
        light_sum = light_sum + jnp.real(patch_now) ** 2 + jnp.imag(patch_now) ** 2
        contribution = lax.optimization_barrier(jnp.sum(jnp.conj(probe_field) * change, axis=0))
        old_num = lax.dynamic_slice(frame_num, (row_at, col_at), (detector, detector))
        frame_num = lax.dynamic_update_slice(frame_num, old_num + contribution, (row_at, col_at))
        old_light = lax.dynamic_slice(frame_light, (row_at, col_at), (detector, detector))
        frame_light = lax.dynamic_update_slice(frame_light, old_light + probe_power, (row_at, col_at))
        return (grad_sum, light_sum, frame_num, frame_light, model_sum)
    initial = (lax.complex(mode_zeros, mode_zeros), jnp.zeros((detector, detector), jnp.float32), lax.complex(frame_zeros, frame_zeros), frame_zeros, jnp.zeros((), jnp.float32))
    grad_sum, light_sum, frame_num, frame_light, model_sum = lax.fori_loop(0, POSITIONS, one_position, initial)
    interior_num = frame_num[detector:-detector, detector:-detector]
    interior_light = frame_light[detector:-detector, detector:-detector]
    new_field = padded[detector:-detector, detector:-detector] + interior_num / (interior_light + object_reg)
    new_specimen = jnp.stack([jnp.real(new_field), jnp.imag(new_field)])
    updated = probe_field + grad_sum / (light_sum + probe_reg)[None]
    updated_rows = jnp.stack([jnp.real(updated), jnp.imag(updated)], axis=1).reshape(2 * mode_count, -1)
    power_ratio = jnp.sum(patterns) / (model_sum + total_eps)
    gram_re, gram_im = gram_parts(updated_rows)
    new_rows = orthonormal_rows(updated_rows, gram_re, gram_im, power_ratio)
    return (new_rows.reshape(probe_modes.shape), new_specimen)
```

```python
import math

import jax
import jax.numpy as jnp
import numpy as np
from jax import lax
from jax.experimental import pallas as pl
from jax.experimental.pallas import tpu as pltpu
from jax.sharding import PartitionSpec as P

NS_STEPS = 8


highest = lax.Precision.HIGHEST
light_floor = 0.05
object_reg = 0.5
probe_reg = 1.0
total_eps = 1e-06


def dft_tables(detector):
    indices = np.arange(detector, dtype=np.int64)
    angles = -2.0 * np.pi / detector * (indices[:, None] * indices[None, :] % detector)
    table_re = np.cos(angles) / np.sqrt(detector)
    table_im = np.sin(angles) / np.sqrt(detector)
    right = np.block([[table_re, table_im], [-table_im, table_re]]).astype(np.float32)
    left = np.ascontiguousarray(right.T)
    parts = []
    for table in (right, left):
        high = table.astype(jnp.bfloat16)
        low = (table - high.astype(np.float32)).astype(jnp.bfloat16)
        parts.append((high, low))
    (rh, rl), (lh, ll) = parts
    return (
        np.concatenate([rh, rl, rh], axis=0),
        np.concatenate([lh, ll, lh], axis=1),
        np.concatenate([rh, rl, rh], axis=1),
        np.concatenate([lh, ll, lh], axis=0),
    )


def halves(value):
    high = value.astype(jnp.bfloat16)
    low = (value - high.astype(jnp.float32)).astype(jnp.bfloat16)
    return high, low


def scan_kernel(
    offs, probe, patterns, extended, right_f, left_f, left_b, right_b,
    packed_a, packed_b, packed_c, totals, frame_out,
    ext, frame, deep, half, far, power, grad, light,
    *, block_rows, block_cols,
):
    packed = (packed_a, packed_b, packed_c)
    modes = probe.shape[0]
    det = probe.shape[-1]
    count = patterns.shape[0]
    col_blocks = extended.shape[2] // det
    f32 = jnp.float32
    row_base = lax.axis_index("scan") * block_rows - det
    col_base = lax.axis_index("tile") * block_cols - det
    lanes = lax.broadcasted_iota(jnp.int32, (det, det), 1)
    for c in range(2):
        for j in range(col_blocks):
            ext[c, j] = extended[c, :, j * det : (j + 1) * det]
        ext[c, col_blocks] = jnp.zeros_like(ext[c, col_blocks])
    frame[...] = jnp.zeros_like(frame)
    grad[...] = jnp.zeros_like(grad)
    light[...] = jnp.zeros_like(light)
    acc = jnp.zeros((det, det), f32)
    for k in range(modes):
        acc = acc + probe[k, 0] * probe[k, 0] + probe[k, 1] * probe[k, 1]
    power[...] = acc

    def one(p, total):
        row = offs[p, 0] - row_base
        col = offs[p, 1] - col_base
        block = col // det
        shift = col - block * det
        back = lax.rem(det - shift, det)
        rows = pl.ds(row, det)

        def patch_part(c):
            first = pltpu.roll(ext[c, block, rows, :], back, 1)
            second = pltpu.roll(ext[c, block + 1, rows, :], back, 1)
            return jnp.where(lanes < det - shift, first, second)

        patch_re = patch_part(0)
        patch_im = patch_part(1)
        patch_light = patch_re * patch_re + patch_im * patch_im
        light[...] = light[...] + patch_light
        total = total + patch_light * power[...]
        for k in range(modes):
            at = pl.ds(k * det, det)
            pr, pi = probe[k, 0], probe[k, 1]
            for c, value in enumerate((pr * patch_re - pi * patch_im, pr * patch_im + pi * patch_re)):
                high, low = halves(value)
                deep[at, pl.ds(c * det, det)] = high
                deep[at, pl.ds((2 + c) * det, det)] = high
                deep[at, pl.ds((4 + c) * det, det)] = low
        half[...] = jnp.dot(deep[...], right_f[...], preferred_element_type=f32)
        model = jnp.zeros((det, det), f32)
        for k in range(0, modes, 2):
            lo_at, hi_at = pl.ds(k * det, det), pl.ds((k + 1) * det, det)
            first, second = half[lo_at, :], half[hi_at, :]
            paired = jnp.concatenate(
                [
                    jnp.concatenate([first[:, :det], second[:, :det]], axis=1),
                    jnp.concatenate([first[:, det:], second[:, det:]], axis=1),
                ],
                axis=0,
            )
            high, low = halves(paired)
            stacked = jnp.concatenate([high, high, low], axis=0)
            out = jnp.dot(left_f[...], stacked, preferred_element_type=f32)
            far[:, pl.ds(k * det, 2 * det)] = out
            squares = out * out
            both = squares[:det] + squares[det:]
            model = model + both[:, :det] + both[:, det:]
        factor = jnp.sqrt(patterns[p]) / jnp.sqrt(jnp.maximum(model, light_floor)) - 1.0
        wide = jnp.concatenate([factor, factor], axis=1)
        wide = jnp.concatenate([wide, wide], axis=0)
        for k in range(0, modes, 2):
            high, low = halves(far[:, pl.ds(k * det, 2 * det)] * wide)
            stacked = jnp.concatenate([high, high, low], axis=0)
            out = jnp.dot(left_b[...], stacked, preferred_element_type=f32)
            high, low = halves(out)
            for m in range(2):
                at = pl.ds((k + m) * det, det)
                for c in range(2):
                    part_h = high[c * det : (c + 1) * det, m * det : (m + 1) * det]
                    part_l = low[c * det : (c + 1) * det, m * det : (m + 1) * det]
                    deep[at, pl.ds(c * det, det)] = part_h
                    deep[at, pl.ds((2 + c) * det, det)] = part_h
                    deep[at, pl.ds((4 + c) * det, det)] = part_l
        half[...] = jnp.dot(deep[...], right_b[...], preferred_element_type=f32)
        num_re = jnp.zeros((det, det), f32)
        num_im = jnp.zeros((det, det), f32)
        for k in range(modes):
            at = pl.ds(k * det, det)
            cr, ci = half[at, :det], half[at, det:]
            pr, pi = probe[k, 0], probe[k, 1]
            grad[0, k] = grad[0, k] + patch_re * cr + patch_im * ci
            grad[1, k] = grad[1, k] + patch_re * ci - patch_im * cr
            num_re = num_re + pr * cr + pi * ci
            num_im = num_im + pr * ci - pi * cr
        zero = jnp.zeros((det, det), f32)
        for c, value in enumerate((num_re, num_im, power[...])):
            turned = pltpu.roll(value, shift, 1)
            frame[c, block, rows, :] = frame[c, block, rows, :] + jnp.where(lanes >= shift, turned, zero)
            frame[c, block + 1, rows, :] = frame[c, block + 1, rows, :] + jnp.where(lanes < shift, turned, zero)
        return total

    model_grid = lax.fori_loop(0, count, one, jnp.zeros((det, det), f32))
    measured = jnp.zeros((det, det), f32)
    for p in range(count):
        measured = measured + patterns[p]
    pack_gradient(packed, grad, light)
    totals[0] = jnp.sum(measured.reshape(det // 8, 8, det), axis=0)
    totals[1] = jnp.sum(model_grid.reshape(det // 8, 8, det), axis=0)
    for c in range(3):
        for j in range(col_blocks):
            frame_out[c, :, j * det : (j + 1) * det] = frame[c, j]


def scan_positions(offsets, probe_modes, patterns, extended, block_rows, block_cols):
    modes, _, det, _ = probe_modes.shape
    f32 = jnp.float32
    ext_rows, ext_cols = extended.shape[1:]
    col_blocks = ext_cols // det
    vmem = pl.BlockSpec(memory_space=pltpu.VMEM)
    tables = [jnp.asarray(t) for t in dft_tables(det)]

    def kernel(*refs):
        scan_kernel(*refs, block_rows=block_rows, block_cols=block_cols)

    return pl.pallas_call(
        kernel,
        name="scan_positions",
        out_shape=(
            *[jax.ShapeDtypeStruct((2,) + shape, f32) for shape in group_shapes(modes, det)],
            jax.ShapeDtypeStruct((2, 8, det), f32),
            jax.ShapeDtypeStruct((3, ext_rows, ext_cols), f32),
        ),
        in_specs=[pl.BlockSpec(memory_space=pltpu.SMEM)] + [vmem] * 7,
        out_specs=(vmem,) * 5,
        scratch_shapes=[
            pltpu.VMEM((2, col_blocks + 1, ext_rows, det), f32),
            pltpu.VMEM((3, col_blocks + 1, ext_rows, det), f32),
            pltpu.VMEM((modes * det, 6 * det), jnp.bfloat16),
            pltpu.VMEM((modes * det, 2 * det), f32),
            pltpu.VMEM((2 * det, modes * det), f32),
            pltpu.VMEM((det, det), f32),
            pltpu.VMEM((2, modes, det, det), f32),
            pltpu.VMEM((det, det), f32),
        ],
        compiler_params=pltpu.CompilerParams(vmem_limit_bytes=48 * 1024 * 1024),
    )(offsets, probe_modes, patterns, extended, *tables)


core_dim = ("scan", 1, 2)
slab_dims = (("scan", 2, 2), ("tile", 1, 2), ("scan", 4, 4))
slab_orders = ((0, 1, 2), (1, 2, 0), (2, 0, 1))
slab_count = math.prod(size for _, _, size in slab_dims)


def extra_bits():
    bits = []
    for axis, bit in (("scan", 16), ("tile", 2)):
        while bit < lax.axis_size(axis):
            bits.append((axis, bit, 2))
            bit *= 2
    return bits


def group_modes(modes):
    return modes // (2 * len(slab_orders))


def group_shapes(modes, det):
    shapes = []
    for q, order in enumerate(slab_orders):
        planes = 2 * group_modes(modes) + (q == len(slab_orders) - 1)
        shapes.append(tuple(slab_dims[i][2] for i in order) + (planes, det // slab_count, det))
    return shapes


def slab_coords(tile):
    coords = []
    for _, _, size in reversed(slab_dims):
        coords.append(tile % size)
        tile = tile // size
    return coords[::-1]


def plane_of(half, q, i, modes):
    per = group_modes(modes)
    return half * (modes // 2) + q * per + i // 2, i % 2


def pack_gradient(packed, grad, light):
    modes, det = grad.shape[1], grad.shape[-1]
    rows = det // slab_count
    for tile in range(slab_count):
        at = slice(tile * rows, (tile + 1) * rows)
        coords = slab_coords(tile)
        for q, order in enumerate(slab_orders):
            spot = tuple(coords[i] for i in order)
            for half in range(2):
                for i in range(2 * group_modes(modes)):
                    k, c = plane_of(half, q, i, modes)
                    packed[q][(half,) + spot + (i,)] = grad[c, k, at, :]
                if q == len(slab_orders) - 1:
                    packed[q][(half,) + spot + (2 * group_modes(modes),)] = light[at, :]


def directions():
    return [(i, j) for i, j in ((1, 0), (-1, 0), (0, 1), (0, -1), (1, 1), (1, -1), (-1, 1), (-1, -1))]


def digit(dim):
    axis, bit, size = dim
    return (lax.axis_index(axis) // bit) % size


def flipped(value, size, d):
    if size == 2:
        return 1 - value if d else value
    low, high = value % 2, value // 2
    low = 1 - low if d % 2 else low
    high = 1 - high if d // 2 else high
    return low + 2 * high


def peer(moves):
    where = {}
    for dim, d in moves:
        axis, bit, size = dim
        here = digit(dim)
        base = where.get(axis, lax.axis_index(axis))
        where[axis] = base + bit * (flipped(here, size, d) - here)
    return where


def full_dot(a, b):
    return jnp.dot(a, b, precision=highest, preferred_element_type=jnp.float32)


def finish_kernel(extra, *refs):
    groups = len(slab_orders)
    packed, refs = refs[:groups], refs[groups:]
    totals, frame, probe, specimen, new_probe, new_specimen, *refs = refs
    land0, refs = refs[:groups], refs[groups:]
    acc, refs = refs[:groups], refs[groups:]
    land = []
    for step in range(3):
        land.append(refs[:groups])
        refs = refs[groups:]
    landx, refs = refs[:groups], refs[groups:]
    full, refs = refs[:groups], refs[groups:]
    slots, refs = refs[:8], refs[8:]
    total_land, gram_out, gram_land, gram_x, interior, send_sem, recv_sem, fold_send, fold_recv = refs
    f32 = jnp.float32
    modes, det = probe.shape[0], probe.shape[-1]
    per = 2 * group_modes(modes)
    rows = det // slab_count
    planes = 2 * modes
    used = [0]

    def remote(src, dst, moves):
        n = used[0]
        used[0] += 1
        return pltpu.make_async_remote_copy(
            src_ref=src, dst_ref=dst, send_sem=send_sem.at[n], recv_sem=recv_sem.at[n],
            device_id=peer(moves), device_id_type=pl.DeviceIdType.MESH,
        )

    def launch(copies):
        for item in copies:
            item.start()
        return copies

    def settle(copies):
        for item in copies:
            item.wait()

    core = digit(core_dim)
    coords = [digit(dim) for dim in slab_dims]
    mine = [tuple(coords[i] for i in order) for order in slab_orders]
    dims = [tuple(slab_dims[i] for i in order) for order in slab_orders]

    here = {axis: lax.axis_index(axis) for axis in ("scan", "tile")}
    sizes = {axis: lax.axis_size(axis) for axis in ("scan", "tile")}
    block_rows, block_cols = interior.shape[1:]

    def span(shift, block):
        low = {-1: 0, 0: det, 1: det + block}[shift]
        return pl.ds(low, block if shift == 0 else det)

    def inner(shift, block):
        low = {-1: block - det, 0: 0, 1: 0}[shift]
        return pl.ds(low, block if shift == 0 else det)

    def valid(shift_rows, shift_cols):
        row, col = here["scan"] + shift_rows, here["tile"] + shift_cols
        return (row >= 0) & (row < sizes["scan"]) & (col >= 0) & (col < sizes["tile"])

    def fold(index):
        shift_rows, shift_cols = directions()[index]
        return pltpu.make_async_remote_copy(
            src_ref=frame.at[:, span(shift_rows, block_rows), span(shift_cols, block_cols)],
            dst_ref=slots[index],
            send_sem=fold_send.at[index],
            recv_sem=fold_recv.at[index],
            device_id={
                "scan": (here["scan"] + shift_rows + sizes["scan"]) % sizes["scan"],
                "tile": (here["tile"] + shift_cols + sizes["tile"]) % sizes["tile"],
            },
            device_id_type=pl.DeviceIdType.MESH,
        )

    def fold_start(indices):
        for index in indices:
            @pl.when(valid(*directions()[index]))
            def _():
                fold(index).start()

    swap = [launch([remote(packed[q].at[1 - core], land0[q], [(core_dim, 1)])]) for q in range(groups)]
    swap.append(launch([remote(totals, total_land, [(core_dim, 1)])]))
    interior[...] = frame[:, det : det + block_rows, det : det + block_cols]

    def reduce_start(q, step):
        dim = dims[q][step]
        copies = []
        for d in range(1, dim[2]):
            spot = mine[q][:step] + (flipped(mine[q][step], dim[2], d),)
            copies.append(remote(acc[q].at[spot], land[step][q].at[d - 1], [(dim, d)]))
        return launch(copies)

    def reduce_end(q, step, copies):
        settle(copies)
        spot = mine[q][: step + 1]
        value = acc[q][spot]
        for d in range(1, dims[q][step][2]):
            value = value + land[step][q][d - 1]
        acc[q][spot] = value

    flying = []
    for q in range(groups):
        settle(swap[q])
        acc[q][...] = packed[q][core] + land0[q][...]
        flying.append(reduce_start(q, 0))
    fold_start((0, 1))
    for step in range(3):
        for q in range(groups):
            reduce_end(q, step, flying[q])
            if step < 2:
                flying[q] = reduce_start(q, step + 1)
        if step == 0:
            fold_start((2, 3))
        if step == 1:
            fold_start((4, 5, 6, 7))
    for e, dim in enumerate(extra):
        for q in range(groups):
            flying[q] = launch([remote(acc[q].at[mine[q]], landx[q].at[e], [(dim, 1)])])
        for q in range(groups):
            settle(flying[q])
            acc[q][mine[q]] = acc[q][mine[q]] + landx[q][e]

    tile = coords[0]
    for i in range(1, 3):
        tile = tile * slab_dims[i][2] + coords[i]
    strip = pl.ds(pl.multiple_of(tile * rows, rows), rows)
    scale = 1.0 / (acc[groups - 1][mine[groups - 1] + (per,)] + probe_reg)
    own = []
    for q in range(groups):
        for i in range(per):
            k, c = plane_of(core, q, i, modes)
            full[q][(core,) + mine[q] + (i,)] = probe[k, c, strip, :] + acc[q][mine[q] + (i,)] * scale
        spot = (core,) + mine[q]
        own.append(remote(full[q].at[spot], full[q].at[spot], [(core_dim, 1)]))
        launch([own[q]])

    def gather_start(q, step):
        dim = dims[q][step]
        spot = (core,) + mine[q][: step + 1]
        return launch([remote(full[q].at[spot], full[q].at[spot], [(dim, d)]) for d in range(1, dim[2])])

    def pass_on(q, step):
        dim = dims[q][step]
        copies = []
        for d in range(1, dim[2]):
            spot = (core,) + mine[q][:step] + (flipped(mine[q][step], dim[2], d),)
            copies.append(remote(full[q].at[spot], full[q].at[spot], [(core_dim, 1)]))
        return launch(copies)

    flying = [gather_start(q, 2) for q in range(groups)]
    handed = []

    def slab_rows(spots):
        values = []
        for p in range(planes):
            c, k = p // modes, p % modes
            half, rest = k // (modes // 2), k % (modes // 2)
            q, m = rest // (per // 2), rest % (per // 2)
            values.append(full[q][(half,) + spots[q] + (2 * m + c,)])
        return jnp.concatenate(values, axis=0)

    tall = planes * rows
    up = lax.broadcasted_iota(jnp.int32, (tall, tall), 0)
    across = lax.broadcasted_iota(jnp.int32, (tall, tall), 1)
    same = jnp.where(((up - across) & (rows - 1)) == 0, 1.0, 0.0).astype(f32)
    plane = lax.broadcasted_iota(jnp.int32, (planes, tall), 0) * rows
    entry = lax.broadcasted_iota(jnp.int32, (planes, tall), 1)
    pick = jnp.where((entry >= plane) & (entry < plane + rows), 1.0, 0.0).astype(f32)
    plane = lax.broadcasted_iota(jnp.int32, (tall, det), 1) * rows
    entry = lax.broadcasted_iota(jnp.int32, (tall, det), 0)
    place = jnp.where((entry >= plane) & (entry < plane + rows), 1.0, 0.0).astype(f32)

    settle(own)
    held = slab_rows(mine)
    turned = jnp.concatenate([-held[tall // 2 :], held[: tall // 2]], axis=0)
    wide = jnp.concatenate([held, turned], axis=1)
    pairs = lax.dot_general(
        wide, wide, (((1,), (1,)), ((), ())), precision=highest, preferred_element_type=f32
    )
    gram = full_dot(full_dot(pick, pairs * same), place)
    settle(swap[groups])
    sums = [jnp.sum(totals[i] + total_land[i]) for i in range(2)]
    lanes = lax.broadcasted_iota(jnp.int32, (8, det), 1)
    first = lax.broadcasted_iota(jnp.int32, (8, det), 0) == 0
    sheet = jnp.where(first & (lanes == det - 2), sums[0], jnp.where(first & (lanes == det - 1), sums[1], 0.0))
    for part in range(planes // 8):
        piece = gram[part * 8 : (part + 1) * 8]
        sheet = sheet + (pltpu.roll(piece, part * 32, 1) if part else piece)
    gram_out[...] = sheet
    spread = []
    slot = 0
    for d0 in range(slab_dims[0][2]):
        for d1 in range(slab_dims[1][2]):
            for d2 in range(slab_dims[2][2]):
                if d0 + d1 + d2:
                    moves = list(zip(slab_dims, (d0, d1, d2)))
                    spread.append(remote(gram_out, gram_land.at[slot], moves))
                    slot += 1
    launch(spread)
    for step in (2, 1):
        for q in range(groups):
            settle(flying[q])
            flying[q] = gather_start(q, step - 1)
            handed += pass_on(q, step)
    settle(spread)
    sheet = gram_out[...]
    for i in range(slab_count - 1):
        sheet = sheet + gram_land[i]
    for e, dim in enumerate(extra):
        gram_x[2 * e] = sheet
        item = launch([remote(gram_x.at[2 * e], gram_x.at[2 * e + 1], [(dim, 1)])])
        settle(item)
        sheet = sheet + gram_x[2 * e + 1]
    measured = jnp.sum(jnp.where(first & (lanes == det - 2), sheet, 0.0))
    modelled = jnp.sum(jnp.where(first & (lanes == det - 1), sheet, 0.0))
    ratio = measured / (modelled + total_eps)
    parts = [sheet[:, part * 32 : part * 32 + planes] for part in range(planes // 8)]
    embedded = jnp.concatenate(parts, axis=0)
    eye = jnp.where(
        lax.broadcasted_iota(jnp.int32, (planes, planes), 0) == lax.broadcasted_iota(jnp.int32, (planes, planes), 1),
        1.0, 0.0,
    ).astype(f32)
    frobenius = jnp.sqrt(jnp.sum(embedded * embedded, keepdims=True))
    current = embedded / frobenius
    inverse = eye
    for repeat in range(NS_STEPS):
        factor = 1.5 * eye - 0.5 * full_dot(inverse, current)
        current = full_dot(current, factor)
        inverse = full_dot(factor, inverse)
    weight = jnp.sqrt(ratio * jnp.sum(embedded * eye, axis=1, keepdims=True))
    mix = weight * (inverse / jnp.sqrt(frobenius))
    spread_mix = lax.dot_general(
        pick, full_dot(mix, pick), (((0,), (0,)), ((), ())), precision=highest, preferred_element_type=f32
    )
    high, low = halves(spread_mix * same)
    mixer = jnp.concatenate([high, low, high], axis=1)
    for q in range(groups):
        settle(flying[q])
        handed += pass_on(q, 0)

    for index, (shift_rows, shift_cols) in enumerate(directions()):
        @pl.when(valid(shift_rows, shift_cols))
        def _():
            fold(index).wait_send()

        @pl.when(valid(-shift_rows, -shift_cols))
        def _():
            fold(index).wait_recv()
            r, c = inner(shift_rows, block_rows), inner(shift_cols, block_cols)
            interior[:, r, c] = interior[:, r, c] + slots[index][...]
    new_specimen[...] = specimen[...] + interior[0:2] / (interior[2] + object_reg)[None]

    settle(handed)
    for t in range(0, slab_count, 2):
        sides = []
        for s in (t, t + 1):
            at = slab_coords(s)
            sides.append(slab_rows([tuple(at[i] for i in order) for order in slab_orders]))
        high, low = halves(jnp.concatenate(sides, axis=1))
        out = jnp.dot(mixer, jnp.concatenate([high, high, low], axis=0), preferred_element_type=f32)
        for p in range(planes):
            for s in range(2):
                new_probe[p % modes, p // modes, (t + s) * rows : (t + s + 1) * rows, :] = out[
                    p * rows : (p + 1) * rows, s * det : (s + 1) * det
                ]


def finish(packed, totals, frame, probe_modes, specimen):
    f32 = jnp.float32
    modes, _, det, _ = probe_modes.shape
    block_rows, block_cols = specimen.shape[1:]
    extra = extra_bits()
    shapes = group_shapes(modes, det)
    planes = 2 * group_modes(modes)
    vmem = pl.BlockSpec(memory_space=pltpu.VMEM)
    count = max(len(extra), 1)
    scratch = [pltpu.VMEM(s, f32) for s in shapes] + [pltpu.VMEM(s, f32) for s in shapes]
    for step in range(3):
        scratch += [pltpu.VMEM((s[step] - 1,) + s[step + 1 :], f32) for s in shapes]
    scratch += [pltpu.VMEM((count,) + s[3:], f32) for s in shapes]
    scratch += [pltpu.VMEM((2,) + s[:3] + (planes,) + s[4:], f32) for s in shapes]
    scratch += [pltpu.VMEM((3, det if i else block_rows, det if j else block_cols), f32) for i, j in directions()]
    sems = 80 + 4 * count
    scratch += [
        pltpu.VMEM(totals.shape, f32),
        pltpu.VMEM((8, det), f32),
        pltpu.VMEM((slab_count - 1, 8, det), f32),
        pltpu.VMEM((2 * count, 8, det), f32),
        pltpu.VMEM((3, block_rows, block_cols), f32),
        pltpu.SemaphoreType.DMA((sems,)),
        pltpu.SemaphoreType.DMA((sems,)),
        pltpu.SemaphoreType.DMA((8,)),
        pltpu.SemaphoreType.DMA((8,)),
    ]

    def kernel(*refs):
        finish_kernel(extra, *refs)

    return pl.pallas_call(
        kernel,
        name="finish",
        out_shape=(
            jax.ShapeDtypeStruct(probe_modes.shape, f32),
            jax.ShapeDtypeStruct(specimen.shape, f32),
        ),
        in_specs=[vmem] * 7,
        out_specs=(vmem, vmem),
        scratch_shapes=scratch,
        compiler_params=pltpu.CompilerParams(has_side_effects=True, vmem_limit_bytes=48 * 1024 * 1024),
    )(*packed, totals, frame, probe_modes, specimen)


def halo_kernel(specimen, out, *rest):
    slots = rest[:8]
    send_sem, recv_sem = rest[8:]
    block_rows, block_cols = specimen.shape[1:]
    det = (out.shape[1] - block_rows) // 2
    here = {axis: lax.axis_index(axis) for axis in ("scan", "tile")}
    sizes = {axis: lax.axis_size(axis) for axis in ("scan", "tile")}

    def edge(shift, block):
        low = {-1: 0, 0: 0, 1: block - det}[shift]
        return pl.ds(low, block if shift == 0 else det)

    def outer(shift, block):
        low = {-1: det + block, 0: det, 1: 0}[shift]
        return pl.ds(low, block if shift == 0 else det)

    def valid(shift_rows, shift_cols):
        row, col = here["scan"] + shift_rows, here["tile"] + shift_cols
        return (row >= 0) & (row < sizes["scan"]) & (col >= 0) & (col < sizes["tile"])

    def send(index):
        shift_rows, shift_cols = directions()[index]
        return pltpu.make_async_remote_copy(
            src_ref=specimen.at[:, edge(shift_rows, block_rows), edge(shift_cols, block_cols)],
            dst_ref=slots[index],
            send_sem=send_sem.at[index],
            recv_sem=recv_sem.at[index],
            device_id={
                "scan": (here["scan"] + shift_rows + sizes["scan"]) % sizes["scan"],
                "tile": (here["tile"] + shift_cols + sizes["tile"]) % sizes["tile"],
            },
            device_id_type=pl.DeviceIdType.MESH,
        )

    for index, shifts in enumerate(directions()):
        @pl.when(valid(*shifts))
        def _():
            send(index).start()
    out[...] = jnp.zeros_like(out)
    out[:, det : det + block_rows, det : det + block_cols] = specimen[...]
    for index, (shift_rows, shift_cols) in enumerate(directions()):
        @pl.when(valid(shift_rows, shift_cols))
        def _():
            send(index).wait_send()

        @pl.when(valid(-shift_rows, -shift_cols))
        def _():
            send(index).wait_recv()
            out[:, outer(shift_rows, block_rows), outer(shift_cols, block_cols)] = slots[index][...]


def with_halo(specimen, det):
    channels, block_rows, block_cols = specimen.shape
    vmem = pl.BlockSpec(memory_space=pltpu.VMEM)
    slots = [
        pltpu.VMEM((channels, det if i else block_rows, det if j else block_cols), jnp.float32)
        for i, j in directions()
    ]
    return pl.pallas_call(
        halo_kernel,
        name="halo",
        out_shape=jax.ShapeDtypeStruct((channels, block_rows + 2 * det, block_cols + 2 * det), jnp.float32),
        in_specs=[vmem],
        out_specs=vmem,
        scratch_shapes=[*slots, pltpu.SemaphoreType.DMA((8,)), pltpu.SemaphoreType.DMA((8,))],
        compiler_params=pltpu.CompilerParams(has_side_effects=True, vmem_limit_bytes=16 * 1024 * 1024),
    )(specimen)


def body(probe_modes, patterns, specimen, offsets):
    detector = probe_modes.shape[-1]
    mode_count = probe_modes.shape[0]
    block_rows = specimen.shape[1]
    block_cols = specimen.shape[2]
    extended = with_halo(specimen, detector)
    *packed, totals, frame_sum = scan_positions(
        offsets, probe_modes, patterns, extended, block_rows, block_cols
    )
    return finish(packed, totals, frame_sum, probe_modes, specimen)


def solution(mesh):
    return jax.shard_map(
        body,
        mesh=mesh,
        in_specs=(
            P(),
            P(("scan", "tile"), None, None),
            P(None, "scan", "tile"),
            P(("scan", "tile"), None),
        ),
        out_specs=(P(), P(None, "scan", "tile")),
        check_vma=False,
    )
```

```python
import math

import jax
import jax.numpy as jnp
import numpy as np
from jax import lax
from jax.experimental import pallas as pl
from jax.experimental.pallas import tpu as pltpu
from jax.sharding import PartitionSpec as P

NS_STEPS = 8


highest = lax.Precision.HIGHEST
light_floor = 0.05
object_reg = 0.5
probe_reg = 1.0
total_eps = 1e-06


def dft_tables(detector):
    indices = np.arange(detector, dtype=np.int64)
    angles = -2.0 * np.pi / detector * (indices[:, None] * indices[None, :] % detector)
    table_re = np.cos(angles) / np.sqrt(detector)
    table_im = np.sin(angles) / np.sqrt(detector)
    right = np.block([[table_re, table_im], [-table_im, table_re]]).astype(np.float32)
    left = np.ascontiguousarray(right.T)
    parts = []
    for table in (right, left):
        high = table.astype(jnp.bfloat16)
        low = (table - high.astype(np.float32)).astype(jnp.bfloat16)
        parts.append((high, low))
    (rh, rl), (lh, ll) = parts
    return (
        np.concatenate([rh, rl, rh], axis=0),
        np.concatenate([lh, ll, lh], axis=1),
        np.concatenate([rh, rl, rh], axis=1),
        np.concatenate([lh, ll, lh], axis=0),
    )


def halves(value):
    high = value.astype(jnp.bfloat16)
    low = (value - high.astype(jnp.float32)).astype(jnp.bfloat16)
    return high, low


core_dim = ("scan", 1, 2)
slab_dims = (("scan", 2, 2), ("tile", 1, 2), ("scan", 4, 4))
slab_orders = ((0, 1, 2), (1, 2, 0), (2, 0, 1))
slab_sizes = tuple(size for _, _, size in slab_dims)
slab_count = math.prod(slab_sizes)
groups = len(slab_orders)


def extra_bits():
    bits = []
    for axis, bit in (("scan", 16), ("tile", 2)):
        while bit < lax.axis_size(axis):
            bits.append((axis, bit, 2))
            bit *= 2
    return bits


def group_planes(modes, q):
    return modes // groups + (q == 0)


def slab_coords(tile):
    coords = []
    for size in reversed(slab_sizes):
        coords.append(tile % size)
        tile = tile // size
    return tuple(coords[::-1])


def directions():
    return [(i, j) for i, j in ((1, 0), (-1, 0), (0, 1), (0, -1), (1, 1), (1, -1), (-1, 1), (-1, -1))]


def digit(dim):
    axis, bit, size = dim
    return (lax.axis_index(axis) // bit) % size


def flipped(value, size, d):
    if size == 2:
        return 1 - value if d else value
    low, high = value % 2, value // 2
    low = 1 - low if d % 2 else low
    high = 1 - high if d // 2 else high
    return low + 2 * high


def peer(moves):
    where = {}
    for dim, d in moves:
        axis, bit, size = dim
        here = digit(dim)
        base = where.get(axis, lax.axis_index(axis))
        where[axis] = base + bit * (flipped(here, size, d) - here)
    return where


def full_dot(a, b):
    return jnp.dot(a, b, precision=highest, preferred_element_type=jnp.float32)


def zeros_into(ref):
    ref[...] = jnp.zeros(ref.shape, ref.dtype)


def update_kernel(extra, names, *refs):
    f32 = jnp.float32
    r = dict(zip(names, refs))
    offs, probe_in, patterns_in, specimen_in = r["offs"], r["probe_in"], r["patterns_in"], r["specimen_in"]
    new_probe, new_specimen = r["new_probe"], r["new_specimen"]
    probe, patterns, specimen, tables = r["probe"], r["patterns"], r["specimen"], [r[f"table{n}"] for n in range(4)]
    ext, pads, frame_num, frame_light = r["ext"], r["pads"], r["frame_num"], r["frame_light"]
    deep, half, far, patch, factor, num = r["deep"], r["half"], r["far"], r["patch"], r["factor"], r["num"]
    power, light, totals, total_land = r["power"], r["light"], r["totals"], r["total_land"]
    packed = [r[f"packed{q}"] for q in range(groups)]
    land0 = [r[f"land0_{q}"] for q in range(groups)]
    acc = [r[f"acc{q}"] for q in range(groups)]
    land = [[r[f"land{s}_{q}"] for q in range(groups)] for s in (1, 2, 3)]
    landx = [r[f"landx{q}"] for q in range(groups)]
    full = [r[f"full{q}"] for q in range(groups)]
    num_slots = [r[f"num_slot{i}"] for i in range(8)]
    light_slots = [r[f"light_slot{i}"] for i in range(8)]
    gram_out, gram_land, gram_x, interior = r["gram_out"], r["gram_land"], r["gram_x"], r["interior"]
    send_sem, recv_sem, local_sem = r["send_sem"], r["recv_sem"], r["local_sem"]
    right_f, left_f, left_b, right_b = tables

    modes, det = probe.shape[0], probe.shape[-1]
    count = patterns.shape[0]
    block_rows, block_cols = specimen.shape[1:]
    own_blocks = block_cols // det
    col_blocks = own_blocks + 2
    ext_rows = block_rows + 2 * det
    per = modes // groups
    pair = per // 2
    rows = det // slab_count
    planes = 2 * modes
    used = [0]

    here = {axis: lax.axis_index(axis) for axis in ("scan", "tile")}
    sizes = {axis: lax.axis_size(axis) for axis in ("scan", "tile")}

    def route(src, dst, device):
        n = used[0]
        used[0] += 1
        return pltpu.make_async_remote_copy(
            src_ref=src, dst_ref=dst, send_sem=send_sem.at[n], recv_sem=recv_sem.at[n],
            device_id=device, device_id_type=pl.DeviceIdType.MESH,
        )

    def remote(src, dst, moves):
        return route(src, dst, peer(moves))

    def shifted(i, j):
        return {
            "scan": (here["scan"] + i + sizes["scan"]) % sizes["scan"],
            "tile": (here["tile"] + j + sizes["tile"]) % sizes["tile"],
        }

    def valid(i, j):
        row, col = here["scan"] + i, here["tile"] + j
        return (row >= 0) & (row < sizes["scan"]) & (col >= 0) & (col < sizes["tile"])

    def launch(copies):
        for item in copies:
            item.start()
        return copies

    def settle(copies):
        for item in copies:
            item.wait()

    core = digit(core_dim)
    mine = [digit(dim) for dim in slab_dims]

    off_shift, on_shift = 2 * core - 1, 1 - 2 * core

    def outer_rows(i):
        return pl.ds(pl.multiple_of((1 - i) // 2 * (det + block_rows), 8), det)

    def edge_rows(i, base):
        return pl.ds(pl.multiple_of(base + (1 + i) // 2 * (block_rows - det), 8), det)

    def edge_block(j):
        return own_blocks - 1 if j == 1 else 0

    def outer_block(j):
        return 0 if j == 1 else own_blocks + 1

    off_valid = valid(off_shift, 0)
    edges = sorted({0, own_blocks - 1})
    inner_blocks = [b for b in range(own_blocks) if b not in edges]
    local = []

    def load(src, dst):
        item = pltpu.make_async_copy(src, dst, local_sem.at[len(local)])
        item.start()
        local.append(item)
        return item

    def row_copies(i, blocks):
        copies = []
        for b in blocks:
            copies.append(
                route(
                    specimen_in.at[:, edge_rows(i, 0), b * det : (b + 1) * det],
                    ext.at[:, 1 + b, outer_rows(i), :],
                    shifted(i, 0),
                )
            )
        return copies

    off_rows = row_copies(off_shift, edges + inner_blocks)
    on_rows = row_copies(on_shift, edges + inner_blocks)

    @pl.when(off_valid)
    def _():
        launch(off_rows[: len(edges)])

    side = {}
    for j in (1, -1):
        b = edge_block(j)
        side[j] = route(
            specimen_in.at[:, :, b * det : (b + 1) * det],
            ext.at[:, outer_block(j), pl.ds(det, block_rows), :],
            shifted(0, j),
        )

        @pl.when(valid(0, j))
        def _():
            side[j].start()

    launch(on_rows)
    if inner_blocks:
        @pl.when(off_valid)
        def _():
            launch(off_rows[len(edges) :])

    probe_load = load(probe_in, probe)
    own_load = [
        load(specimen_in.at[:, :, b * det : (b + 1) * det], ext.at[:, 1 + b, pl.ds(det, block_rows), :])
        for b in range(own_blocks)
    ]
    other_loads = [load(patterns_in, patterns), load(specimen_in, specimen)]
    for n in range(4):
        other_loads.append(load(r[f"table_in{n}"], tables[n]))

    blank = jnp.zeros((2, det, det), f32)
    zeros_into(ext.at[:, col_blocks])

    @pl.when(jnp.logical_not(off_valid))
    def _():
        for b in range(col_blocks):
            ext[:, b, outer_rows(-off_shift), :] = blank

    for j in (1, -1):
        @pl.when(jnp.logical_not(valid(0, -j)))
        def _():
            ext[:, outer_block(j), pl.ds(det, block_rows), :] = jnp.zeros((2, block_rows, det), f32)
            ext[:, outer_block(j), outer_rows(1), :] = blank
            ext[:, outer_block(j), outer_rows(-1), :] = blank

    zeros_into(pads)
    for q in range(groups):
        zeros_into(packed[q])
    zeros_into(light)

    lanes = lax.broadcasted_iota(jnp.int32, (det, det), 1)
    row_base = here["scan"] * block_rows - det
    col_base = here["tile"] * block_cols - det

    def place(p):
        row = jnp.clip(offs[p, 0] - row_base, 0, block_rows + det)
        col = jnp.clip(offs[p, 1] - col_base, 0, block_cols + det)
        block = col // det
        return row, col, block, col - block * det

    def build_frame(frame, channels):
        chunk = 64
        strip_lanes = lax.broadcasted_iota(jnp.int32, (chunk, det), 1)

        def some(n, carry):
            base = pl.multiple_of(n * chunk, chunk)
            for c in range(channels):
                values = [jnp.zeros((chunk, det), f32) for _ in range(col_blocks)]
                for p in range(count):
                    row, col, _, _ = place(p)
                    piece = pads[p, c, pl.ds(ext_rows - det - row + base, chunk), :]
                    for j in range(col_blocks):
                        at = strip_lanes + (j * det - col)
                        values[j] = values[j] + jnp.where((at >= 0) & (at < det), piece, 0.0)
                for j in range(col_blocks):
                    frame[c, pl.ds(base, chunk), j * det : (j + 1) * det] = values[j]
            return carry

        lax.fori_loop(0, ext_rows // chunk, some, 0)

    pad_at = pl.ds(ext_rows - det, det)
    probe_load.wait()
    value = jnp.zeros((det, det), f32)
    for k in range(modes):
        value = value + probe[k, 0] * probe[k, 0] + probe[k, 1] * probe[k, 1]
    power[...] = value
    for p in range(count):
        pads[p, 0, pad_at, :] = pltpu.roll(power[...], place(p)[3], 1)
    build_frame(frame_light, 1)

    @pl.when(off_valid)
    def _():
        for item in off_rows[: len(edges)]:
            item.wait()

    relay = []
    for j in (1, -1):
        b = edge_block(j)
        item = route(
            ext.at[:, 1 + b, outer_rows(-off_shift), :],
            ext.at[:, outer_block(j), outer_rows(-off_shift), :],
            shifted(0, j),
        )
        relay.append((item, off_valid & valid(0, j), off_valid & valid(0, -j)))

        @pl.when(off_valid & valid(0, j))
        def _():
            item.start()

    for j in (1, -1):
        @pl.when(valid(0, j))
        def _():
            side[j].wait_send()

        item = route(
            ext.at[:, outer_block(j), edge_rows(on_shift, det), :],
            ext.at[:, outer_block(j), outer_rows(on_shift), :],
            shifted(on_shift, 0),
        )
        relay.append((item, valid(0, -j), valid(0, -j)))

        @pl.when(valid(0, -j))
        def _():
            side[j].wait_recv()
            item.start()

    settle(on_rows)
    if inner_blocks:
        @pl.when(off_valid)
        def _():
            settle(off_rows[len(edges) :])
    for item, sent, came in relay:
        @pl.when(sent)
        def _():
            item.wait_send()

        @pl.when(came)
        def _():
            item.wait_recv()
    for item in own_load + other_loads:
        item.wait()

    def span(shift, block):
        low = {-1: 0, 0: det, 1: det + block}[shift]
        return pl.ds(low, block if shift == 0 else det)

    def inner(shift, block):
        low = {-1: block - det, 0: 0, 1: 0}[shift]
        return pl.ds(low, block if shift == 0 else det)

    def fold_copies(frame, slots):
        copies = []
        for index, (i, j) in enumerate(directions()):
            copies.append(
                route(frame.at[:, span(i, block_rows), span(j, block_cols)], slots[index], shifted(i, j))
            )
        return copies

    def fold_start(copies, indices):
        for index in indices:
            @pl.when(valid(*directions()[index]))
            def _():
                copies[index].start()

    def fold_end(copies, slots, into):
        for index, (i, j) in enumerate(directions()):
            @pl.when(valid(i, j))
            def _():
                copies[index].wait_send()

            @pl.when(valid(-i, -j))
            def _():
                copies[index].wait_recv()
                a, b = inner(i, block_rows), inner(j, block_cols)
                interior[into, a, b] = interior[into, a, b] + slots[index][...]

    light_fold = fold_copies(frame_light, light_slots)
    fold_start(light_fold, range(8))

    def forward(p, total):
        row, _, block, shift = place(p)
        back = lax.rem(det - shift, det)

        def patch_part(c):
            first = pltpu.roll(ext[c, block, pl.ds(row, det), :], back, 1)
            second = pltpu.roll(ext[c, block + 1, pl.ds(row, det), :], back, 1)
            return jnp.where(lanes < det - shift, first, second)

        patch_re = patch_part(0)
        patch_im = patch_part(1)
        patch[p, 0] = patch_re
        patch[p, 1] = patch_im
        patch_light = patch_re * patch_re + patch_im * patch_im
        light[...] = light[...] + patch_light
        total = total + patch_light * power[...]
        for k in range(modes):
            at = pl.ds(k * det, det)
            pr, pi = probe[k, 0], probe[k, 1]
            for c, value in enumerate((pr * patch_re - pi * patch_im, pr * patch_im + pi * patch_re)):
                high, low = halves(value)
                deep[at, pl.ds(c * det, det)] = high
                deep[at, pl.ds((2 + c) * det, det)] = high
                deep[at, pl.ds((4 + c) * det, det)] = low
        half[...] = jnp.dot(deep[...], right_f[...], preferred_element_type=f32)
        model = jnp.zeros((det, det), f32)
        for k in range(0, modes, 2):
            lo_at, hi_at = pl.ds(k * det, det), pl.ds((k + 1) * det, det)
            first, second = half[lo_at, :], half[hi_at, :]
            paired = jnp.concatenate(
                [
                    jnp.concatenate([first[:, :det], second[:, :det]], axis=1),
                    jnp.concatenate([first[:, det:], second[:, det:]], axis=1),
                ],
                axis=0,
            )
            high, low = halves(paired)
            stacked = jnp.concatenate([high, high, low], axis=0)
            out = jnp.dot(left_f[...], stacked, preferred_element_type=f32)
            far[p, :, pl.ds(k * det, 2 * det)] = out
            squares = out * out
            both = squares[:det] + squares[det:]
            model = model + both[:, :det] + both[:, det:]
        factor[p] = jnp.sqrt(patterns[p]) / jnp.sqrt(jnp.maximum(model, light_floor)) - 1.0
        return total

    total = lax.fori_loop(0, count, forward, jnp.zeros((det, det), f32))
    measured = jnp.zeros((det, det), f32)
    for p in range(count):
        measured = measured + patterns[p]
    totals[0] = jnp.sum(measured.reshape(det // 8, 8, det), axis=0)
    totals[1] = jnp.sum(total.reshape(det // 8, 8, det), axis=0)
    spread_shape = slab_sizes + (rows, det)
    for h in range(2):
        packed[0][h, :, :, :, per] = light[...].reshape(spread_shape)

    def spot_of(q, known, last=None):
        spot = [slice(None)] * 3
        for n in range(known):
            spot[slab_orders[q][n]] = mine[slab_orders[q][n]]
        if last is not None:
            spot[slab_orders[q][known]] = last
        return tuple(spot)

    def other(q, step, d):
        i = slab_orders[q][step]
        return flipped(mine[i], slab_sizes[i], d)

    def reach(q, step):
        return slab_dims[slab_orders[q][step]]

    swap = [remote(packed[q].at[1 - core], land0[q], [(core_dim, 1)]) for q in range(groups)]
    total_swap = remote(totals, total_land, [(core_dim, 1)])
    reducing = []
    for q in range(groups):
        reducing.append([])
        for step in range(3):
            dim = reach(q, step)
            reducing[q].append(
                [
                    remote(acc[q].at[spot_of(q, step, other(q, step, d))], land[step][q].at[d - 1], [(dim, d)])
                    for d in range(1, dim[2])
                ]
            )

    def swap_end(q):
        swap[q].wait()
        acc[q][...] = packed[q][core] + land0[q][...]
        launch(reducing[q][0])

    def reduce_end(q, step):
        settle(reducing[q][step])
        spot = spot_of(q, step + 1)
        value = acc[q][spot]
        for d in range(1, reach(q, step)[2]):
            value = value + land[step][q][d - 1]
        acc[q][spot] = value
        if step < 2:
            launch(reducing[q][step + 1])

    def backward(q, events):
        def one(p, carry):
            for when, event in events:
                @pl.when(p == when)
                def _():
                    event()

            wide = jnp.concatenate([factor[p], factor[p]], axis=1)
            wide = jnp.concatenate([wide, wide], axis=0)
            chosen = [h * (modes // 2) + q * pair + m for h in range(2) for m in range(pair)]
            for n in range(0, per, 2):
                high, low = halves(far[p, :, pl.ds(chosen[n] * det, 2 * det)] * wide)
                stacked = jnp.concatenate([high, high, low], axis=0)
                out = jnp.dot(left_b[...], stacked, preferred_element_type=f32)
                high, low = halves(out)
                for m in range(2):
                    at = pl.ds((n + m) * det, det)
                    for c in range(2):
                        part_h = high[c * det : (c + 1) * det, m * det : (m + 1) * det]
                        part_l = low[c * det : (c + 1) * det, m * det : (m + 1) * det]
                        deep[at, pl.ds(c * det, det)] = part_h
                        deep[at, pl.ds((2 + c) * det, det)] = part_h
                        deep[at, pl.ds((4 + c) * det, det)] = part_l
            some = pl.ds(0, per * det)
            half[some, :] = jnp.dot(deep[some, :], right_b[...], preferred_element_type=f32)
            patch_re, patch_im = patch[p, 0], patch[p, 1]
            num_re = jnp.zeros((det, det), f32)
            num_im = jnp.zeros((det, det), f32)
            for n, k in enumerate(chosen):
                at = pl.ds(n * det, det)
                cr, ci = half[at, :det], half[at, det:]
                pr, pi = probe[k, 0], probe[k, 1]
                h, i = n // pair, n % pair
                for c, value in enumerate((patch_re * cr + patch_im * ci, patch_re * ci - patch_im * cr)):
                    spot = (h, slice(None), slice(None), slice(None), 2 * i + c)
                    packed[q][spot] = packed[q][spot] + value.reshape(spread_shape)
                num_re = num_re + pr * cr + pi * ci
                num_im = num_im + pr * ci - pi * cr
            if q:
                num_re = num_re + num[p, 0]
                num_im = num_im + num[p, 1]
            if q < groups - 1:
                num[p, 0] = num_re
                num[p, 1] = num_im
            else:
                shift = place(p)[3]
                pads[p, 0, pad_at, :] = pltpu.roll(num_re, shift, 1)
                pads[p, 1, pad_at, :] = pltpu.roll(num_im, shift, 1)
            return carry

        lax.fori_loop(0, count, one, 0)

    backward(0, [])
    swap[0].start()
    total_swap.start()
    backward(1, [(2, lambda: swap_end(0))])
    swap[1].start()
    backward(2, [(2, lambda: (swap_end(1), reduce_end(0, 0)))])
    swap[2].start()
    build_frame(frame_num, 2)
    num_fold = fold_copies(frame_num, num_slots)
    reduce_end(0, 1)
    swap_end(2)
    fold_start(num_fold, (0, 1))
    reduce_end(1, 0)
    reduce_end(0, 2)
    fold_start(num_fold, (2, 3))
    reduce_end(1, 1)
    reduce_end(2, 0)
    fold_start(num_fold, (4, 5, 6, 7))

    tile = mine[0]
    for i in range(1, 3):
        tile = tile * slab_sizes[i] + mine[i]
    strip = pl.ds(pl.multiple_of(tile * rows, rows), rows)
    home = tuple(mine)
    own = [remote(full[q].at[(core,) + home], full[q].at[(core,) + home], [(core_dim, 1)]) for q in range(groups)]
    gathering, passing = [], []
    for q in range(groups):
        gathering.append([])
        passing.append([])
        for step in range(3):
            dim = reach(q, step)
            spot = (core,) + spot_of(q, step + 1)
            gathering[q].append(
                [remote(full[q].at[spot], full[q].at[spot], [(dim, d)]) for d in range(1, dim[2])]
            )
            passed = []
            for d in range(1, dim[2]):
                spot = (core,) + spot_of(q, step, other(q, step, d))
                passed.append(remote(full[q].at[spot], full[q].at[spot], [(core_dim, 1)]))
            passing[q].append(passed)

    def update_slab(q):
        for e, dim in enumerate(extra):
            item = remote(acc[q].at[home], landx[q].at[e], [(dim, 1)])
            item.start()
            item.wait()
            acc[q][home] = acc[q][home] + landx[q][e]
        scale = 1.0 / (acc[0][home + (per,)] + probe_reg)
        for i in range(per):
            k = core * (modes // 2) + q * pair + i // 2
            full[q][(core,) + home + (i,)] = probe[k, i % 2, strip, :] + acc[q][home + (i,)] * scale
        own[q].start()
        launch(gathering[q][2])

    def gather_end(q, step):
        settle(gathering[q][step])
        if step:
            launch(gathering[q][step - 1])
        launch(passing[q][step])

    update_slab(0)
    reduce_end(1, 2)
    update_slab(1)
    reduce_end(2, 1)
    gather_end(0, 2)
    reduce_end(2, 2)
    update_slab(2)
    gather_end(1, 2)
    gather_end(0, 1)

    def slab_rows(spot):
        values = []
        for n in range(planes):
            c, k = n // modes, n % modes
            h, rest = k // (modes // 2), k % (modes // 2)
            q, m = rest // pair, rest % pair
            values.append(full[q][(h,) + spot + (2 * m + c,)])
        return jnp.concatenate(values, axis=0)

    tall = planes * rows
    up = lax.broadcasted_iota(jnp.int32, (tall, tall), 0)
    across = lax.broadcasted_iota(jnp.int32, (tall, tall), 1)
    same = jnp.where(((up - across) & (rows - 1)) == 0, 1.0, 0.0).astype(f32)
    plane = lax.broadcasted_iota(jnp.int32, (planes, tall), 0) * rows
    entry = lax.broadcasted_iota(jnp.int32, (planes, tall), 1)
    pick = jnp.where((entry >= plane) & (entry < plane + rows), 1.0, 0.0).astype(f32)
    plane = lax.broadcasted_iota(jnp.int32, (tall, det), 1) * rows
    entry = lax.broadcasted_iota(jnp.int32, (tall, det), 0)
    settled = jnp.where((entry >= plane) & (entry < plane + rows), 1.0, 0.0).astype(f32)

    settle(own)
    held = slab_rows(home)
    turned = jnp.concatenate([-held[tall // 2 :], held[: tall // 2]], axis=0)
    wide = jnp.concatenate([held, turned], axis=1)
    pairs = lax.dot_general(
        wide, wide, (((1,), (1,)), ((), ())), precision=highest, preferred_element_type=f32
    )
    gram = full_dot(full_dot(pick, pairs * same), settled)
    total_swap.wait()
    sums = [jnp.sum(totals[i] + total_land[i]) for i in range(2)]
    sheet_lanes = lax.broadcasted_iota(jnp.int32, (8, det), 1)
    first = lax.broadcasted_iota(jnp.int32, (8, det), 0) == 0
    at_measured = first & (sheet_lanes == det - 2)
    at_modelled = first & (sheet_lanes == det - 1)
    sheet = jnp.where(at_measured, sums[0], jnp.where(at_modelled, sums[1], 0.0))
    for part in range(planes // 8):
        piece = gram[part * 8 : (part + 1) * 8]
        sheet = sheet + (pltpu.roll(piece, part * 32, 1) if part else piece)
    gram_out[...] = sheet
    spread = []
    for slot in range(1, slab_count):
        moves = list(zip(slab_dims, slab_coords(slot)))
        spread.append(remote(gram_out, gram_land.at[slot - 1], moves))
    launch(spread)
    gather_end(2, 2)
    gather_end(1, 1)
    gather_end(2, 1)
    settle(spread)
    sheet = gram_out[...]
    for i in range(slab_count - 1):
        sheet = sheet + gram_land[i]
    for e, dim in enumerate(extra):
        gram_x[2 * e] = sheet
        item = remote(gram_x.at[2 * e], gram_x.at[2 * e + 1], [(dim, 1)])
        item.start()
        item.wait()
        sheet = sheet + gram_x[2 * e + 1]
    measured = jnp.sum(jnp.where(at_measured, sheet, 0.0))
    modelled = jnp.sum(jnp.where(at_modelled, sheet, 0.0))
    ratio = measured / (modelled + total_eps)
    parts = [sheet[:, part * 32 : part * 32 + planes] for part in range(planes // 8)]
    embedded = jnp.concatenate(parts, axis=0)
    eye = jnp.where(
        lax.broadcasted_iota(jnp.int32, (planes, planes), 0) == lax.broadcasted_iota(jnp.int32, (planes, planes), 1),
        1.0, 0.0,
    ).astype(f32)
    frobenius = jnp.sqrt(jnp.sum(embedded * embedded, keepdims=True))
    current = embedded / frobenius
    inverse = eye
    for repeat in range(NS_STEPS):
        scaled = 1.5 * eye - 0.5 * full_dot(inverse, current)
        current = full_dot(current, scaled)
        inverse = full_dot(scaled, inverse)
    weight = jnp.sqrt(ratio * jnp.sum(embedded * eye, axis=1, keepdims=True))
    mix = weight * (inverse / jnp.sqrt(frobenius))
    mix = lax.dot_general(
        pick, full_dot(mix, pick), (((0,), (0,)), ((), ())), precision=highest, preferred_element_type=f32
    )
    high, low = halves(mix * same)
    mixer = jnp.concatenate([high, low, high], axis=1)
    for q in range(groups):
        gather_end(q, 0)

    interior[0:2] = frame_num[:, det : det + block_rows, det : det + block_cols]
    interior[2] = frame_light[0, det : det + block_rows, det : det + block_cols]
    fold_end(light_fold, light_slots, slice(2, 3))
    fold_end(num_fold, num_slots, slice(0, 2))
    new_specimen[...] = specimen[...] + interior[0:2] / (interior[2] + object_reg)[None]

    for q in range(groups):
        for step in range(3):
            settle(passing[q][step])
    for t in range(0, slab_count, 2):
        sides = [slab_rows(slab_coords(s)) for s in (t, t + 1)]
        high, low = halves(jnp.concatenate(sides, axis=1))
        out = jnp.dot(mixer, jnp.concatenate([high, high, low], axis=0), preferred_element_type=f32)
        for n in range(planes):
            for s in range(2):
                new_probe[n % modes, n // modes, (t + s) * rows : (t + s + 1) * rows, :] = out[
                    n * rows : (n + 1) * rows, s * det : (s + 1) * det
                ]


def body(probe_modes, patterns, specimen, offsets):
    f32 = jnp.float32
    modes, _, det, _ = probe_modes.shape
    count = patterns.shape[0]
    block_rows, block_cols = specimen.shape[1:]
    col_blocks = block_cols // det + 2
    ext_rows = block_rows + 2 * det
    ext_cols = block_cols + 2 * det
    extra = extra_bits()
    more = max(len(extra), 1)
    rows = det // slab_count
    bf16 = jnp.bfloat16
    tables = [jnp.asarray(t) for t in dft_tables(det)]
    sems = 160 + 6 * more
    scratch = {
        "probe": pltpu.VMEM(probe_modes.shape, f32),
        "patterns": pltpu.VMEM(patterns.shape, f32),
        "specimen": pltpu.VMEM(specimen.shape, f32),
        **{f"table{n}": pltpu.VMEM(t.shape, bf16) for n, t in enumerate(tables)},
        "ext": pltpu.VMEM((2, col_blocks + 1, ext_rows, det), f32),
        "pads": pltpu.VMEM((count, 2, 2 * (ext_rows - det) + det, det), f32),
        "frame_num": pltpu.VMEM((2, ext_rows, ext_cols), f32),
        "frame_light": pltpu.VMEM((1, ext_rows, ext_cols), f32),
        "deep": pltpu.VMEM((modes * det, 6 * det), bf16),
        "half": pltpu.VMEM((modes * det, 2 * det), f32),
        "far": pltpu.VMEM((count, 2 * det, modes * det), f32),
        "patch": pltpu.VMEM((count, 2, det, det), f32),
        "factor": pltpu.VMEM((count, det, det), f32),
        "num": pltpu.VMEM((count, 2, det, det), f32),
        "power": pltpu.VMEM((det, det), f32),
        "light": pltpu.VMEM((det, det), f32),
        "totals": pltpu.VMEM((2, 8, det), f32),
        "total_land": pltpu.VMEM((2, 8, det), f32),
        "gram_out": pltpu.VMEM((8, det), f32),
        "gram_land": pltpu.VMEM((slab_count - 1, 8, det), f32),
        "gram_x": pltpu.VMEM((2 * more, 8, det), f32),
        "interior": pltpu.VMEM((3, block_rows, block_cols), f32),
        "send_sem": pltpu.SemaphoreType.DMA((sems,)),
        "recv_sem": pltpu.SemaphoreType.DMA((sems,)),
        "local_sem": pltpu.SemaphoreType.DMA((16,)),
    }
    for q, order in enumerate(slab_orders):
        tile = (group_planes(modes, q), rows, det)
        scratch[f"packed{q}"] = pltpu.VMEM((2,) + slab_sizes + tile, f32)
        scratch[f"land0_{q}"] = pltpu.VMEM(slab_sizes + tile, f32)
        scratch[f"acc{q}"] = pltpu.VMEM(slab_sizes + tile, f32)
        scratch[f"landx{q}"] = pltpu.VMEM((more,) + tile, f32)
        scratch[f"full{q}"] = pltpu.VMEM((2,) + slab_sizes + (modes // groups, rows, det), f32)
        for step in range(3):
            kept = tuple(slab_sizes[i] for i in range(3) if i not in order[: step + 1])
            scratch[f"land{step + 1}_{q}"] = pltpu.VMEM((slab_sizes[order[step]] - 1,) + kept + tile, f32)
    for index, (i, j) in enumerate(directions()):
        shape = (det if i else block_rows, det if j else block_cols)
        scratch[f"num_slot{index}"] = pltpu.VMEM((2,) + shape, f32)
        scratch[f"light_slot{index}"] = pltpu.VMEM((1,) + shape, f32)
    names = ["offs", "probe_in", "patterns_in", "specimen_in"]
    names += [f"table_in{n}" for n in range(4)] + ["new_probe", "new_specimen"] + list(scratch)

    def kernel(*refs):
        update_kernel(extra, names, *refs)

    vmem = pl.BlockSpec(memory_space=pltpu.VMEM)
    return pl.pallas_call(
        kernel,
        name="update",
        out_shape=(
            jax.ShapeDtypeStruct(probe_modes.shape, f32),
            jax.ShapeDtypeStruct(specimen.shape, f32),
        ),
        in_specs=[pl.BlockSpec(memory_space=pltpu.SMEM)] + [pl.BlockSpec(memory_space=pl.ANY)] * 7,
        out_specs=(vmem, vmem),
        scratch_shapes=list(scratch.values()),
        compiler_params=pltpu.CompilerParams(has_side_effects=True, vmem_limit_bytes=56 * 1024 * 1024),
    )(offsets, probe_modes, patterns, specimen, *tables)


def solution(mesh):
    return jax.shard_map(
        body,
        mesh=mesh,
        in_specs=(
            P(),
            P(("scan", "tile"), None, None),
            P(None, "scan", "tile"),
            P(("scan", "tile"), None),
        ),
        out_specs=(P(), P(None, "scan", "tile")),
        check_vma=False,
    )
```

```python
import math

import jax
import jax.numpy as jnp
import numpy as np
from jax import lax
from jax.experimental import pallas as pl
from jax.experimental.pallas import tpu as pltpu
from jax.sharding import PartitionSpec as P

NS_STEPS = 8


highest = lax.Precision.HIGHEST
light_floor = 0.05
object_reg = 0.5
probe_reg = 1.0
total_eps = 1e-06


def dft_tables(detector):
    indices = np.arange(detector, dtype=np.int64)
    angles = -2.0 * np.pi / detector * (indices[:, None] * indices[None, :] % detector)
    table_re = np.cos(angles) / np.sqrt(detector)
    table_im = np.sin(angles) / np.sqrt(detector)
    right = np.block([[table_re, table_im], [-table_im, table_re]]).astype(np.float32)
    left = np.ascontiguousarray(right.T)
    parts = []
    for table in (right, left):
        high = table.astype(jnp.bfloat16)
        low = (table - high.astype(np.float32)).astype(jnp.bfloat16)
        parts.append((high, low))
    (rh, rl), (lh, ll) = parts
    return (
        np.concatenate([rh, rl, rh], axis=0),
        np.concatenate([lh, ll, lh], axis=1),
        np.concatenate([rh, rl, rh], axis=1),
        np.concatenate([lh, ll, lh], axis=0),
    )


def halves(value):
    high = value.astype(jnp.bfloat16)
    low = (value - high.astype(jnp.float32)).astype(jnp.bfloat16)
    return high, low


core_dim = ("scan", 1, 2)
slab_dims = (("scan", 2, 2), ("tile", 1, 2), ("scan", 4, 4))
slab_sizes = tuple(size for _, _, size in slab_dims)
slab_count = math.prod(slab_sizes)


def extra_bits():
    bits = []
    for axis, bit in (("scan", 16), ("tile", 2)):
        while bit < lax.axis_size(axis):
            bits.append((axis, bit, 2))
            bit *= 2
    return bits


def order_of(q):
    return (1, 0, 2) if q % 2 else (0, 1, 2)


def slab_coords(tile):
    coords = []
    for size in reversed(slab_sizes):
        coords.append(tile % size)
        tile = tile // size
    return tuple(coords[::-1])


def directions():
    return [(i, j) for i, j in ((1, 0), (-1, 0), (0, 1), (0, -1), (1, 1), (1, -1), (-1, 1), (-1, -1))]


def digit(dim):
    axis, bit, size = dim
    return (lax.axis_index(axis) // bit) % size


def flipped(value, size, d):
    if size == 2:
        return 1 - value if d else value
    low, high = value % 2, value // 2
    low = 1 - low if d % 2 else low
    high = 1 - high if d // 2 else high
    return low + 2 * high


def peer(moves):
    where = {}
    for dim, d in moves:
        axis, bit, size = dim
        here = digit(dim)
        base = where.get(axis, lax.axis_index(axis))
        where[axis] = base + bit * (flipped(here, size, d) - here)
    return where


def full_dot(a, b):
    return jnp.dot(a, b, precision=highest, preferred_element_type=jnp.float32)


def zeros_into(ref):
    ref[...] = jnp.zeros(ref.shape, ref.dtype)


def update_kernel(extra, names, *refs):
    f32 = jnp.float32
    r = dict(zip(names, refs))
    offs, probe_in, patterns_in, specimen_in = r["offs"], r["probe_in"], r["patterns_in"], r["specimen_in"]
    new_probe, new_specimen = r["new_probe"], r["new_specimen"]
    probe, patterns, specimen, tables = r["probe"], r["patterns"], r["specimen"], [r[f"table{n}"] for n in range(4)]
    ext, pads, frame_num, frame_light = r["ext"], r["pads"], r["frame_num"], r["frame_light"]
    deep, half, far, patch, factor, num = r["deep"], r["half"], r["far"], r["patch"], r["factor"], r["num"]
    power, light, totals, total_land = r["power"], r["light"], r["totals"], r["total_land"]
    packed, land0, acc, full = r["packed"], r["land0"], r["acc"], r["full"]
    land1, land2, land3, landx, land_all = r["land1"], r["land2"], r["land3"], r["landx"], r["land_all"]
    num_slots = [r[f"num_slot{i}"] for i in range(8)]
    light_slots = [r[f"light_slot{i}"] for i in range(8)]
    gram_out, gram_land, gram_x, interior = r["gram_out"], r["gram_land"], r["gram_x"], r["interior"]
    send_sem, recv_sem, local_sem = r["send_sem"], r["recv_sem"], r["local_sem"]
    right_f, left_f, left_b, right_b = tables

    modes, det = probe.shape[0], probe.shape[-1]
    count = patterns.shape[0]
    block_rows, block_cols = specimen.shape[1:]
    own_blocks = block_cols // det
    col_blocks = own_blocks + 2
    ext_rows = block_rows + 2 * det
    groups = modes // 2
    mode_order = [q + h * groups for q in range(groups) for h in range(2)]
    rows = det // slab_count
    planes = 2 * modes
    used = [0]

    here = {axis: lax.axis_index(axis) for axis in ("scan", "tile")}
    sizes = {axis: lax.axis_size(axis) for axis in ("scan", "tile")}

    def route(src, dst, device):
        n = used[0]
        used[0] += 1
        return pltpu.make_async_remote_copy(
            src_ref=src, dst_ref=dst, send_sem=send_sem.at[n], recv_sem=recv_sem.at[n],
            device_id=device, device_id_type=pl.DeviceIdType.MESH,
        )

    def remote(src, dst, moves):
        return route(src, dst, peer(moves))

    class Batch:
        def __init__(self, whole):
            self.whole = whole
            self.n = used[0]
            used[0] += 1

        def make(self, src, dst, device):
            return pltpu.make_async_remote_copy(
                src_ref=src, dst_ref=dst, send_sem=send_sem.at[self.n], recv_sem=recv_sem.at[self.n],
                device_id=device, device_id_type=pl.DeviceIdType.MESH,
            )

        def send(self, src, dst, moves):
            self.make(src, dst, peer(moves)).start()

        def wait(self):
            self.make(self.whole, self.whole, peer([(core_dim, 1)])).wait()

    def shifted(i, j):
        return {
            "scan": (here["scan"] + i + sizes["scan"]) % sizes["scan"],
            "tile": (here["tile"] + j + sizes["tile"]) % sizes["tile"],
        }

    def valid(i, j):
        row, col = here["scan"] + i, here["tile"] + j
        return (row >= 0) & (row < sizes["scan"]) & (col >= 0) & (col < sizes["tile"])

    def launch(copies):
        for item in copies:
            item.start()
        return copies

    def settle(copies):
        for item in copies:
            item.wait()

    core = digit(core_dim)
    mine = [digit(dim) for dim in slab_dims]

    off_shift, on_shift = 2 * core - 1, 1 - 2 * core

    def outer_rows(i):
        return pl.ds(pl.multiple_of((1 - i) // 2 * (det + block_rows), 8), det)

    def edge_rows(i, base):
        return pl.ds(pl.multiple_of(base + (1 + i) // 2 * (block_rows - det), 8), det)

    def edge_block(j):
        return own_blocks - 1 if j == 1 else 0

    def outer_block(j):
        return 0 if j == 1 else own_blocks + 1

    off_valid = valid(off_shift, 0)
    edges = sorted({0, own_blocks - 1})
    inner_blocks = [b for b in range(own_blocks) if b not in edges]
    local = []

    def load(src, dst):
        item = pltpu.make_async_copy(src, dst, local_sem.at[len(local)])
        item.start()
        local.append(item)
        return item

    def row_copies(i, blocks):
        copies = []
        for b in blocks:
            copies.append(
                route(
                    specimen_in.at[:, edge_rows(i, 0), b * det : (b + 1) * det],
                    ext.at[:, 1 + b, outer_rows(i), :],
                    shifted(i, 0),
                )
            )
        return copies

    off_rows = row_copies(off_shift, edges + inner_blocks)
    on_rows = row_copies(on_shift, edges + inner_blocks)

    @pl.when(off_valid)
    def _():
        launch(off_rows[: len(edges)])

    side = {}
    for j in (1, -1):
        b = edge_block(j)
        side[j] = route(
            specimen_in.at[:, :, b * det : (b + 1) * det],
            ext.at[:, outer_block(j), pl.ds(det, block_rows), :],
            shifted(0, j),
        )

        @pl.when(valid(0, j))
        def _():
            side[j].start()

    launch(on_rows)
    if inner_blocks:
        @pl.when(off_valid)
        def _():
            launch(off_rows[len(edges) :])

    probe_load = load(probe_in, probe)
    own_load = [
        load(specimen_in.at[:, :, b * det : (b + 1) * det], ext.at[:, 1 + b, pl.ds(det, block_rows), :])
        for b in range(own_blocks)
    ]
    other_loads = [load(patterns_in, patterns), load(specimen_in, specimen)]
    for n in range(4):
        other_loads.append(load(r[f"table_in{n}"], tables[n]))

    blank = jnp.zeros((2, det, det), f32)
    zeros_into(ext.at[:, col_blocks])

    @pl.when(jnp.logical_not(off_valid))
    def _():
        for b in range(col_blocks):
            ext[:, b, outer_rows(-off_shift), :] = blank

    for j in (1, -1):
        @pl.when(jnp.logical_not(valid(0, -j)))
        def _():
            ext[:, outer_block(j), pl.ds(det, block_rows), :] = jnp.zeros((2, block_rows, det), f32)
            ext[:, outer_block(j), outer_rows(1), :] = blank
            ext[:, outer_block(j), outer_rows(-1), :] = blank

    zeros_into(pads)
    zeros_into(num)
    zeros_into(light)

    lanes = lax.broadcasted_iota(jnp.int32, (det, det), 1)
    row_base = here["scan"] * block_rows - det
    col_base = here["tile"] * block_cols - det

    def place(p):
        row = jnp.clip(offs[0, p] - row_base, 0, block_rows + det)
        col = jnp.clip(offs[1, p] - col_base, 0, block_cols + det)
        block = col // det
        return row, col, block, col - block * det

    def build_frame(frame, channels):
        chunk = 64
        strip_lanes = lax.broadcasted_iota(jnp.int32, (chunk, det), 1)

        def some(n, carry):
            base = pl.multiple_of(n * chunk, chunk)
            for c in range(channels):
                values = [jnp.zeros((chunk, det), f32) for _ in range(col_blocks)]
                for p in range(count):
                    row, col, _, _ = place(p)
                    piece = pads[p, c, pl.ds(ext_rows - det - row + base, chunk), :]
                    for j in range(col_blocks):
                        at = strip_lanes + (j * det - col)
                        values[j] = values[j] + jnp.where((at >= 0) & (at < det), piece, 0.0)
                for j in range(col_blocks):
                    frame[c, pl.ds(base, chunk), j * det : (j + 1) * det] = values[j]
            return carry

        lax.fori_loop(0, ext_rows // chunk, some, 0)

    pad_at = pl.ds(ext_rows - det, det)
    probe_load.wait()
    value = jnp.zeros((det, det), f32)
    for k in range(modes):
        value = value + probe[k, 0] * probe[k, 0] + probe[k, 1] * probe[k, 1]
    power[...] = value
    for p in range(count):
        pads[p, 0, pad_at, :] = pltpu.roll(power[...], place(p)[3], 1)
    build_frame(frame_light, 1)

    @pl.when(off_valid)
    def _():
        for item in off_rows[: len(edges)]:
            item.wait()

    relay = []
    for j in (1, -1):
        b = edge_block(j)
        item = route(
            ext.at[:, 1 + b, outer_rows(-off_shift), :],
            ext.at[:, outer_block(j), outer_rows(-off_shift), :],
            shifted(0, j),
        )
        relay.append((item, off_valid & valid(0, j), off_valid & valid(0, -j)))

        @pl.when(off_valid & valid(0, j))
        def _():
            item.start()

    for j in (1, -1):
        @pl.when(valid(0, j))
        def _():
            side[j].wait_send()

        item = route(
            ext.at[:, outer_block(j), edge_rows(on_shift, det), :],
            ext.at[:, outer_block(j), outer_rows(on_shift), :],
            shifted(on_shift, 0),
        )
        relay.append((item, valid(0, -j), valid(0, -j)))

        @pl.when(valid(0, -j))
        def _():
            side[j].wait_recv()
            item.start()

    settle(on_rows)
    if inner_blocks:
        @pl.when(off_valid)
        def _():
            settle(off_rows[len(edges) :])
    for item, sent, came in relay:
        @pl.when(sent)
        def _():
            item.wait_send()

        @pl.when(came)
        def _():
            item.wait_recv()
    for item in own_load + other_loads:
        item.wait()

    def span(shift, block):
        low = {-1: 0, 0: det, 1: det + block}[shift]
        return pl.ds(low, block if shift == 0 else det)

    def inner(shift, block):
        low = {-1: block - det, 0: 0, 1: 0}[shift]
        return pl.ds(low, block if shift == 0 else det)

    def fold_copies(frame, slots):
        copies = []
        for index, (i, j) in enumerate(directions()):
            copies.append(
                route(frame.at[:, span(i, block_rows), span(j, block_cols)], slots[index], shifted(i, j))
            )
        return copies

    def fold_start(copies, indices):
        for index in indices:
            @pl.when(valid(*directions()[index]))
            def _():
                copies[index].start()

    def fold_end(copies, slots, into):
        for index, (i, j) in enumerate(directions()):
            @pl.when(valid(i, j))
            def _():
                copies[index].wait_send()

            @pl.when(valid(-i, -j))
            def _():
                copies[index].wait_recv()
                a, b = inner(i, block_rows), inner(j, block_cols)
                interior[into, a, b] = interior[into, a, b] + slots[index][...]

    light_fold = fold_copies(frame_light, light_slots)
    fold_start(light_fold, range(8))

    def forward(p, total):
        row, _, block, shift = place(p)
        back = lax.rem(det - shift, det)

        def patch_part(c):
            first = pltpu.roll(ext[c, block, pl.ds(row, det), :], back, 1)
            second = pltpu.roll(ext[c, block + 1, pl.ds(row, det), :], back, 1)
            return jnp.where(lanes < det - shift, first, second)

        patch_re = patch_part(0)
        patch_im = patch_part(1)
        patch[p, 0] = patch_re
        patch[p, 1] = patch_im
        patch_light = patch_re * patch_re + patch_im * patch_im
        light[...] = light[...] + patch_light
        total = total + patch_light * power[...]
        for n, k in enumerate(mode_order):
            at = pl.ds(n * det, det)
            pr, pi = probe[k, 0], probe[k, 1]
            for c, value in enumerate((pr * patch_re - pi * patch_im, pr * patch_im + pi * patch_re)):
                high, low = halves(value)
                deep[at, pl.ds(c * det, det)] = high
                deep[at, pl.ds((2 + c) * det, det)] = high
                deep[at, pl.ds((4 + c) * det, det)] = low
        half[...] = jnp.dot(deep[...], right_f[...], preferred_element_type=f32)
        model = jnp.zeros((det, det), f32)
        for k in range(0, modes, 2):
            lo_at, hi_at = pl.ds(k * det, det), pl.ds((k + 1) * det, det)
            first, second = half[lo_at, :], half[hi_at, :]
            paired = jnp.concatenate(
                [
                    jnp.concatenate([first[:, :det], second[:, :det]], axis=1),
                    jnp.concatenate([first[:, det:], second[:, det:]], axis=1),
                ],
                axis=0,
            )
            high, low = halves(paired)
            stacked = jnp.concatenate([high, high, low], axis=0)
            out = jnp.dot(left_f[...], stacked, preferred_element_type=f32)
            far[p, :, pl.ds(k * det, 2 * det)] = out
            squares = out * out
            both = squares[:det] + squares[det:]
            model = model + both[:, :det] + both[:, det:]
        factor[p] = jnp.sqrt(patterns[p]) / jnp.sqrt(jnp.maximum(model, light_floor)) - 1.0
        return total

    total = lax.fori_loop(0, count, forward, jnp.zeros((det, det), f32))
    measured = jnp.zeros((det, det), f32)
    for p in range(count):
        measured = measured + patterns[p]
    totals[0] = jnp.sum(measured.reshape(det // 8, 8, det), axis=0)
    totals[1] = jnp.sum(total.reshape(det // 8, 8, det), axis=0)
    spread_shape = slab_sizes + (rows, det)
    for h in range(2):
        r["packed_light"][h, :, :, :, 0] = light[...].reshape(spread_shape)

    home = tuple(mine)

    def spot_of(order, known, d=0):
        spot = [slice(None)] * 3
        for n in range(known):
            spot[order[n]] = mine[order[n]]
        if d:
            i = order[known]
            spot[i] = flipped(mine[i], slab_sizes[i], d)
        return tuple(spot)

    class Sum:
        def __init__(self, order, direct, source, land0, acc, lands, landx):
            self.order, self.direct, self.source, self.acc = order, direct, source, acc
            self.land0, self.lands, self.landx = land0, lands, landx
            self.swap = remote(source.at[1 - core], land0, [(core_dim, 1)])
            self.batches = [Batch(land) for land in lands]

        def send(self, step):
            batch, land = self.batches[step], self.lands[step]
            if self.direct:
                for slot in range(1, slab_count):
                    flips = slab_coords(slot)
                    spot = tuple(flipped(mine[i], slab_sizes[i], flips[i]) for i in range(3))
                    batch.send(self.acc.at[spot], land.at[slot - 1], list(zip(slab_dims, flips)))
                return
            dim = slab_dims[self.order[step]]
            for d in range(1, dim[2]):
                batch.send(self.acc.at[spot_of(self.order, step, d)], land.at[d - 1], [(dim, d)])

        def swapped(self):
            self.swap.wait()
            self.acc[...] = self.source[core] + self.land0[...]
            self.send(0)

        def reduced(self, step):
            self.batches[step].wait()
            land = self.lands[step]
            last = step == len(self.lands) - 1
            spot = home if last else spot_of(self.order, step + 1)
            value = self.acc[spot]
            for d in range(land.shape[0]):
                value = value + land[d]
            self.acc[spot] = value
            if not last:
                self.send(step + 1)
                return
            for e, dim in enumerate(extra):
                item = remote(self.acc.at[home], self.landx.at[e], [(dim, 1)])
                item.start()
                item.wait()
                self.acc[home] = self.acc[home] + self.landx[e]

    light_sum = Sum(
        order_of(1), False, r["packed_light"], r["land0_light"], r["acc_light"],
        [r["land1_light"], r["land2_light"], r["land3_light"]], r["landx_light"],
    )
    sums = []
    for q in range(groups):
        direct = q == groups - 1
        lands = [land_all] if direct else [land1.at[q], land2.at[q], land3.at[q]]
        sums.append(Sum(order_of(q), direct, packed.at[q], land0.at[q], acc.at[q], lands, landx.at[q]))
    total_swap = remote(totals, total_land, [(core_dim, 1)])

    def at_group(n):
        if n == 0:
            light_sum.swap.start()
            total_swap.start()
            return
        sums[n - 1].swap.start()
        if n == 1:
            light_sum.swapped()
        if n >= 2:
            sums[n - 2].swapped()
        if n == 3:
            light_sum.reduced(0)
        if n >= 4:
            sums[n - 4].reduced(0)
        if n == 5:
            light_sum.reduced(1)
        if n >= 6:
            sums[n - 6].reduced(1)

    def backward(q, carry):
        for n in range(groups):
            @pl.when(q == n)
            def _():
                at_group(n)

        columns = pl.ds(pl.multiple_of(q * 2 * det, 2 * det), 2 * det)
        for p in range(count):
            wide = jnp.concatenate([factor[p], factor[p]], axis=1)
            wide = jnp.concatenate([wide, wide], axis=0)
            high, low = halves(far[p, :, columns] * wide)
            stacked = jnp.concatenate([high, high, low], axis=0)
            out = jnp.dot(left_b[...], stacked, preferred_element_type=f32)
            high, low = halves(out)
            for m in range(2):
                at = pl.ds((2 * p + m) * det, det)
                for c in range(2):
                    part_h = high[c * det : (c + 1) * det, m * det : (m + 1) * det]
                    part_l = low[c * det : (c + 1) * det, m * det : (m + 1) * det]
                    deep[at, pl.ds(c * det, det)] = part_h
                    deep[at, pl.ds((2 + c) * det, det)] = part_h
                    deep[at, pl.ds((4 + c) * det, det)] = part_l
        some = pl.ds(0, 2 * count * det)
        half[some, :] = jnp.dot(deep[some, :], right_b[...], preferred_element_type=f32)
        for m in range(2):
            pr, pi = probe[q + m * groups, 0], probe[q + m * groups, 1]
            grad_re = jnp.zeros((det, det), f32)
            grad_im = jnp.zeros((det, det), f32)
            for p in range(count):
                at = pl.ds((2 * p + m) * det, det)
                cr, ci = half[at, :det], half[at, det:]
                patch_re, patch_im = patch[p, 0], patch[p, 1]
                grad_re = grad_re + patch_re * cr + patch_im * ci
                grad_im = grad_im + patch_re * ci - patch_im * cr
                num[p, 0] = num[p, 0] + (pr * cr + pi * ci)
                num[p, 1] = num[p, 1] + (pr * ci - pi * cr)
            packed[q, m, :, :, :, 0] = grad_re.reshape(spread_shape)
            packed[q, m, :, :, :, 1] = grad_im.reshape(spread_shape)
        return carry

    lax.fori_loop(0, groups, backward, 0)

    tile = mine[0]
    for i in range(1, 3):
        tile = tile * slab_sizes[i] + mine[i]
    strip = pl.ds(pl.multiple_of(tile * rows, rows), rows)
    own = Batch(full.at[(slice(None), core) + home])

    class Gather:
        def __init__(self, q):
            self.q, self.order = q, order_of(q)
            self.direct = q >= groups - 2
            self.view = full.at[q, core]
            if self.direct:
                self.batches = [Batch(land_all)]
            else:
                wholes = [self.view.at[home[:2] + (pl.ds(0, slab_sizes[2] - 1),)]]
                wholes += [self.view.at[spot_of(self.order, known)] for known in (2, 1)]
                self.batches = [Batch(whole) for whole in wholes]
            self.passing = Batch(land_all)

        def both(self, batch, spot, moves):
            batch.send(self.view.at[spot], self.view.at[spot], moves)

        def hand(self, known):
            for d in range(1, slab_sizes[self.order[known]]):
                self.both(self.passing, spot_of(self.order, known, d), [(core_dim, 1)])

        def send(self, step):
            known = 3 - step
            dim = slab_dims[self.order[known - 1]]
            for d in range(1, dim[2]):
                self.both(self.batches[step], spot_of(self.order, known), [(dim, d)])

        def begin(self):
            q = self.q
            for c in range(2):
                value = probe[core * groups + q, c, strip, :] + acc[(q,) + home + (c,)] * scale
                full[(q, core) + home + (c,)] = value
            self.both(own, home, [(core_dim, 1)])
            if self.direct:
                for slot in range(1, slab_count):
                    self.both(self.batches[0], home, list(zip(slab_dims, slab_coords(slot))))
            else:
                self.send(0)

        def got(self, step):
            self.batches[step].wait()
            if self.direct:
                for known in range(3):
                    self.hand(known)
                return
            if step < 2:
                self.send(step + 1)
            self.hand(2 - step)

    gathers = [Gather(q) for q in range(groups)]

    at_group(groups)
    for p in range(count):
        shift = place(p)[3]
        for c in range(2):
            pads[p, c, pad_at, :] = pltpu.roll(num[p, c], shift, 1)
    build_frame(frame_num, 2)
    num_fold = fold_copies(frame_num, num_slots)
    sums[5].swapped()
    sums[1].reduced(1)
    light_sum.reduced(2)
    scale = 1.0 / (r["acc_light"][home + (0,)] + probe_reg)
    sums[3].reduced(0)
    fold_start(num_fold, range(8))
    sums[2].reduced(1)
    sums[4].reduced(0)
    sums[0].reduced(2)
    gathers[0].begin()
    sums[3].reduced(1)
    sums[1].reduced(2)
    gathers[1].begin()
    sums[4].reduced(1)
    sums[2].reduced(2)
    gathers[2].begin()
    gathers[0].got(0)
    sums[3].reduced(2)
    gathers[3].begin()
    sums[5].reduced(0)
    gathers[5].begin()
    sums[4].reduced(2)
    gathers[4].begin()
    gathers[1].got(0)
    gathers[0].got(1)

    def slab_rows(spot):
        values = []
        for n in range(planes):
            c, k = n // modes, n % modes
            values.append(full[(k % groups, k // groups) + spot + (c,)])
        return jnp.concatenate(values, axis=0)

    tall = planes * rows
    up = lax.broadcasted_iota(jnp.int32, (tall, tall), 0)
    across = lax.broadcasted_iota(jnp.int32, (tall, tall), 1)
    same = jnp.where(((up - across) & (rows - 1)) == 0, 1.0, 0.0).astype(f32)
    plane = lax.broadcasted_iota(jnp.int32, (planes, tall), 0) * rows
    entry = lax.broadcasted_iota(jnp.int32, (planes, tall), 1)
    pick = jnp.where((entry >= plane) & (entry < plane + rows), 1.0, 0.0).astype(f32)
    plane = lax.broadcasted_iota(jnp.int32, (tall, det), 1) * rows
    entry = lax.broadcasted_iota(jnp.int32, (tall, det), 0)
    settled = jnp.where((entry >= plane) & (entry < plane + rows), 1.0, 0.0).astype(f32)

    own.wait()
    held = slab_rows(home)
    turned = jnp.concatenate([-held[tall // 2 :], held[: tall // 2]], axis=0)
    wide = jnp.concatenate([held, turned], axis=1)
    pairs = lax.dot_general(
        wide, wide, (((1,), (1,)), ((), ())), precision=highest, preferred_element_type=f32
    )
    gram = full_dot(full_dot(pick, pairs * same), settled)
    total_swap.wait()
    both = [jnp.sum(totals[i] + total_land[i]) for i in range(2)]
    sheet_lanes = lax.broadcasted_iota(jnp.int32, (8, det), 1)
    first = lax.broadcasted_iota(jnp.int32, (8, det), 0) == 0
    at_measured = first & (sheet_lanes == det - 2)
    at_modelled = first & (sheet_lanes == det - 1)
    sheet = jnp.where(at_measured, both[0], jnp.where(at_modelled, both[1], 0.0))
    for part in range(planes // 8):
        piece = gram[part * 8 : (part + 1) * 8]
        sheet = sheet + (pltpu.roll(piece, part * 32, 1) if part else piece)
    gram_out[...] = sheet
    spread = Batch(gram_land)
    for slot in range(1, slab_count):
        spread.send(gram_out, gram_land.at[slot - 1], list(zip(slab_dims, slab_coords(slot))))
    gathers[2].got(0)
    gathers[1].got(1)
    gathers[3].got(0)
    gathers[2].got(1)
    gathers[0].got(2)
    gathers[3].got(1)
    gathers[1].got(2)
    spread.wait()
    sheet = gram_out[...]
    for i in range(slab_count - 1):
        sheet = sheet + gram_land[i]
    for e, dim in enumerate(extra):
        gram_x[2 * e] = sheet
        item = remote(gram_x.at[2 * e], gram_x.at[2 * e + 1], [(dim, 1)])
        item.start()
        item.wait()
        sheet = sheet + gram_x[2 * e + 1]
    measured = jnp.sum(jnp.where(at_measured, sheet, 0.0))
    modelled = jnp.sum(jnp.where(at_modelled, sheet, 0.0))
    ratio = measured / (modelled + total_eps)
    parts = [sheet[:, part * 32 : part * 32 + planes] for part in range(planes // 8)]
    embedded = jnp.concatenate(parts, axis=0)
    eye = jnp.where(
        lax.broadcasted_iota(jnp.int32, (planes, planes), 0) == lax.broadcasted_iota(jnp.int32, (planes, planes), 1),
        1.0, 0.0,
    ).astype(f32)
    frobenius = jnp.sqrt(jnp.sum(embedded * embedded, keepdims=True))
    current = embedded / frobenius
    inverse = eye
    for repeat in range(NS_STEPS):
        scaled = 1.5 * eye - 0.5 * full_dot(inverse, current)
        current = full_dot(current, scaled)
        inverse = full_dot(scaled, inverse)
    weight = jnp.sqrt(ratio * jnp.sum(embedded * eye, axis=1, keepdims=True))
    mix = weight * (inverse / jnp.sqrt(frobenius))
    mix = lax.dot_general(
        pick, full_dot(mix, pick), (((0,), (0,)), ((), ())), precision=highest, preferred_element_type=f32
    )
    high, low = halves(mix * same)
    mixer = jnp.concatenate([high, low, high], axis=1)
    gathers[2].got(2)
    gathers[5].got(0)
    gathers[4].got(0)
    gathers[3].got(2)

    interior[0:2] = frame_num[:, det : det + block_rows, det : det + block_cols]
    interior[2] = frame_light[0, det : det + block_rows, det : det + block_cols]
    fold_end(light_fold, light_slots, slice(2, 3))
    fold_end(num_fold, num_slots, slice(0, 2))
    new_specimen[...] = specimen[...] + interior[0:2] / (interior[2] + object_reg)[None]

    for item in gathers:
        item.passing.wait()
    for t in range(0, slab_count, 2):
        sides = [slab_rows(slab_coords(s)) for s in (t, t + 1)]
        high, low = halves(jnp.concatenate(sides, axis=1))
        out = jnp.dot(mixer, jnp.concatenate([high, high, low], axis=0), preferred_element_type=f32)
        for n in range(planes):
            for s in range(2):
                new_probe[n % modes, n // modes, (t + s) * rows : (t + s + 1) * rows, :] = out[
                    n * rows : (n + 1) * rows, s * det : (s + 1) * det
                ]


def body(probe_modes, patterns, specimen, offsets):
    f32 = jnp.float32
    modes, _, det, _ = probe_modes.shape
    count = patterns.shape[0]
    block_rows, block_cols = specimen.shape[1:]
    col_blocks = block_cols // det + 2
    ext_rows = block_rows + 2 * det
    ext_cols = block_cols + 2 * det
    extra = extra_bits()
    more = max(len(extra), 1)
    rows = det // slab_count
    groups = modes // 2
    bf16 = jnp.bfloat16
    tables = [jnp.asarray(t) for t in dft_tables(det)]
    sems = 84 + (groups + 2) * len(extra)
    scratch = {
        "probe": pltpu.VMEM(probe_modes.shape, f32),
        "patterns": pltpu.VMEM(patterns.shape, f32),
        "specimen": pltpu.VMEM(specimen.shape, f32),
        **{f"table{n}": pltpu.VMEM(t.shape, bf16) for n, t in enumerate(tables)},
        "ext": pltpu.VMEM((2, col_blocks + 1, ext_rows, det), f32),
        "pads": pltpu.VMEM((count, 2, 2 * (ext_rows - det) + det, det), f32),
        "frame_num": pltpu.VMEM((2, ext_rows, ext_cols), f32),
        "frame_light": pltpu.VMEM((1, ext_rows, ext_cols), f32),
        "deep": pltpu.VMEM((modes * det, 6 * det), bf16),
        "half": pltpu.VMEM((modes * det, 2 * det), f32),
        "far": pltpu.VMEM((count, 2 * det, modes * det), f32),
        "patch": pltpu.VMEM((count, 2, det, det), f32),
        "factor": pltpu.VMEM((count, det, det), f32),
        "num": pltpu.VMEM((count, 2, det, det), f32),
        "power": pltpu.VMEM((det, det), f32),
        "light": pltpu.VMEM((det, det), f32),
        "totals": pltpu.VMEM((2, 8, det), f32),
        "total_land": pltpu.VMEM((2, 8, det), f32),
        "gram_out": pltpu.VMEM((8, det), f32),
        "gram_land": pltpu.VMEM((slab_count - 1, 8, det), f32),
        "gram_x": pltpu.VMEM((2 * more, 8, det), f32),
        "interior": pltpu.VMEM((3, block_rows, block_cols), f32),
        "send_sem": pltpu.SemaphoreType.DMA((sems,)),
        "recv_sem": pltpu.SemaphoreType.DMA((sems,)),
        "local_sem": pltpu.SemaphoreType.DMA((16,)),
    }
    for end, lead, planes in (("", (groups,), 2), ("_light", (), 1)):
        tile = (planes, rows, det)
        scratch["packed" + end] = pltpu.VMEM(lead + (2,) + slab_sizes + tile, f32)
        scratch["land0" + end] = pltpu.VMEM(lead + slab_sizes + tile, f32)
        scratch["acc" + end] = pltpu.VMEM(lead + slab_sizes + tile, f32)
        scratch["land1" + end] = pltpu.VMEM(lead + (1, 2, slab_sizes[2]) + tile, f32)
        scratch["land2" + end] = pltpu.VMEM(lead + (1, slab_sizes[2]) + tile, f32)
        scratch["land3" + end] = pltpu.VMEM(lead + (slab_sizes[2] - 1,) + tile, f32)
        scratch["landx" + end] = pltpu.VMEM(lead + (more,) + tile, f32)
    scratch["land_all"] = pltpu.VMEM((slab_count - 1, 2, rows, det), f32)
    scratch["full"] = pltpu.VMEM((groups, 2) + slab_sizes + (2, rows, det), f32)
    for index, (i, j) in enumerate(directions()):
        shape = (det if i else block_rows, det if j else block_cols)
        scratch[f"num_slot{index}"] = pltpu.VMEM((2,) + shape, f32)
        scratch[f"light_slot{index}"] = pltpu.VMEM((1,) + shape, f32)
    names = ["offs", "probe_in", "patterns_in", "specimen_in"]
    names += [f"table_in{n}" for n in range(4)] + ["new_probe", "new_specimen"] + list(scratch)

    def kernel(*refs):
        update_kernel(extra, names, *refs)

    vmem = pl.BlockSpec(memory_space=pltpu.VMEM)
    return pl.pallas_call(
        kernel,
        name="update",
        out_shape=(
            jax.ShapeDtypeStruct(probe_modes.shape, f32),
            jax.ShapeDtypeStruct(specimen.shape, f32),
        ),
        in_specs=[pl.BlockSpec(memory_space=pltpu.SMEM)] + [pl.BlockSpec(memory_space=pl.ANY)] * 7,
        out_specs=(vmem, vmem),
        scratch_shapes=list(scratch.values()),
        compiler_params=pltpu.CompilerParams(has_side_effects=True, vmem_limit_bytes=56 * 1024 * 1024),
    )(offsets.T, probe_modes, patterns, specimen, *tables)


def solution(mesh):
    return jax.shard_map(
        body,
        mesh=mesh,
        in_specs=(
            P(),
            P(("scan", "tile"), None, None),
            P(None, "scan", "tile"),
            P(("scan", "tile"), None),
        ),
        out_specs=(P(), P(None, "scan", "tile")),
        check_vma=False,
    )
```

```python
import math

import jax
import jax.numpy as jnp
import numpy as np
from jax import lax
from jax.experimental import pallas as pl
from jax.experimental.pallas import tpu as pltpu
from jax.sharding import PartitionSpec as P

NS_STEPS = 8


highest = lax.Precision.HIGHEST
light_floor = 0.05
object_reg = 0.5
probe_reg = 1.0
total_eps = 1e-06


def dft_tables(detector):
    indices = np.arange(detector, dtype=np.int64)
    angles = -2.0 * np.pi / detector * (indices[:, None] * indices[None, :] % detector)
    table_re = np.cos(angles) / np.sqrt(detector)
    table_im = np.sin(angles) / np.sqrt(detector)
    right = np.block([[table_re, table_im], [-table_im, table_re]]).astype(np.float32)
    left = np.ascontiguousarray(right.T)
    parts = []
    for table in (right, left):
        high = table.astype(jnp.bfloat16)
        low = (table - high.astype(np.float32)).astype(jnp.bfloat16)
        parts.append((high, low))
    (rh, rl), (lh, ll) = parts
    return (
        np.concatenate([rh, rl, rh], axis=0),
        np.concatenate([lh, ll, lh], axis=1),
        np.concatenate([rh, rl, rh], axis=1),
        np.concatenate([lh, ll, lh], axis=0),
    )


def halves(value):
    high = value.astype(jnp.bfloat16)
    low = (value - high.astype(jnp.float32)).astype(jnp.bfloat16)
    return high, low


core_dim = ("scan", 1, 2)
slab_dims = (("scan", 2, 2), ("tile", 1, 2), ("scan", 4, 4))
slab_sizes = tuple(size for _, _, size in slab_dims)
slab_count = math.prod(slab_sizes)


def extra_bits():
    bits = []
    for axis, bit in (("scan", 16), ("tile", 2)):
        while bit < lax.axis_size(axis):
            bits.append((axis, bit, 2))
            bit *= 2
    return bits


def slab_coords(tile):
    coords = []
    for size in reversed(slab_sizes):
        coords.append(tile % size)
        tile = tile // size
    return tuple(coords[::-1])


def directions():
    return [(i, j) for i, j in ((1, 0), (-1, 0), (0, 1), (0, -1), (1, 1), (1, -1), (-1, 1), (-1, -1))]


def digit(dim):
    axis, bit, size = dim
    return (lax.axis_index(axis) // bit) % size


def flipped(value, size, d):
    if size == 2:
        return 1 - value if d else value
    low, high = value % 2, value // 2
    low = 1 - low if d % 2 else low
    high = 1 - high if d // 2 else high
    return low + 2 * high


def peer(moves):
    where = {}
    for dim, d in moves:
        axis, bit, size = dim
        here = digit(dim)
        base = where.get(axis, lax.axis_index(axis))
        where[axis] = base + bit * (flipped(here, size, d) - here)
    return where


def full_dot(a, b):
    return jnp.dot(a, b, precision=highest, preferred_element_type=jnp.float32)


def zeros_into(ref):
    ref[...] = jnp.zeros(ref.shape, ref.dtype)


def update_kernel(extra, names, *refs):
    f32 = jnp.float32
    r = dict(zip(names, refs))
    offs, probe_in, patterns_in, specimen_in = r["offs"], r["probe_in"], r["patterns_in"], r["specimen_in"]
    new_probe, new_specimen = r["new_probe"], r["new_specimen"]
    probe, patterns, specimen, tables = r["probe"], r["patterns"], r["specimen"], [r[f"table{n}"] for n in range(4)]
    ext, pads, frame_num, frame_light = r["ext"], r["pads"], r["frame_num"], r["frame_light"]
    deep, half, far, patch, factor, num = r["deep"], r["half"], r["far"], r["patch"], r["factor"], r["num"]
    power, light, totals, total_land = r["power"], r["light"], r["totals"], r["total_land"]
    packed, land0, acc, full = r["packed"], r["land0"], r["acc"], r["full"]
    land1, land2, landx, land_all = r["land1"], r["land2"], r["landx"], r["land_all"]
    num_slots = [r[f"num_slot{i}"] for i in range(8)]
    light_slots = [r[f"light_slot{i}"] for i in range(8)]
    gram_out, gram_land, gram_x, interior = r["gram_out"], r["gram_land"], r["gram_x"], r["interior"]
    send_sem, recv_sem, local_sem = r["send_sem"], r["recv_sem"], r["local_sem"]
    right_f, left_f, left_b, right_b = tables

    modes, det = probe.shape[0], probe.shape[-1]
    count = patterns.shape[0]
    block_rows, block_cols = specimen.shape[1:]
    own_blocks = block_cols // det
    col_blocks = own_blocks + 2
    ext_rows = block_rows + 2 * det
    groups = modes // 2
    direct_sums = (groups - 1,)
    direct_gathers = (groups - 1,)
    fold_pieces = 2
    rows = det // slab_count
    planes = 2 * modes
    used = [0]

    here = {axis: lax.axis_index(axis) for axis in ("scan", "tile")}
    sizes = {axis: lax.axis_size(axis) for axis in ("scan", "tile")}

    def route(src, dst, device):
        n = used[0]
        used[0] += 1
        return pltpu.make_async_remote_copy(
            src_ref=src, dst_ref=dst, send_sem=send_sem.at[n], recv_sem=recv_sem.at[n],
            device_id=device, device_id_type=pl.DeviceIdType.MESH,
        )

    def remote(src, dst, moves):
        return route(src, dst, peer(moves))

    class Batch:
        def __init__(self, whole):
            self.whole = whole
            self.n = used[0]
            used[0] += 1

        def make(self, src, dst, device):
            return pltpu.make_async_remote_copy(
                src_ref=src, dst_ref=dst, send_sem=send_sem.at[self.n], recv_sem=recv_sem.at[self.n],
                device_id=device, device_id_type=pl.DeviceIdType.MESH,
            )

        def send(self, src, dst, moves):
            self.make(src, dst, peer(moves)).start()

        def wait(self):
            self.make(self.whole, self.whole, peer([(core_dim, 1)])).wait()

    def shifted(i, j):
        return {
            "scan": (here["scan"] + i + sizes["scan"]) % sizes["scan"],
            "tile": (here["tile"] + j + sizes["tile"]) % sizes["tile"],
        }

    def valid(i, j):
        row, col = here["scan"] + i, here["tile"] + j
        return (row >= 0) & (row < sizes["scan"]) & (col >= 0) & (col < sizes["tile"])

    def launch(copies):
        for item in copies:
            item.start()
        return copies

    def settle(copies):
        for item in copies:
            item.wait()

    core = digit(core_dim)
    mine = [digit(dim) for dim in slab_dims]

    off_shift, on_shift = 2 * core - 1, 1 - 2 * core

    def outer_rows(i):
        return pl.ds(pl.multiple_of((1 - i) // 2 * (det + block_rows), 8), det)

    def edge_rows(i, base):
        return pl.ds(pl.multiple_of(base + (1 + i) // 2 * (block_rows - det), 8), det)

    def edge_block(j):
        return own_blocks - 1 if j == 1 else 0

    def outer_block(j):
        return 0 if j == 1 else own_blocks + 1

    off_valid = valid(off_shift, 0)
    right_valid, left_valid = valid(0, 1), valid(0, -1)
    near = jnp.where(right_valid, own_blocks - 1, 0)
    distant = own_blocks - 1 - near
    inner_blocks = list(range(1, own_blocks - 1))
    local = []

    def load(src, dst):
        item = pltpu.make_async_copy(src, dst, local_sem.at[len(local)])
        item.start()
        local.append(item)
        return item

    def row_copy(i, b, c, channels):
        channel = pl.ds(c, channels)
        return route(
            specimen_in.at[channel, edge_rows(i, 0), pl.ds(pl.multiple_of(b * det, det), det)],
            ext.at[channel, 1 + b, outer_rows(i), :],
            shifted(i, 0),
        )

    near_rows = [row_copy(off_shift, near, c, 1) for c in range(2)]
    rest = [distant] * (own_blocks > 1) + inner_blocks
    off_rows = [row_copy(off_shift, b, 0, 2) for b in rest]
    on_rows = [row_copy(on_shift, b, 0, 2) for b in range(own_blocks)]

    @pl.when(off_valid)
    def _():
        launch(near_rows)

    side = {}
    for j in (1, -1):
        b = edge_block(j)
        side[j] = route(
            specimen_in.at[:, :, b * det : (b + 1) * det],
            ext.at[:, outer_block(j), pl.ds(det, block_rows), :],
            shifted(0, j),
        )

        @pl.when(valid(0, j))
        def _():
            side[j].start()

    launch(on_rows)
    @pl.when(off_valid)
    def _():
        launch(off_rows)

    probe_load = load(probe_in, probe)
    own_load = [
        load(specimen_in.at[:, :, b * det : (b + 1) * det], ext.at[:, 1 + b, pl.ds(det, block_rows), :])
        for b in range(own_blocks)
    ]
    other_loads = [load(patterns_in, patterns), load(specimen_in, specimen)]
    for n in range(4):
        other_loads.append(load(r[f"table_in{n}"], tables[n]))

    blank = jnp.zeros((2, det, det), f32)
    zeros_into(ext.at[:, col_blocks])

    @pl.when(jnp.logical_not(off_valid))
    def _():
        for b in range(col_blocks):
            ext[:, b, outer_rows(-off_shift), :] = blank

    for j in (1, -1):
        @pl.when(jnp.logical_not(valid(0, -j)))
        def _():
            ext[:, outer_block(j), pl.ds(det, block_rows), :] = jnp.zeros((2, block_rows, det), f32)
            ext[:, outer_block(j), outer_rows(1), :] = blank
            ext[:, outer_block(j), outer_rows(-1), :] = blank

    zeros_into(pads)
    zeros_into(num)
    zeros_into(light)

    lanes = lax.broadcasted_iota(jnp.int32, (det, det), 1)
    row_base = here["scan"] * block_rows - det
    col_base = here["tile"] * block_cols - det

    def place(p):
        row = jnp.clip(offs[0, p] - row_base, 0, block_rows + det)
        col = jnp.clip(offs[1, p] - col_base, 0, block_cols + det)
        block = col // det
        return row, col, block, col - block * det

    def build_frame(frame, channels):
        chunk = 64
        strip_lanes = lax.broadcasted_iota(jnp.int32, (chunk, det), 1)

        def some(n, carry):
            base = pl.multiple_of(n * chunk, chunk)
            for c in range(channels):
                values = [jnp.zeros((chunk, det), f32) for _ in range(col_blocks)]
                for p in range(count):
                    row, col, _, _ = place(p)
                    piece = pads[p, c, pl.ds(ext_rows - det - row + base, chunk), :]
                    for j in range(col_blocks):
                        at = strip_lanes + (j * det - col)
                        values[j] = values[j] + jnp.where((at >= 0) & (at < det), piece, 0.0)
                for j in range(col_blocks):
                    frame[c, pl.ds(base, chunk), j * det : (j + 1) * det] = values[j]
            return carry

        lax.fori_loop(0, ext_rows // chunk, some, 0)

    pad_at = pl.ds(ext_rows - det, det)
    probe_load.wait()
    value = jnp.zeros((det, det), f32)
    for k in range(modes):
        value = value + probe[k, 0] * probe[k, 0] + probe[k, 1] * probe[k, 1]
    power[...] = value
    for p in range(count):
        pads[p, 0, pad_at, :] = pltpu.roll(power[...], place(p)[3], 1)
    build_frame(frame_light, 1)

    def corner(j, c):
        channel = pl.ds(c, 1)
        return route(
            ext.at[channel, 1 + edge_block(j), outer_rows(-off_shift), :],
            ext.at[channel, outer_block(j), outer_rows(-off_shift), :],
            shifted(0, j),
        )

    relay = []
    corners = {j: [corner(j, c) for c in range(2)] for j in (1, -1)}
    for j in (1, -1):
        relay += [(item, off_valid & valid(0, j), off_valid & valid(0, -j)) for item in corners[j]]
    for c in range(2):
        @pl.when(off_valid)
        def _():
            near_rows[c].wait()

        @pl.when(off_valid & right_valid)
        def _():
            corners[1][c].start()

        @pl.when(off_valid & left_valid & jnp.logical_not(right_valid))
        def _():
            corners[-1][c].start()

    for j in (1, -1):
        @pl.when(valid(0, j))
        def _():
            side[j].wait_send()

        item = route(
            ext.at[:, outer_block(j), edge_rows(on_shift, det), :],
            ext.at[:, outer_block(j), outer_rows(on_shift), :],
            shifted(on_shift, 0),
        )
        relay.append((item, valid(0, -j), valid(0, -j)))

        @pl.when(valid(0, -j))
        def _():
            side[j].wait_recv()
            item.start()

    settle(on_rows)

    @pl.when(off_valid)
    def _():
        settle(off_rows)

    @pl.when(off_valid & left_valid & right_valid)
    def _():
        launch(corners[-1])

    for item, sent, came in relay:
        @pl.when(sent)
        def _():
            item.wait_send()

        @pl.when(came)
        def _():
            item.wait_recv()
    for item in own_load + other_loads:
        item.wait()

    def span(shift, block):
        low = {-1: 0, 0: det, 1: det + block}[shift]
        return pl.ds(low, block if shift == 0 else det)

    def inner(shift, block):
        low = {-1: block - det, 0: 0, 1: 0}[shift]
        return pl.ds(low, block if shift == 0 else det)

    class Fold:
        def __init__(self, frame, slots, first):
            self.slots, self.first = slots, first
            self.batches = [Batch(slot) for slot in slots]
            self.pending = []
            channels = frame.shape[0]
            for index in (0, 1, 4, 5, 6, 7, 2, 3):
                i, j = directions()[index]
                height = det if i else block_rows
                low = span(i, block_rows).start
                pieces = fold_pieces if j == 0 else 1
                for c in range(channels):
                    for n in range(pieces):
                        size = height // pieces
                        source = frame.at[pl.ds(c, 1), pl.ds(low + n * size, size), span(j, block_cols)]
                        target = slots[index].at[pl.ds(c, 1), pl.ds(n * size, size)]
                        self.pending.append((index, source, target))

        def some(self, n):
            for index, source, target in self.pending[:n]:
                i, j = directions()[index]

                @pl.when(valid(i, j))
                def _():
                    self.batches[index].make(source, target, shifted(i, j)).start()
            self.pending = self.pending[n:]

        def end(self):
            into = slice(self.first, self.first + self.slots[0].shape[0])
            for index, (i, j) in enumerate(directions()):
                item = self.batches[index].make(self.slots[index], self.slots[index], shifted(i, j))

                @pl.when(valid(i, j))
                def _():
                    item.wait_send()

                @pl.when(valid(-i, -j))
                def _():
                    item.wait_recv()
                    a, b = inner(i, block_rows), inner(j, block_cols)
                    interior[into, a, b] = interior[into, a, b] + self.slots[index][...]

    light_fold = Fold(frame_light, light_slots, 2)
    light_fold.some(100)

    total = jnp.zeros((det, det), f32)
    for p in range(count):
        row, _, block, shift = place(p)
        back = lax.rem(det - shift, det)
        for c in range(2):
            first = pltpu.roll(ext[c, block, pl.ds(row, det), :], back, 1)
            second = pltpu.roll(ext[c, block + 1, pl.ds(row, det), :], back, 1)
            patch[p, c] = jnp.where(lanes < det - shift, first, second)
        patch_light = patch[p, 0] * patch[p, 0] + patch[p, 1] * patch[p, 1]
        light[...] = light[...] + patch_light
        total = total + patch_light * power[...]
        factor[p] = jnp.zeros((det, det), f32)
    some = pl.ds(0, 2 * count * det)

    def forward(q, carry):
        columns = pl.ds(pl.multiple_of(q * 2 * det, 2 * det), 2 * det)
        for p in range(count):
            patch_re, patch_im = patch[p, 0], patch[p, 1]
            for m in range(2):
                at = pl.ds((2 * p + m) * det, det)
                pr, pi = probe[q + m * groups, 0], probe[q + m * groups, 1]
                for c, value in enumerate((pr * patch_re - pi * patch_im, pr * patch_im + pi * patch_re)):
                    high, low = halves(value)
                    deep[at, pl.ds(c * det, det)] = high
                    deep[at, pl.ds((2 + c) * det, det)] = high
                    deep[at, pl.ds((4 + c) * det, det)] = low
        half[some, :] = jnp.dot(deep[some, :], right_f[...], preferred_element_type=f32)
        for p in range(count):
            first, second = [half[pl.ds((2 * p + m) * det, det), :] for m in range(2)]
            paired = jnp.concatenate(
                [
                    jnp.concatenate([first[:, :det], second[:, :det]], axis=1),
                    jnp.concatenate([first[:, det:], second[:, det:]], axis=1),
                ],
                axis=0,
            )
            high, low = halves(paired)
            stacked = jnp.concatenate([high, high, low], axis=0)
            out = jnp.dot(left_f[...], stacked, preferred_element_type=f32)
            far[p, :, columns] = out
            squares = out * out
            both = squares[:det] + squares[det:]
            factor[p] = factor[p] + (both[:, :det] + both[:, det:])
        return carry

    lax.fori_loop(0, groups, forward, 0)
    for p in range(count):
        factor[p] = jnp.sqrt(patterns[p]) / jnp.sqrt(jnp.maximum(factor[p], light_floor)) - 1.0
    measured = jnp.zeros((det, det), f32)
    for p in range(count):
        measured = measured + patterns[p]
    totals[0] = jnp.sum(measured.reshape(det // 8, 8, det), axis=0)
    totals[1] = jnp.sum(total.reshape(det // 8, 8, det), axis=0)
    spread_shape = slab_sizes + (rows, det)
    for h in range(2):
        r["packed_light"][h, :, :, :, 0] = light[...].reshape(spread_shape)

    home = tuple(mine)

    def flips_of(stage):
        flips = [()]
        for i in range(3):
            flips = [f + (d,) for f in flips for d in range(slab_sizes[i] if i in stage else 1)]
        return flips[1:]

    def spot_of(known, flips=(0, 0, 0)):
        return tuple(flipped(mine[i], slab_sizes[i], flips[i]) if i in known else slice(None) for i in range(3))

    def moves_of(flips):
        return list(zip(slab_dims, flips))

    two_steps, one_step = ((0, 1), (2,)), ((0, 1, 2),)

    class Sum:
        def __init__(self, stages, source, land0, acc, lands, landx):
            self.stages, self.source, self.acc = stages, source, acc
            self.land0, self.lands, self.landx = land0, lands, landx
            self.swap = remote(source.at[1 - core], land0, [(core_dim, 1)])
            self.batches = [Batch(land) for land in lands]

        def known(self, step):
            return [i for stage in self.stages[: step + 1] for i in stage]

        def send(self, step):
            for n, flips in enumerate(flips_of(self.stages[step])):
                source = self.acc.at[spot_of(self.known(step), flips)]
                self.batches[step].send(source, self.lands[step].at[n], moves_of(flips))

        def swapped(self):
            self.swap.wait()
            self.acc[...] = self.source[core] + self.land0[...]
            self.send(0)

        def reduced(self, step):
            self.batches[step].wait()
            land = self.lands[step]
            spot = spot_of(self.known(step))
            value = self.acc[spot]
            for d in range(land.shape[0]):
                value = value + land[d]
            self.acc[spot] = value
            if step < len(self.lands) - 1:
                self.send(step + 1)
                return
            for e, dim in enumerate(extra):
                item = remote(self.acc.at[home], self.landx.at[e], [(dim, 1)])
                item.start()
                item.wait()
                self.acc[home] = self.acc[home] + self.landx[e]

    light_sum = Sum(
        two_steps, r["packed_light"], r["land0_light"], r["acc_light"],
        [r["land1_light"], r["land2_light"]], r["landx_light"],
    )
    sums = []
    for q in range(groups):
        direct = q in direct_sums
        sums.append(
            Sum(
                one_step if direct else two_steps, packed.at[q], land0.at[q], acc.at[q],
                [land_all.at[q]] if direct else [land1.at[q], land2.at[q]], landx.at[q],
            )
        )
    total_swap = remote(totals, total_land, [(core_dim, 1)])

    def at_group(n):
        if n == 0:
            light_sum.swap.start()
            total_swap.start()
            return
        sums[n - 1].swap.start()
        if n == 2:
            light_sum.swapped()
        if n >= 3:
            sums[n - 3].swapped()

    def backward(q, carry):
        for n in range(groups):
            @pl.when(q == n)
            def _():
                at_group(n)

        columns = pl.ds(pl.multiple_of(q * 2 * det, 2 * det), 2 * det)
        for p in range(count):
            wide = jnp.concatenate([factor[p], factor[p]], axis=1)
            wide = jnp.concatenate([wide, wide], axis=0)
            high, low = halves(far[p, :, columns] * wide)
            stacked = jnp.concatenate([high, high, low], axis=0)
            out = jnp.dot(left_b[...], stacked, preferred_element_type=f32)
            high, low = halves(out)
            for m in range(2):
                at = pl.ds((2 * p + m) * det, det)
                for c in range(2):
                    part_h = high[c * det : (c + 1) * det, m * det : (m + 1) * det]
                    part_l = low[c * det : (c + 1) * det, m * det : (m + 1) * det]
                    deep[at, pl.ds(c * det, det)] = part_h
                    deep[at, pl.ds((2 + c) * det, det)] = part_h
                    deep[at, pl.ds((4 + c) * det, det)] = part_l
        half[some, :] = jnp.dot(deep[some, :], right_b[...], preferred_element_type=f32)
        for m in range(2):
            pr, pi = probe[q + m * groups, 0], probe[q + m * groups, 1]
            grad_re = jnp.zeros((det, det), f32)
            grad_im = jnp.zeros((det, det), f32)
            for p in range(count):
                at = pl.ds((2 * p + m) * det, det)
                cr, ci = half[at, :det], half[at, det:]
                patch_re, patch_im = patch[p, 0], patch[p, 1]
                grad_re = grad_re + patch_re * cr + patch_im * ci
                grad_im = grad_im + patch_re * ci - patch_im * cr
                num[p, 0] = num[p, 0] + (pr * cr + pi * ci)
                num[p, 1] = num[p, 1] + (pr * ci - pi * cr)
            packed[q, m, :, :, :, 0] = grad_re.reshape(spread_shape)
            packed[q, m, :, :, :, 1] = grad_im.reshape(spread_shape)
        return carry

    lax.fori_loop(0, groups, backward, 0)

    tile = mine[0]
    for i in range(1, 3):
        tile = tile * slab_sizes[i] + mine[i]
    strip = pl.ds(pl.multiple_of(tile * rows, rows), rows)
    own = Batch(full.at[(slice(None), core) + home])

    class Gather:
        def __init__(self, q):
            self.q = q
            self.view = full.at[q, core]
            if q in direct_gathers:
                self.stages = one_step
                self.batches = [Batch(land_all.at[0])]
            else:
                self.stages = two_steps[::-1]
                self.batches = [Batch(land2.at[0]), Batch(land1.at[0])]
            self.passing = Batch(land_all.at[0])

        def both(self, batch, spot, moves):
            batch.send(self.view.at[spot], self.view.at[spot], moves)

        def left(self, step):
            return [i for stage in self.stages[step:] for i in stage]

        def send(self, step):
            for flips in flips_of(self.stages[step]):
                self.both(self.batches[step], spot_of(self.left(step)), moves_of(flips))

        def begin(self):
            q = self.q
            for c in range(2):
                value = probe[core * groups + q, c, strip, :] + acc[(q,) + home + (c,)] * scale
                full[(q, core) + home + (c,)] = value
            self.both(own, home, [(core_dim, 1)])
            self.send(0)

        def got(self, step):
            self.batches[step].wait()
            if step < len(self.stages) - 1:
                self.send(step + 1)
            for flips in flips_of(self.stages[step]):
                self.both(self.passing, spot_of(self.left(step), flips), [(core_dim, 1)])

    gathers = [Gather(q) for q in range(groups)]

    at_group(groups)
    for p in range(count):
        shift = place(p)[3]
        for c in range(2):
            pads[p, c, pad_at, :] = pltpu.roll(num[p, c], shift, 1)
    build_frame(frame_num, 2)
    sums[groups - 2].swapped()
    sums[groups - 1].swapped()
    light_sum.reduced(0)
    num_fold = Fold(frame_num, num_slots, 0)
    for q in range(groups - 1):
        sums[q].reduced(0)
        num_fold.some(2)
    light_sum.reduced(1)
    scale = 1.0 / (r["acc_light"][home + (0,)] + probe_reg)
    for q in range(groups):
        if q not in direct_sums:
            sums[q].reduced(1)
            gathers[q].begin()
            num_fold.some(2)
    sums[groups - 1].reduced(0)
    gathers[groups - 1].begin()
    num_fold.some(2)

    def slab_rows(spot):
        values = []
        for n in range(planes):
            c, k = n // modes, n % modes
            values.append(full[(k % groups, k // groups) + spot + (c,)])
        return jnp.concatenate(values, axis=0)

    tall = planes * rows
    up = lax.broadcasted_iota(jnp.int32, (tall, tall), 0)
    across = lax.broadcasted_iota(jnp.int32, (tall, tall), 1)
    same = jnp.where(((up - across) & (rows - 1)) == 0, 1.0, 0.0).astype(f32)
    plane = lax.broadcasted_iota(jnp.int32, (planes, tall), 0) * rows
    entry = lax.broadcasted_iota(jnp.int32, (planes, tall), 1)
    pick = jnp.where((entry >= plane) & (entry < plane + rows), 1.0, 0.0).astype(f32)
    plane = lax.broadcasted_iota(jnp.int32, (tall, det), 1) * rows
    entry = lax.broadcasted_iota(jnp.int32, (tall, det), 0)
    settled = jnp.where((entry >= plane) & (entry < plane + rows), 1.0, 0.0).astype(f32)

    own.wait()
    held = slab_rows(home)
    turned = jnp.concatenate([-held[tall // 2 :], held[: tall // 2]], axis=0)
    wide = jnp.concatenate([held, turned], axis=1)
    pairs = lax.dot_general(
        wide, wide, (((1,), (1,)), ((), ())), precision=highest, preferred_element_type=f32
    )
    gram = full_dot(full_dot(pick, pairs * same), settled)
    total_swap.wait()
    both = [jnp.sum(totals[i] + total_land[i]) for i in range(2)]
    sheet_lanes = lax.broadcasted_iota(jnp.int32, (8, det), 1)
    first = lax.broadcasted_iota(jnp.int32, (8, det), 0) == 0
    at_measured = first & (sheet_lanes == det - 2)
    at_modelled = first & (sheet_lanes == det - 1)
    sheet = jnp.where(at_measured, both[0], jnp.where(at_modelled, both[1], 0.0))
    for part in range(planes // 8):
        piece = gram[part * 8 : (part + 1) * 8]
        sheet = sheet + (pltpu.roll(piece, part * 32, 1) if part else piece)
    gram_out[...] = sheet
    spread = Batch(gram_land)
    for slot in range(1, slab_count):
        spread.send(gram_out, gram_land.at[slot - 1], list(zip(slab_dims, slab_coords(slot))))
    for q in range(groups):
        if q not in direct_gathers:
            gathers[q].got(0)
            num_fold.some(2)
    num_fold.some(100)
    spread.wait()
    sheet = gram_out[...]
    for i in range(slab_count - 1):
        sheet = sheet + gram_land[i]
    for e, dim in enumerate(extra):
        gram_x[2 * e] = sheet
        item = remote(gram_x.at[2 * e], gram_x.at[2 * e + 1], [(dim, 1)])
        item.start()
        item.wait()
        sheet = sheet + gram_x[2 * e + 1]
    measured = jnp.sum(jnp.where(at_measured, sheet, 0.0))
    modelled = jnp.sum(jnp.where(at_modelled, sheet, 0.0))
    ratio = measured / (modelled + total_eps)
    parts = [sheet[:, part * 32 : part * 32 + planes] for part in range(planes // 8)]
    embedded = jnp.concatenate(parts, axis=0)
    eye = jnp.where(
        lax.broadcasted_iota(jnp.int32, (planes, planes), 0) == lax.broadcasted_iota(jnp.int32, (planes, planes), 1),
        1.0, 0.0,
    ).astype(f32)
    frobenius = jnp.sqrt(jnp.sum(embedded * embedded, keepdims=True))
    current = embedded / frobenius
    inverse = eye
    for repeat in range(NS_STEPS):
        scaled = 1.5 * eye - 0.5 * full_dot(inverse, current)
        current = full_dot(current, scaled)
        inverse = full_dot(scaled, inverse)
    weight = jnp.sqrt(ratio * jnp.sum(embedded * eye, axis=1, keepdims=True))
    mix = weight * (inverse / jnp.sqrt(frobenius))
    mix = lax.dot_general(
        pick, full_dot(mix, pick), (((0,), (0,)), ((), ())), precision=highest, preferred_element_type=f32
    )
    high, low = halves(mix * same)
    mixer = jnp.concatenate([high, low, high], axis=1)
    for q in range(groups):
        gathers[q].got(0 if q in direct_gathers else 1)

    interior[0:2] = frame_num[:, det : det + block_rows, det : det + block_cols]
    interior[2] = frame_light[0, det : det + block_rows, det : det + block_cols]
    light_fold.end()
    num_fold.end()
    new_specimen[...] = specimen[...] + interior[0:2] / (interior[2] + object_reg)[None]

    for item in gathers:
        item.passing.wait()
    for t in range(0, slab_count, 2):
        sides = [slab_rows(slab_coords(s)) for s in (t, t + 1)]
        high, low = halves(jnp.concatenate(sides, axis=1))
        out = jnp.dot(mixer, jnp.concatenate([high, high, low], axis=0), preferred_element_type=f32)
        for n in range(planes):
            for s in range(2):
                new_probe[n % modes, n // modes, (t + s) * rows : (t + s + 1) * rows, :] = out[
                    n * rows : (n + 1) * rows, s * det : (s + 1) * det
                ]


def body(probe_modes, patterns, specimen, offsets):
    f32 = jnp.float32
    modes, _, det, _ = probe_modes.shape
    count = patterns.shape[0]
    block_rows, block_cols = specimen.shape[1:]
    col_blocks = block_cols // det + 2
    ext_rows = block_rows + 2 * det
    ext_cols = block_cols + 2 * det
    extra = extra_bits()
    more = max(len(extra), 1)
    rows = det // slab_count
    groups = modes // 2
    bf16 = jnp.bfloat16
    tables = [jnp.asarray(t) for t in dft_tables(det)]
    sems = 84 + (groups + 2) * len(extra)
    scratch = {
        "probe": pltpu.VMEM(probe_modes.shape, f32),
        "patterns": pltpu.VMEM(patterns.shape, f32),
        "specimen": pltpu.VMEM(specimen.shape, f32),
        **{f"table{n}": pltpu.VMEM(t.shape, bf16) for n, t in enumerate(tables)},
        "ext": pltpu.VMEM((2, col_blocks + 1, ext_rows, det), f32),
        "pads": pltpu.VMEM((count, 2, 2 * (ext_rows - det) + det, det), f32),
        "frame_num": pltpu.VMEM((2, ext_rows, ext_cols), f32),
        "frame_light": pltpu.VMEM((1, ext_rows, ext_cols), f32),
        "deep": pltpu.VMEM((2 * count * det, 6 * det), bf16),
        "half": pltpu.VMEM((2 * count * det, 2 * det), f32),
        "far": pltpu.VMEM((count, 2 * det, modes * det), f32),
        "patch": pltpu.VMEM((count, 2, det, det), f32),
        "factor": pltpu.VMEM((count, det, det), f32),
        "num": pltpu.VMEM((count, 2, det, det), f32),
        "power": pltpu.VMEM((det, det), f32),
        "light": pltpu.VMEM((det, det), f32),
        "totals": pltpu.VMEM((2, 8, det), f32),
        "total_land": pltpu.VMEM((2, 8, det), f32),
        "gram_out": pltpu.VMEM((8, det), f32),
        "gram_land": pltpu.VMEM((slab_count - 1, 8, det), f32),
        "gram_x": pltpu.VMEM((2 * more, 8, det), f32),
        "interior": pltpu.VMEM((3, block_rows, block_cols), f32),
        "send_sem": pltpu.SemaphoreType.DMA((sems,)),
        "recv_sem": pltpu.SemaphoreType.DMA((sems,)),
        "local_sem": pltpu.SemaphoreType.DMA((16,)),
    }
    for end, lead, planes in (("", (groups,), 2), ("_light", (), 1)):
        tile = (planes, rows, det)
        scratch["packed" + end] = pltpu.VMEM(lead + (2,) + slab_sizes + tile, f32)
        scratch["land0" + end] = pltpu.VMEM(lead + slab_sizes + tile, f32)
        scratch["acc" + end] = pltpu.VMEM(lead + slab_sizes + tile, f32)
        scratch["land1" + end] = pltpu.VMEM(lead + (slab_sizes[0] * slab_sizes[1] - 1, slab_sizes[2]) + tile, f32)
        scratch["land2" + end] = pltpu.VMEM(lead + (slab_sizes[2] - 1,) + tile, f32)
        scratch["landx" + end] = pltpu.VMEM(lead + (more,) + tile, f32)
    scratch["land_all"] = pltpu.VMEM((groups, slab_count - 1, 2, rows, det), f32)
    scratch["full"] = pltpu.VMEM((groups, 2) + slab_sizes + (2, rows, det), f32)
    for index, (i, j) in enumerate(directions()):
        shape = (det if i else block_rows, det if j else block_cols)
        scratch[f"num_slot{index}"] = pltpu.VMEM((2,) + shape, f32)
        scratch[f"light_slot{index}"] = pltpu.VMEM((1,) + shape, f32)
    names = ["offs", "probe_in", "patterns_in", "specimen_in"]
    names += [f"table_in{n}" for n in range(4)] + ["new_probe", "new_specimen"] + list(scratch)

    def kernel(*refs):
        update_kernel(extra, names, *refs)

    vmem = pl.BlockSpec(memory_space=pltpu.VMEM)
    return pl.pallas_call(
        kernel,
        name="update",
        out_shape=(
            jax.ShapeDtypeStruct(probe_modes.shape, f32),
            jax.ShapeDtypeStruct(specimen.shape, f32),
        ),
        in_specs=[pl.BlockSpec(memory_space=pltpu.SMEM)] + [pl.BlockSpec(memory_space=pl.ANY)] * 7,
        out_specs=(vmem, vmem),
        scratch_shapes=list(scratch.values()),
        compiler_params=pltpu.CompilerParams(has_side_effects=True, vmem_limit_bytes=56 * 1024 * 1024),
    )(offsets.T, probe_modes, patterns, specimen, *tables)


def solution(mesh):
    return jax.shard_map(
        body,
        mesh=mesh,
        in_specs=(
            P(),
            P(("scan", "tile"), None, None),
            P(None, "scan", "tile"),
            P(("scan", "tile"), None),
        ),
        out_specs=(P(), P(None, "scan", "tile")),
        check_vma=False,
    )
```

```python
import math

import jax
import jax.numpy as jnp
import numpy as np
from jax import lax
from jax.experimental import pallas as pl
from jax.experimental.pallas import tpu as pltpu
from jax.sharding import PartitionSpec as P

NS_STEPS = 8


highest = lax.Precision.HIGHEST
light_floor = 0.05
object_reg = 0.5
probe_reg = 1.0
total_eps = 1e-06


def dft_tables(detector):
    indices = np.arange(detector, dtype=np.int64)
    angles = -2.0 * np.pi / detector * (indices[:, None] * indices[None, :] % detector)
    table_re = np.cos(angles) / np.sqrt(detector)
    table_im = np.sin(angles) / np.sqrt(detector)
    right = np.block([[table_re, table_im], [-table_im, table_re]]).astype(np.float32)
    left = np.ascontiguousarray(right.T)
    parts = []
    for table in (right, left):
        high = table.astype(jnp.bfloat16)
        low = (table - high.astype(np.float32)).astype(jnp.bfloat16)
        parts.append((high, low))
    (rh, rl), (lh, ll) = parts
    return (
        np.concatenate([rh, rl, rh], axis=0),
        np.concatenate([lh, ll, lh], axis=1),
        np.concatenate([rh, rl, rh], axis=1),
        np.concatenate([lh, ll, lh], axis=0),
    )


def halves(value):
    high = value.astype(jnp.bfloat16)
    low = (value - high.astype(jnp.float32)).astype(jnp.bfloat16)
    return high, low


core_dim = ("scan", 1, 2)
slab_dims = (("scan", 2, 2), ("tile", 1, 2), ("scan", 4, 4))
slab_sizes = tuple(size for _, _, size in slab_dims)
slab_count = math.prod(slab_sizes)


def extra_bits():
    bits = []
    for axis, bit in (("scan", 16), ("tile", 2)):
        while bit < lax.axis_size(axis):
            bits.append((axis, bit, 2))
            bit *= 2
    return bits


def slab_coords(tile):
    coords = []
    for size in reversed(slab_sizes):
        coords.append(tile % size)
        tile = tile // size
    return tuple(coords[::-1])


def directions():
    return [(i, j) for i, j in ((1, 0), (-1, 0), (0, 1), (0, -1), (1, 1), (1, -1), (-1, 1), (-1, -1))]


def digit(dim):
    axis, bit, size = dim
    return (lax.axis_index(axis) // bit) % size


def flipped(value, size, d):
    if size == 2:
        return 1 - value if d else value
    low, high = value % 2, value // 2
    low = 1 - low if d % 2 else low
    high = 1 - high if d // 2 else high
    return low + 2 * high


def peer(moves):
    where = {}
    for dim, d in moves:
        axis, bit, size = dim
        here = digit(dim)
        base = where.get(axis, lax.axis_index(axis))
        where[axis] = base + bit * (flipped(here, size, d) - here)
    return where


def full_dot(a, b):
    return jnp.dot(a, b, precision=highest, preferred_element_type=jnp.float32)


def zeros_into(ref):
    ref[...] = jnp.zeros(ref.shape, ref.dtype)


def update_kernel(extra, names, *refs):
    f32 = jnp.float32
    r = dict(zip(names, refs))
    offs, probe_in, patterns_in, specimen_in = r["offs"], r["probe_in"], r["patterns_in"], r["specimen_in"]
    new_probe, new_specimen = r["new_probe"], r["new_specimen"]
    probe, patterns, specimen, tables = r["probe"], r["patterns"], r["specimen"], [r[f"table{n}"] for n in range(4)]
    ext, pads, frame_num, frame_light = r["ext"], r["pads"], r["frame_num"], r["frame_light"]
    deep, half, far, patch, factor, num = r["deep"], r["half"], r["far"], r["patch"], r["factor"], r["num"]
    power, light, totals, total_land = r["power"], r["light"], r["totals"], r["total_land"]
    packed, land0, acc, full = r["packed"], r["land0"], r["acc"], r["full"]
    land1, land2, landx, land_all = r["land1"], r["land2"], r["landx"], r["land_all"]
    num_slots = [r[f"num_slot{i}"] for i in range(8)]
    light_slots = [r[f"light_slot{i}"] for i in range(8)]
    gram_out, gram_land, gram_x, interior = r["gram_out"], r["gram_land"], r["gram_x"], r["interior"]
    send_sem, recv_sem, local_sem = r["send_sem"], r["recv_sem"], r["local_sem"]
    right_f, left_f, left_b, right_b = tables

    modes, det = probe.shape[0], probe.shape[-1]
    count = patterns.shape[0]
    block_rows, block_cols = specimen.shape[1:]
    own_blocks = block_cols // det
    col_blocks = own_blocks + 2
    ext_rows = block_rows + 2 * det
    groups = modes // 2
    direct_sums = (groups - 1,)
    direct_gathers = ()
    fold_pieces = 2
    rows = det // slab_count
    planes = 2 * modes
    used = [0]

    here = {axis: lax.axis_index(axis) for axis in ("scan", "tile")}
    sizes = {axis: lax.axis_size(axis) for axis in ("scan", "tile")}

    def route(src, dst, device):
        n = used[0]
        used[0] += 1
        return pltpu.make_async_remote_copy(
            src_ref=src, dst_ref=dst, send_sem=send_sem.at[n], recv_sem=recv_sem.at[n],
            device_id=device, device_id_type=pl.DeviceIdType.MESH,
        )

    def remote(src, dst, moves):
        return route(src, dst, peer(moves))

    class Batch:
        def __init__(self, whole):
            self.whole = whole
            self.n = used[0]
            used[0] += 1

        def make(self, src, dst, device):
            return pltpu.make_async_remote_copy(
                src_ref=src, dst_ref=dst, send_sem=send_sem.at[self.n], recv_sem=recv_sem.at[self.n],
                device_id=device, device_id_type=pl.DeviceIdType.MESH,
            )

        def send(self, src, dst, moves):
            self.make(src, dst, peer(moves)).start()

        def wait(self):
            self.make(self.whole, self.whole, peer([(core_dim, 1)])).wait()

    def shifted(i, j):
        return {
            "scan": (here["scan"] + i + sizes["scan"]) % sizes["scan"],
            "tile": (here["tile"] + j + sizes["tile"]) % sizes["tile"],
        }

    def valid(i, j):
        row, col = here["scan"] + i, here["tile"] + j
        return (row >= 0) & (row < sizes["scan"]) & (col >= 0) & (col < sizes["tile"])

    def launch(copies):
        for item in copies:
            item.start()
        return copies

    def settle(copies):
        for item in copies:
            item.wait()

    core = digit(core_dim)
    mine = [digit(dim) for dim in slab_dims]

    off_shift, on_shift = 2 * core - 1, 1 - 2 * core

    def outer_rows(i):
        return pl.ds(pl.multiple_of((1 - i) // 2 * (det + block_rows), 8), det)

    def edge_rows(i, base):
        return pl.ds(pl.multiple_of(base + (1 + i) // 2 * (block_rows - det), 8), det)

    def edge_block(j):
        return own_blocks - 1 if j == 1 else 0

    def outer_block(j):
        return 0 if j == 1 else own_blocks + 1

    off_valid = valid(off_shift, 0)
    right_valid, left_valid = valid(0, 1), valid(0, -1)
    near = jnp.where(right_valid, own_blocks - 1, 0)
    distant = own_blocks - 1 - near
    inner_blocks = list(range(1, own_blocks - 1))
    local = []

    def load(src, dst):
        item = pltpu.make_async_copy(src, dst, local_sem.at[len(local)])
        item.start()
        local.append(item)
        return item

    def row_copy(i, b, c, channels):
        channel = pl.ds(c, channels)
        return route(
            specimen_in.at[channel, edge_rows(i, 0), pl.ds(pl.multiple_of(b * det, det), det)],
            ext.at[channel, 1 + b, outer_rows(i), :],
            shifted(i, 0),
        )

    near_rows = [row_copy(off_shift, near, c, 1) for c in range(2)]
    rest = [distant] * (own_blocks > 1) + inner_blocks
    off_rows = [row_copy(off_shift, b, 0, 2) for b in rest]
    on_rows = [row_copy(on_shift, b, 0, 2) for b in range(own_blocks)]

    @pl.when(off_valid)
    def _():
        launch(near_rows)

    side = {}
    for j in (1, -1):
        b = edge_block(j)
        side[j] = route(
            specimen_in.at[:, :, b * det : (b + 1) * det],
            ext.at[:, outer_block(j), pl.ds(det, block_rows), :],
            shifted(0, j),
        )

        @pl.when(valid(0, j))
        def _():
            side[j].start()

    launch(on_rows)
    @pl.when(off_valid)
    def _():
        launch(off_rows)

    probe_load = load(probe_in, probe)
    own_load = [
        load(specimen_in.at[:, :, b * det : (b + 1) * det], ext.at[:, 1 + b, pl.ds(det, block_rows), :])
        for b in range(own_blocks)
    ]
    other_loads = [load(patterns_in, patterns), load(specimen_in, specimen)]
    for n in range(4):
        other_loads.append(load(r[f"table_in{n}"], tables[n]))

    blank = jnp.zeros((2, det, det), f32)
    zeros_into(ext.at[:, col_blocks])

    @pl.when(jnp.logical_not(off_valid))
    def _():
        for b in range(col_blocks):
            ext[:, b, outer_rows(-off_shift), :] = blank

    for j in (1, -1):
        @pl.when(jnp.logical_not(valid(0, -j)))
        def _():
            ext[:, outer_block(j), pl.ds(det, block_rows), :] = jnp.zeros((2, block_rows, det), f32)
            ext[:, outer_block(j), outer_rows(1), :] = blank
            ext[:, outer_block(j), outer_rows(-1), :] = blank

    zeros_into(pads)
    zeros_into(num)
    zeros_into(light)

    lanes = lax.broadcasted_iota(jnp.int32, (det, det), 1)
    row_base = here["scan"] * block_rows - det
    col_base = here["tile"] * block_cols - det

    def place(p):
        row = jnp.clip(offs[0, p] - row_base, 0, block_rows + det)
        col = jnp.clip(offs[1, p] - col_base, 0, block_cols + det)
        block = col // det
        return row, col, block, col - block * det

    def build_frame(frame, channels):
        chunk = 64
        strip_lanes = lax.broadcasted_iota(jnp.int32, (chunk, det), 1)

        def some(n, carry):
            base = pl.multiple_of(n * chunk, chunk)
            for c in range(channels):
                values = [jnp.zeros((chunk, det), f32) for _ in range(col_blocks)]
                for p in range(count):
                    row, col, _, _ = place(p)
                    piece = pads[p, c, pl.ds(ext_rows - det - row + base, chunk), :]
                    for j in range(col_blocks):
                        at = strip_lanes + (j * det - col)
                        values[j] = values[j] + jnp.where((at >= 0) & (at < det), piece, 0.0)
                for j in range(col_blocks):
                    frame[c, pl.ds(base, chunk), j * det : (j + 1) * det] = values[j]
            return carry

        lax.fori_loop(0, ext_rows // chunk, some, 0)

    pad_at = pl.ds(ext_rows - det, det)
    probe_load.wait()
    value = jnp.zeros((det, det), f32)
    for k in range(modes):
        value = value + probe[k, 0] * probe[k, 0] + probe[k, 1] * probe[k, 1]
    power[...] = value
    for p in range(count):
        pads[p, 0, pad_at, :] = pltpu.roll(power[...], place(p)[3], 1)
    build_frame(frame_light, 1)

    def corner(j, c):
        channel = pl.ds(c, 1)
        return route(
            ext.at[channel, 1 + edge_block(j), outer_rows(-off_shift), :],
            ext.at[channel, outer_block(j), outer_rows(-off_shift), :],
            shifted(0, j),
        )

    relay = []
    corners = {j: [corner(j, c) for c in range(2)] for j in (1, -1)}
    for j in (1, -1):
        relay += [(item, off_valid & valid(0, j), off_valid & valid(0, -j)) for item in corners[j]]
    for c in range(2):
        @pl.when(off_valid)
        def _():
            near_rows[c].wait()

        @pl.when(off_valid & right_valid)
        def _():
            corners[1][c].start()

        @pl.when(off_valid & left_valid & jnp.logical_not(right_valid))
        def _():
            corners[-1][c].start()

    for j in (1, -1):
        @pl.when(valid(0, j))
        def _():
            side[j].wait_send()

        item = route(
            ext.at[:, outer_block(j), edge_rows(on_shift, det), :],
            ext.at[:, outer_block(j), outer_rows(on_shift), :],
            shifted(on_shift, 0),
        )
        relay.append((item, valid(0, -j), valid(0, -j)))

        @pl.when(valid(0, -j))
        def _():
            side[j].wait_recv()
            item.start()

    settle(on_rows)

    @pl.when(off_valid)
    def _():
        settle(off_rows)

    @pl.when(off_valid & left_valid & right_valid)
    def _():
        launch(corners[-1])

    for item, sent, came in relay:
        @pl.when(sent)
        def _():
            item.wait_send()

        @pl.when(came)
        def _():
            item.wait_recv()
    for item in own_load + other_loads:
        item.wait()

    def span(shift, block):
        low = {-1: 0, 0: det, 1: det + block}[shift]
        return pl.ds(low, block if shift == 0 else det)

    def inner(shift, block):
        low = {-1: block - det, 0: 0, 1: 0}[shift]
        return pl.ds(low, block if shift == 0 else det)

    class Fold:
        def __init__(self, frame, slots, first):
            self.slots, self.first = slots, first
            self.batches = [Batch(slot) for slot in slots]
            self.pending = []
            channels = frame.shape[0]
            for index in (0, 1, 4, 5, 6, 7, 2, 3):
                i, j = directions()[index]
                height = det if i else block_rows
                low = span(i, block_rows).start
                pieces = fold_pieces if j == 0 else 1
                for c in range(channels):
                    for n in range(pieces):
                        size = height // pieces
                        source = frame.at[pl.ds(c, 1), pl.ds(low + n * size, size), span(j, block_cols)]
                        target = slots[index].at[pl.ds(c, 1), pl.ds(n * size, size)]
                        self.pending.append((index, source, target))

        def some(self, n):
            for index, source, target in self.pending[:n]:
                i, j = directions()[index]

                @pl.when(valid(i, j))
                def _():
                    self.batches[index].make(source, target, shifted(i, j)).start()
            self.pending = self.pending[n:]

        def end(self):
            into = slice(self.first, self.first + self.slots[0].shape[0])
            for index, (i, j) in enumerate(directions()):
                item = self.batches[index].make(self.slots[index], self.slots[index], shifted(i, j))

                @pl.when(valid(i, j))
                def _():
                    item.wait_send()

                @pl.when(valid(-i, -j))
                def _():
                    item.wait_recv()
                    a, b = inner(i, block_rows), inner(j, block_cols)
                    interior[into, a, b] = interior[into, a, b] + self.slots[index][...]

    light_fold = Fold(frame_light, light_slots, 2)
    light_fold.some(100)

    total = jnp.zeros((det, det), f32)
    for p in range(count):
        row, _, block, shift = place(p)
        back = lax.rem(det - shift, det)
        for c in range(2):
            first = pltpu.roll(ext[c, block, pl.ds(row, det), :], back, 1)
            second = pltpu.roll(ext[c, block + 1, pl.ds(row, det), :], back, 1)
            patch[p, c] = jnp.where(lanes < det - shift, first, second)
        patch_light = patch[p, 0] * patch[p, 0] + patch[p, 1] * patch[p, 1]
        light[...] = light[...] + patch_light
        total = total + patch_light * power[...]
        factor[p] = jnp.zeros((det, det), f32)
    some = pl.ds(0, 2 * count * det)

    def forward(q, carry):
        columns = pl.ds(pl.multiple_of(q * 2 * det, 2 * det), 2 * det)
        for p in range(count):
            patch_re, patch_im = patch[p, 0], patch[p, 1]
            for m in range(2):
                at = pl.ds((2 * p + m) * det, det)
                pr, pi = probe[q + m * groups, 0], probe[q + m * groups, 1]
                for c, value in enumerate((pr * patch_re - pi * patch_im, pr * patch_im + pi * patch_re)):
                    high, low = halves(value)
                    deep[at, pl.ds(c * det, det)] = high
                    deep[at, pl.ds((2 + c) * det, det)] = high
                    deep[at, pl.ds((4 + c) * det, det)] = low
        half[some, :] = jnp.dot(deep[some, :], right_f[...], preferred_element_type=f32)
        for p in range(count):
            first, second = [half[pl.ds((2 * p + m) * det, det), :] for m in range(2)]
            paired = jnp.concatenate(
                [
                    jnp.concatenate([first[:, :det], second[:, :det]], axis=1),
                    jnp.concatenate([first[:, det:], second[:, det:]], axis=1),
                ],
                axis=0,
            )
            high, low = halves(paired)
            stacked = jnp.concatenate([high, high, low], axis=0)
            out = jnp.dot(left_f[...], stacked, preferred_element_type=f32)
            far[p, :, columns] = out
            squares = out * out
            both = squares[:det] + squares[det:]
            factor[p] = factor[p] + (both[:, :det] + both[:, det:])
        return carry

    lax.fori_loop(0, groups, forward, 0)
    for p in range(count):
        factor[p] = jnp.sqrt(patterns[p]) / jnp.sqrt(jnp.maximum(factor[p], light_floor)) - 1.0
    measured = jnp.zeros((det, det), f32)
    for p in range(count):
        measured = measured + patterns[p]
    totals[0] = jnp.sum(measured.reshape(det // 8, 8, det), axis=0)
    totals[1] = jnp.sum(total.reshape(det // 8, 8, det), axis=0)
    spread_shape = slab_sizes + (rows, det)
    for h in range(2):
        r["packed_light"][h, :, :, :, 0] = light[...].reshape(spread_shape)

    home = tuple(mine)

    def flips_of(stage):
        flips = [()]
        for i in range(3):
            flips = [f + (d,) for f in flips for d in range(slab_sizes[i] if i in stage else 1)]
        return flips[1:]

    def spot_of(known, flips=(0, 0, 0)):
        return tuple(flipped(mine[i], slab_sizes[i], flips[i]) if i in known else slice(None) for i in range(3))

    def moves_of(flips):
        return list(zip(slab_dims, flips))

    two_steps, one_step = ((0, 1), (2,)), ((0, 1, 2),)

    class Sum:
        def __init__(self, stages, source, land0, acc, lands, landx):
            self.stages, self.source, self.acc = stages, source, acc
            self.land0, self.lands, self.landx = land0, lands, landx
            self.swap = remote(source.at[1 - core], land0, [(core_dim, 1)])
            self.batches = [Batch(land) for land in lands]

        def known(self, step):
            return [i for stage in self.stages[: step + 1] for i in stage]

        def send(self, step):
            for n, flips in enumerate(flips_of(self.stages[step])):
                source = self.acc.at[spot_of(self.known(step), flips)]
                self.batches[step].send(source, self.lands[step].at[n], moves_of(flips))

        def swapped(self):
            self.swap.wait()
            self.acc[...] = self.source[core] + self.land0[...]
            self.send(0)

        def reduced(self, step):
            self.batches[step].wait()
            land = self.lands[step]
            spot = spot_of(self.known(step))
            value = self.acc[spot]
            for d in range(land.shape[0]):
                value = value + land[d]
            self.acc[spot] = value
            if step < len(self.lands) - 1:
                self.send(step + 1)
                return
            for e, dim in enumerate(extra):
                item = remote(self.acc.at[home], self.landx.at[e], [(dim, 1)])
                item.start()
                item.wait()
                self.acc[home] = self.acc[home] + self.landx[e]

    light_sum = Sum(
        two_steps, r["packed_light"], r["land0_light"], r["acc_light"],
        [r["land1_light"], r["land2_light"]], r["landx_light"],
    )
    sums = []
    for q in range(groups):
        direct = q in direct_sums
        sums.append(
            Sum(
                one_step if direct else two_steps, packed.at[q], land0.at[q], acc.at[q],
                [land_all.at[q]] if direct else [land1.at[q], land2.at[q]], landx.at[q],
            )
        )
    total_swap = remote(totals, total_land, [(core_dim, 1)])

    def at_group(n):
        if n == 0:
            light_sum.swap.start()
            total_swap.start()
            return
        sums[n - 1].swap.start()
        if n == 2:
            light_sum.swapped()
        if n >= 3:
            sums[n - 3].swapped()

    def backward(q, carry):
        for n in range(groups):
            @pl.when(q == n)
            def _():
                at_group(n)

        columns = pl.ds(pl.multiple_of(q * 2 * det, 2 * det), 2 * det)
        for p in range(count):
            wide = jnp.concatenate([factor[p], factor[p]], axis=1)
            wide = jnp.concatenate([wide, wide], axis=0)
            high, low = halves(far[p, :, columns] * wide)
            stacked = jnp.concatenate([high, high, low], axis=0)
            out = jnp.dot(left_b[...], stacked, preferred_element_type=f32)
            high, low = halves(out)
            for m in range(2):
                at = pl.ds((2 * p + m) * det, det)
                for c in range(2):
                    part_h = high[c * det : (c + 1) * det, m * det : (m + 1) * det]
                    part_l = low[c * det : (c + 1) * det, m * det : (m + 1) * det]
                    deep[at, pl.ds(c * det, det)] = part_h
                    deep[at, pl.ds((2 + c) * det, det)] = part_h
                    deep[at, pl.ds((4 + c) * det, det)] = part_l
        half[some, :] = jnp.dot(deep[some, :], right_b[...], preferred_element_type=f32)
        for m in range(2):
            pr, pi = probe[q + m * groups, 0], probe[q + m * groups, 1]
            grad_re = jnp.zeros((det, det), f32)
            grad_im = jnp.zeros((det, det), f32)
            for p in range(count):
                at = pl.ds((2 * p + m) * det, det)
                cr, ci = half[at, :det], half[at, det:]
                patch_re, patch_im = patch[p, 0], patch[p, 1]
                grad_re = grad_re + patch_re * cr + patch_im * ci
                grad_im = grad_im + patch_re * ci - patch_im * cr
                num[p, 0] = num[p, 0] + (pr * cr + pi * ci)
                num[p, 1] = num[p, 1] + (pr * ci - pi * cr)
            packed[q, m, :, :, :, 0] = grad_re.reshape(spread_shape)
            packed[q, m, :, :, :, 1] = grad_im.reshape(spread_shape)
        return carry

    lax.fori_loop(0, groups, backward, 0)

    tile = mine[0]
    for i in range(1, 3):
        tile = tile * slab_sizes[i] + mine[i]
    strip = pl.ds(pl.multiple_of(tile * rows, rows), rows)
    own = Batch(full.at[(slice(None), core) + home])

    class Gather:
        def __init__(self, q):
            self.q = q
            self.view = full.at[q, core]
            if q in direct_gathers:
                self.stages = one_step
                self.batches = [Batch(land_all.at[0])]
            else:
                self.stages = two_steps[::-1]
                self.batches = [Batch(land2.at[0]), Batch(land1.at[0])]
            self.passing = Batch(land_all.at[0])

        def both(self, batch, spot, moves):
            batch.send(self.view.at[spot], self.view.at[spot], moves)

        def left(self, step):
            return [i for stage in self.stages[step:] for i in stage]

        def send(self, step):
            for flips in flips_of(self.stages[step]):
                self.both(self.batches[step], spot_of(self.left(step)), moves_of(flips))

        def begin(self):
            q = self.q
            for c in range(2):
                value = probe[core * groups + q, c, strip, :] + acc[(q,) + home + (c,)] * scale
                full[(q, core) + home + (c,)] = value
            self.both(own, home, [(core_dim, 1)])
            self.send(0)

        def got(self, step):
            self.batches[step].wait()
            if step < len(self.stages) - 1:
                self.send(step + 1)
            for flips in flips_of(self.stages[step]):
                self.both(self.passing, spot_of(self.left(step), flips), [(core_dim, 1)])

    gathers = [Gather(q) for q in range(groups)]

    at_group(groups)
    for p in range(count):
        shift = place(p)[3]
        for c in range(2):
            pads[p, c, pad_at, :] = pltpu.roll(num[p, c], shift, 1)
    build_frame(frame_num, 2)
    sums[groups - 2].swapped()
    sums[groups - 1].swapped()
    light_sum.reduced(0)
    num_fold = Fold(frame_num, num_slots, 0)
    for q in range(groups - 1):
        sums[q].reduced(0)
        num_fold.some(2)
    light_sum.reduced(1)
    scale = 1.0 / (r["acc_light"][home + (0,)] + probe_reg)
    for q in range(groups):
        if q not in direct_sums:
            sums[q].reduced(1)
            num_fold.some(2)
    sums[groups - 1].reduced(0)
    for q in range(groups):
        gathers[q].begin()
    num_fold.some(2)

    def slab_rows(spot):
        values = []
        for n in range(planes):
            c, k = n // modes, n % modes
            values.append(full[(k % groups, k // groups) + spot + (c,)])
        return jnp.concatenate(values, axis=0)

    tall = planes * rows
    up = lax.broadcasted_iota(jnp.int32, (tall, tall), 0)
    across = lax.broadcasted_iota(jnp.int32, (tall, tall), 1)
    same = jnp.where(((up - across) & (rows - 1)) == 0, 1.0, 0.0).astype(f32)
    plane = lax.broadcasted_iota(jnp.int32, (planes, tall), 0) * rows
    entry = lax.broadcasted_iota(jnp.int32, (planes, tall), 1)
    pick = jnp.where((entry >= plane) & (entry < plane + rows), 1.0, 0.0).astype(f32)
    plane = lax.broadcasted_iota(jnp.int32, (tall, det), 1) * rows
    entry = lax.broadcasted_iota(jnp.int32, (tall, det), 0)
    settled = jnp.where((entry >= plane) & (entry < plane + rows), 1.0, 0.0).astype(f32)

    own.wait()
    held = slab_rows(home)
    turned = jnp.concatenate([-held[tall // 2 :], held[: tall // 2]], axis=0)
    wide = jnp.concatenate([held, turned], axis=1)
    pairs = lax.dot_general(
        wide, wide, (((1,), (1,)), ((), ())), precision=highest, preferred_element_type=f32
    )
    gram = full_dot(full_dot(pick, pairs * same), settled)
    total_swap.wait()
    both = [jnp.sum(totals[i] + total_land[i]) for i in range(2)]
    sheet_lanes = lax.broadcasted_iota(jnp.int32, (8, det), 1)
    first = lax.broadcasted_iota(jnp.int32, (8, det), 0) == 0
    at_measured = first & (sheet_lanes == det - 2)
    at_modelled = first & (sheet_lanes == det - 1)
    sheet = jnp.where(at_measured, both[0], jnp.where(at_modelled, both[1], 0.0))
    for part in range(planes // 8):
        piece = gram[part * 8 : (part + 1) * 8]
        sheet = sheet + (pltpu.roll(piece, part * 32, 1) if part else piece)
    gram_out[...] = sheet
    spread = Batch(gram_land)
    for slot in range(1, slab_count):
        spread.send(gram_out, gram_land.at[slot - 1], list(zip(slab_dims, slab_coords(slot))))
    for q in range(groups):
        if q not in direct_gathers:
            gathers[q].got(0)
            num_fold.some(2)
    num_fold.some(100)
    spread.wait()
    sheet = gram_out[...]
    for i in range(slab_count - 1):
        sheet = sheet + gram_land[i]
    for e, dim in enumerate(extra):
        gram_x[2 * e] = sheet
        item = remote(gram_x.at[2 * e], gram_x.at[2 * e + 1], [(dim, 1)])
        item.start()
        item.wait()
        sheet = sheet + gram_x[2 * e + 1]
    measured = jnp.sum(jnp.where(at_measured, sheet, 0.0))
    modelled = jnp.sum(jnp.where(at_modelled, sheet, 0.0))
    ratio = measured / (modelled + total_eps)
    parts = [sheet[:, part * 32 : part * 32 + planes] for part in range(planes // 8)]
    embedded = jnp.concatenate(parts, axis=0)
    eye = jnp.where(
        lax.broadcasted_iota(jnp.int32, (planes, planes), 0) == lax.broadcasted_iota(jnp.int32, (planes, planes), 1),
        1.0, 0.0,
    ).astype(f32)
    frobenius = jnp.sqrt(jnp.sum(embedded * embedded, keepdims=True))
    current = embedded / frobenius
    inverse = eye
    for repeat in range(NS_STEPS):
        scaled = 1.5 * eye - 0.5 * full_dot(inverse, current)
        current = full_dot(current, scaled)
        inverse = full_dot(scaled, inverse)
    weight = jnp.sqrt(ratio * jnp.sum(embedded * eye, axis=1, keepdims=True))
    mix = weight * (inverse / jnp.sqrt(frobenius))
    mix = lax.dot_general(
        pick, full_dot(mix, pick), (((0,), (0,)), ((), ())), precision=highest, preferred_element_type=f32
    )
    high, low = halves(mix * same)
    mixer = jnp.concatenate([high, low, high], axis=1)
    for q in range(groups):
        gathers[q].got(0 if q in direct_gathers else 1)

    interior[0:2] = frame_num[:, det : det + block_rows, det : det + block_cols]
    interior[2] = frame_light[0, det : det + block_rows, det : det + block_cols]
    light_fold.end()
    num_fold.end()
    new_specimen[...] = specimen[...] + interior[0:2] / (interior[2] + object_reg)[None]

    for item in gathers:
        item.passing.wait()
    for t in range(0, slab_count, 2):
        sides = [slab_rows(slab_coords(s)) for s in (t, t + 1)]
        high, low = halves(jnp.concatenate(sides, axis=1))
        out = jnp.dot(mixer, jnp.concatenate([high, high, low], axis=0), preferred_element_type=f32)
        for n in range(planes):
            for s in range(2):
                new_probe[n % modes, n // modes, (t + s) * rows : (t + s + 1) * rows, :] = out[
                    n * rows : (n + 1) * rows, s * det : (s + 1) * det
                ]


def emit_kernel(*refs):
    sources, targets, held = refs[:2], refs[2:4], refs[4:6]
    come, gone = refs[6:]
    steps = []
    for source, target, buffer in zip(sources, targets, held):
        rows = max(source.shape[0] // 6, 1)
        for low in range(0, source.shape[0], rows):
            at = pl.ds(low, rows)
            n = len(steps)
            steps.append(
                (
                    pltpu.make_async_copy(source.at[at], buffer.at[at], come.at[n]),
                    pltpu.make_async_copy(buffer.at[at], target.at[at], gone.at[n]),
                )
            )
    for arrive, _ in steps:
        arrive.start()
    for arrive, leave in steps:
        arrive.wait()
        leave.start()
    for _, leave in steps:
        leave.wait()


def emit(probe, specimen):
    anywhere = pl.BlockSpec(memory_space=pl.ANY)
    return pl.pallas_call(
        emit_kernel,
        name="emit",
        out_shape=tuple(jax.ShapeDtypeStruct(x.shape, x.dtype) for x in (probe, specimen)),
        in_specs=[anywhere] * 2,
        out_specs=(anywhere,) * 2,
        scratch_shapes=[
            pltpu.VMEM(probe.shape, probe.dtype),
            pltpu.VMEM(specimen.shape, specimen.dtype),
            pltpu.SemaphoreType.DMA((16,)),
            pltpu.SemaphoreType.DMA((16,)),
        ],
        compiler_params=pltpu.CompilerParams(vmem_limit_bytes=56 * 1024 * 1024),
    )(probe, specimen)


def body(probe_modes, patterns, specimen, offsets):
    f32 = jnp.float32
    modes, _, det, _ = probe_modes.shape
    count = patterns.shape[0]
    block_rows, block_cols = specimen.shape[1:]
    col_blocks = block_cols // det + 2
    ext_rows = block_rows + 2 * det
    ext_cols = block_cols + 2 * det
    extra = extra_bits()
    more = max(len(extra), 1)
    rows = det // slab_count
    groups = modes // 2
    bf16 = jnp.bfloat16
    tables = [jnp.asarray(t) for t in dft_tables(det)]
    sems = 84 + (groups + 2) * len(extra)
    scratch = {
        "probe": pltpu.VMEM(probe_modes.shape, f32),
        "patterns": pltpu.VMEM(patterns.shape, f32),
        "specimen": pltpu.VMEM(specimen.shape, f32),
        **{f"table{n}": pltpu.VMEM(t.shape, bf16) for n, t in enumerate(tables)},
        "ext": pltpu.VMEM((2, col_blocks + 1, ext_rows, det), f32),
        "pads": pltpu.VMEM((count, 2, 2 * (ext_rows - det) + det, det), f32),
        "frame_num": pltpu.VMEM((2, ext_rows, ext_cols), f32),
        "frame_light": pltpu.VMEM((1, ext_rows, ext_cols), f32),
        "deep": pltpu.VMEM((2 * count * det, 6 * det), bf16),
        "half": pltpu.VMEM((2 * count * det, 2 * det), f32),
        "far": pltpu.VMEM((count, 2 * det, modes * det), f32),
        "patch": pltpu.VMEM((count, 2, det, det), f32),
        "factor": pltpu.VMEM((count, det, det), f32),
        "num": pltpu.VMEM((count, 2, det, det), f32),
        "power": pltpu.VMEM((det, det), f32),
        "light": pltpu.VMEM((det, det), f32),
        "totals": pltpu.VMEM((2, 8, det), f32),
        "total_land": pltpu.VMEM((2, 8, det), f32),
        "gram_out": pltpu.VMEM((8, det), f32),
        "gram_land": pltpu.VMEM((slab_count - 1, 8, det), f32),
        "gram_x": pltpu.VMEM((2 * more, 8, det), f32),
        "interior": pltpu.VMEM((3, block_rows, block_cols), f32),
        "send_sem": pltpu.SemaphoreType.DMA((sems,)),
        "recv_sem": pltpu.SemaphoreType.DMA((sems,)),
        "local_sem": pltpu.SemaphoreType.DMA((16,)),
    }
    for end, lead, planes in (("", (groups,), 2), ("_light", (), 1)):
        tile = (planes, rows, det)
        scratch["packed" + end] = pltpu.VMEM(lead + (2,) + slab_sizes + tile, f32)
        scratch["land0" + end] = pltpu.VMEM(lead + slab_sizes + tile, f32)
        scratch["acc" + end] = pltpu.VMEM(lead + slab_sizes + tile, f32)
        scratch["land1" + end] = pltpu.VMEM(lead + (slab_sizes[0] * slab_sizes[1] - 1, slab_sizes[2]) + tile, f32)
        scratch["land2" + end] = pltpu.VMEM(lead + (slab_sizes[2] - 1,) + tile, f32)
        scratch["landx" + end] = pltpu.VMEM(lead + (more,) + tile, f32)
    scratch["land_all"] = pltpu.VMEM((groups, slab_count - 1, 2, rows, det), f32)
    scratch["full"] = pltpu.VMEM((groups, 2) + slab_sizes + (2, rows, det), f32)
    for index, (i, j) in enumerate(directions()):
        shape = (det if i else block_rows, det if j else block_cols)
        scratch[f"num_slot{index}"] = pltpu.VMEM((2,) + shape, f32)
        scratch[f"light_slot{index}"] = pltpu.VMEM((1,) + shape, f32)
    names = ["offs", "probe_in", "patterns_in", "specimen_in"]
    names += [f"table_in{n}" for n in range(4)] + ["new_probe", "new_specimen"] + list(scratch)

    def kernel(*refs):
        update_kernel(extra, names, *refs)

    vmem = pl.BlockSpec(memory_space=pltpu.VMEM)
    results = pl.pallas_call(
        kernel,
        name="update",
        out_shape=(
            jax.ShapeDtypeStruct(probe_modes.shape, f32),
            jax.ShapeDtypeStruct(specimen.shape, f32),
        ),
        in_specs=[pl.BlockSpec(memory_space=pltpu.SMEM)] + [pl.BlockSpec(memory_space=pl.ANY)] * 7,
        out_specs=(vmem, vmem),
        scratch_shapes=list(scratch.values()),
        compiler_params=pltpu.CompilerParams(has_side_effects=True, vmem_limit_bytes=56 * 1024 * 1024),
    )(offsets.T, probe_modes, patterns, specimen, *tables)
    return emit(*results)


def solution(mesh):
    return jax.shard_map(
        body,
        mesh=mesh,
        in_specs=(
            P(),
            P(("scan", "tile"), None, None),
            P(None, "scan", "tile"),
            P(("scan", "tile"), None),
        ),
        out_specs=(P(), P(None, "scan", "tile")),
        check_vma=False,
    )
```

```python
import math

import jax
import jax.numpy as jnp
import numpy as np
from jax import lax
from jax.experimental import pallas as pl
from jax.experimental.pallas import tpu as pltpu
from jax.sharding import PartitionSpec as P

NS_STEPS = 8


highest = lax.Precision.HIGHEST
light_floor = 0.05
object_reg = 0.5
probe_reg = 1.0
total_eps = 1e-06


def dft_tables(detector):
    indices = np.arange(detector, dtype=np.int64)
    angles = -2.0 * np.pi / detector * (indices[:, None] * indices[None, :] % detector)
    table_re = np.cos(angles) / np.sqrt(detector)
    table_im = np.sin(angles) / np.sqrt(detector)
    right = np.block([[table_re, table_im], [-table_im, table_re]]).astype(np.float32)
    left = np.ascontiguousarray(right.T)
    parts = []
    for table in (right, left):
        high = table.astype(jnp.bfloat16)
        low = (table - high.astype(np.float32)).astype(jnp.bfloat16)
        parts.append((high, low))
    (rh, rl), (lh, ll) = parts
    return (
        np.concatenate([rh, rl, rh], axis=0),
        np.concatenate([lh, ll, lh], axis=1),
        np.concatenate([rh, rl, rh], axis=1),
        np.concatenate([lh, ll, lh], axis=0),
    )


def halves(value):
    high = value.astype(jnp.bfloat16)
    low = (value - high.astype(jnp.float32)).astype(jnp.bfloat16)
    return high, low


core_dim = ("scan", 1, 2)
slab_dims = (("scan", 2, 2), ("tile", 1, 2), ("scan", 4, 4))
slab_sizes = tuple(size for _, _, size in slab_dims)
slab_count = math.prod(slab_sizes)


def extra_bits():
    bits = []
    for axis, bit in (("scan", 16), ("tile", 2)):
        while bit < lax.axis_size(axis):
            bits.append((axis, bit, 2))
            bit *= 2
    return bits


def slab_coords(tile):
    coords = []
    for size in reversed(slab_sizes):
        coords.append(tile % size)
        tile = tile // size
    return tuple(coords[::-1])


def directions():
    return [(i, j) for i, j in ((1, 0), (-1, 0), (0, 1), (0, -1), (1, 1), (1, -1), (-1, 1), (-1, -1))]


def digit(dim):
    axis, bit, size = dim
    return (lax.axis_index(axis) // bit) % size


def flipped(value, size, d):
    if size == 2:
        return 1 - value if d else value
    low, high = value % 2, value // 2
    low = 1 - low if d % 2 else low
    high = 1 - high if d // 2 else high
    return low + 2 * high


def peer(moves):
    where = {}
    for dim, d in moves:
        axis, bit, size = dim
        here = digit(dim)
        base = where.get(axis, lax.axis_index(axis))
        where[axis] = base + bit * (flipped(here, size, d) - here)
    return where


def full_dot(a, b):
    return jnp.dot(a, b, precision=highest, preferred_element_type=jnp.float32)


def zeros_into(ref):
    ref[...] = jnp.zeros(ref.shape, ref.dtype)


def update_kernel(extra, names, *refs):
    f32 = jnp.float32
    r = dict(zip(names, refs))
    offs, probe_in, patterns_in, specimen_in = r["offs"], r["probe_in"], r["patterns_in"], r["specimen_in"]
    new_probe, new_specimen = r["new_probe"], r["new_specimen"]
    probe, patterns, specimen, tables = r["probe"], r["patterns"], r["specimen"], [r[f"table{n}"] for n in range(4)]
    ext, pads, frame_num, frame_light = r["ext"], r["pads"], r["frame_num"], r["frame_light"]
    deep, half, far, patch, factor, num = r["deep"], r["half"], r["far"], r["patch"], r["factor"], r["num"]
    power, light, totals, total_land = r["power"], r["light"], r["totals"], r["total_land"]
    packed, land0, acc, full = r["packed"], r["land0"], r["acc"], r["full"]
    land1, land2, landx, land_all = r["land1"], r["land2"], r["landx"], r["land_all"]
    num_slots = [r[f"num_slot{i}"] for i in range(8)]
    light_slots = [r[f"light_slot{i}"] for i in range(8)]
    gram_out, gram_land, gram_x, interior = r["gram_out"], r["gram_land"], r["gram_x"], r["interior"]
    send_sem, recv_sem, local_sem = r["send_sem"], r["recv_sem"], r["local_sem"]
    right_f, left_f, left_b, right_b = tables

    modes, det = probe.shape[0], probe.shape[-1]
    count = patterns.shape[0]
    block_rows, block_cols = specimen.shape[1:]
    own_blocks = block_cols // det
    col_blocks = own_blocks + 2
    ext_rows = block_rows + 2 * det
    groups = modes // 2
    direct_sums = (groups - 1,)
    direct_gathers = ()
    fold_pieces = 2
    rows = det // slab_count
    planes = 2 * modes
    used = [0]

    here = {axis: lax.axis_index(axis) for axis in ("scan", "tile")}
    sizes = {axis: lax.axis_size(axis) for axis in ("scan", "tile")}

    def route(src, dst, device):
        n = used[0]
        used[0] += 1
        return pltpu.make_async_remote_copy(
            src_ref=src, dst_ref=dst, send_sem=send_sem.at[n], recv_sem=recv_sem.at[n],
            device_id=device, device_id_type=pl.DeviceIdType.MESH,
        )

    def remote(src, dst, moves):
        return route(src, dst, peer(moves))

    class Batch:
        def __init__(self, whole):
            self.whole = whole
            self.n = used[0]
            used[0] += 1

        def make(self, src, dst, device):
            return pltpu.make_async_remote_copy(
                src_ref=src, dst_ref=dst, send_sem=send_sem.at[self.n], recv_sem=recv_sem.at[self.n],
                device_id=device, device_id_type=pl.DeviceIdType.MESH,
            )

        def send(self, src, dst, moves):
            self.make(src, dst, peer(moves)).start()

        def wait(self):
            self.make(self.whole, self.whole, peer([(core_dim, 1)])).wait()

    def shifted(i, j):
        return {
            "scan": (here["scan"] + i + sizes["scan"]) % sizes["scan"],
            "tile": (here["tile"] + j + sizes["tile"]) % sizes["tile"],
        }

    def valid(i, j):
        row, col = here["scan"] + i, here["tile"] + j
        return (row >= 0) & (row < sizes["scan"]) & (col >= 0) & (col < sizes["tile"])

    def launch(copies):
        for item in copies:
            item.start()
        return copies

    def settle(copies):
        for item in copies:
            item.wait()

    core = digit(core_dim)
    mine = [digit(dim) for dim in slab_dims]

    off_shift, on_shift = 2 * core - 1, 1 - 2 * core

    def outer_rows(i):
        return pl.ds(pl.multiple_of((1 - i) // 2 * (det + block_rows), 8), det)

    def edge_rows(i, base):
        return pl.ds(pl.multiple_of(base + (1 + i) // 2 * (block_rows - det), 8), det)

    def edge_block(j):
        return own_blocks - 1 if j == 1 else 0

    def outer_block(j):
        return 0 if j == 1 else own_blocks + 1

    off_valid = valid(off_shift, 0)
    right_valid, left_valid = valid(0, 1), valid(0, -1)
    near = jnp.where(right_valid, own_blocks - 1, 0)
    distant = own_blocks - 1 - near
    inner_blocks = list(range(1, own_blocks - 1))
    local = []

    def load(src, dst):
        item = pltpu.make_async_copy(src, dst, local_sem.at[len(local)])
        item.start()
        local.append(item)
        return item

    def row_copy(i, b, c, channels):
        channel = pl.ds(c, channels)
        return route(
            specimen_in.at[channel, edge_rows(i, 0), pl.ds(pl.multiple_of(b * det, det), det)],
            ext.at[channel, 1 + b, outer_rows(i), :],
            shifted(i, 0),
        )

    near_rows = [row_copy(off_shift, near, c, 1) for c in range(2)]
    rest = [distant] * (own_blocks > 1) + inner_blocks
    off_rows = [row_copy(off_shift, b, 0, 2) for b in rest]
    on_rows = [row_copy(on_shift, b, 0, 2) for b in range(own_blocks)]

    @pl.when(off_valid)
    def _():
        launch(near_rows)

    side = {}
    for j in (1, -1):
        b = edge_block(j)
        side[j] = route(
            specimen_in.at[:, :, b * det : (b + 1) * det],
            ext.at[:, outer_block(j), pl.ds(det, block_rows), :],
            shifted(0, j),
        )

        @pl.when(valid(0, j))
        def _():
            side[j].start()

    launch(on_rows)
    @pl.when(off_valid)
    def _():
        launch(off_rows)

    probe_load = load(probe_in, probe)
    own_load = [
        load(specimen_in.at[:, :, b * det : (b + 1) * det], ext.at[:, 1 + b, pl.ds(det, block_rows), :])
        for b in range(own_blocks)
    ]
    other_loads = [load(patterns_in, patterns), load(specimen_in, specimen)]
    for n in range(4):
        other_loads.append(load(r[f"table_in{n}"], tables[n]))

    blank = jnp.zeros((2, det, det), f32)
    zeros_into(ext.at[:, col_blocks])

    @pl.when(jnp.logical_not(off_valid))
    def _():
        for b in range(col_blocks):
            ext[:, b, outer_rows(-off_shift), :] = blank

    for j in (1, -1):
        @pl.when(jnp.logical_not(valid(0, -j)))
        def _():
            ext[:, outer_block(j), pl.ds(det, block_rows), :] = jnp.zeros((2, block_rows, det), f32)
            ext[:, outer_block(j), outer_rows(1), :] = blank
            ext[:, outer_block(j), outer_rows(-1), :] = blank

    zeros_into(pads)
    zeros_into(num)
    zeros_into(light)

    lanes = lax.broadcasted_iota(jnp.int32, (det, det), 1)
    row_base = here["scan"] * block_rows - det
    col_base = here["tile"] * block_cols - det

    def place(p):
        row = jnp.clip(offs[0, p] - row_base, 0, block_rows + det)
        col = jnp.clip(offs[1, p] - col_base, 0, block_cols + det)
        block = col // det
        return row, col, block, col - block * det

    def build_frame(frame, channels):
        chunk = 64
        strip_lanes = lax.broadcasted_iota(jnp.int32, (chunk, det), 1)

        def some(n, carry):
            base = pl.multiple_of(n * chunk, chunk)
            for c in range(channels):
                values = [jnp.zeros((chunk, det), f32) for _ in range(col_blocks)]
                for p in range(count):
                    row, col, _, _ = place(p)
                    piece = pads[p, c, pl.ds(ext_rows - det - row + base, chunk), :]
                    for j in range(col_blocks):
                        at = strip_lanes + (j * det - col)
                        values[j] = values[j] + jnp.where((at >= 0) & (at < det), piece, 0.0)
                for j in range(col_blocks):
                    frame[c, pl.ds(base, chunk), j * det : (j + 1) * det] = values[j]
            return carry

        lax.fori_loop(0, ext_rows // chunk, some, 0)

    pad_at = pl.ds(ext_rows - det, det)
    probe_load.wait()
    value = jnp.zeros((det, det), f32)
    for k in range(modes):
        value = value + probe[k, 0] * probe[k, 0] + probe[k, 1] * probe[k, 1]
    power[...] = value
    for p in range(count):
        pads[p, 0, pad_at, :] = pltpu.roll(power[...], place(p)[3], 1)
    build_frame(frame_light, 1)

    def corner(j, c):
        channel = pl.ds(c, 1)
        return route(
            ext.at[channel, 1 + edge_block(j), outer_rows(-off_shift), :],
            ext.at[channel, outer_block(j), outer_rows(-off_shift), :],
            shifted(0, j),
        )

    relay = []
    corners = {j: [corner(j, c) for c in range(2)] for j in (1, -1)}
    for j in (1, -1):
        relay += [(item, off_valid & valid(0, j), off_valid & valid(0, -j)) for item in corners[j]]
    for c in range(2):
        @pl.when(off_valid)
        def _():
            near_rows[c].wait()

        @pl.when(off_valid & right_valid)
        def _():
            corners[1][c].start()

        @pl.when(off_valid & left_valid & jnp.logical_not(right_valid))
        def _():
            corners[-1][c].start()

    for j in (1, -1):
        @pl.when(valid(0, j))
        def _():
            side[j].wait_send()

        item = route(
            ext.at[:, outer_block(j), edge_rows(on_shift, det), :],
            ext.at[:, outer_block(j), outer_rows(on_shift), :],
            shifted(on_shift, 0),
        )
        relay.append((item, valid(0, -j), valid(0, -j)))

        @pl.when(valid(0, -j))
        def _():
            side[j].wait_recv()
            item.start()

    settle(on_rows)

    @pl.when(off_valid)
    def _():
        settle(off_rows)

    @pl.when(off_valid & left_valid & right_valid)
    def _():
        launch(corners[-1])

    for item, sent, came in relay:
        @pl.when(sent)
        def _():
            item.wait_send()

        @pl.when(came)
        def _():
            item.wait_recv()
    for item in own_load + other_loads:
        item.wait()

    def span(shift, block):
        low = {-1: 0, 0: det, 1: det + block}[shift]
        return pl.ds(low, block if shift == 0 else det)

    def inner(shift, block):
        low = {-1: block - det, 0: 0, 1: 0}[shift]
        return pl.ds(low, block if shift == 0 else det)

    class Fold:
        def __init__(self, frame, slots, first):
            self.slots, self.first = slots, first
            self.batches = [Batch(slot) for slot in slots]
            self.pending = []
            channels = frame.shape[0]
            for index in (0, 1, 4, 5, 6, 7, 2, 3):
                i, j = directions()[index]
                height = det if i else block_rows
                low = span(i, block_rows).start
                pieces = fold_pieces if j == 0 else 1
                for c in range(channels):
                    for n in range(pieces):
                        size = height // pieces
                        source = frame.at[pl.ds(c, 1), pl.ds(low + n * size, size), span(j, block_cols)]
                        target = slots[index].at[pl.ds(c, 1), pl.ds(n * size, size)]
                        self.pending.append((index, source, target))

        def some(self, n):
            for index, source, target in self.pending[:n]:
                i, j = directions()[index]

                @pl.when(valid(i, j))
                def _():
                    self.batches[index].make(source, target, shifted(i, j)).start()
            self.pending = self.pending[n:]

        def end(self):
            into = slice(self.first, self.first + self.slots[0].shape[0])
            for index, (i, j) in enumerate(directions()):
                item = self.batches[index].make(self.slots[index], self.slots[index], shifted(i, j))

                @pl.when(valid(i, j))
                def _():
                    item.wait_send()

                @pl.when(valid(-i, -j))
                def _():
                    item.wait_recv()
                    a, b = inner(i, block_rows), inner(j, block_cols)
                    interior[into, a, b] = interior[into, a, b] + self.slots[index][...]

    light_fold = Fold(frame_light, light_slots, 2)
    light_fold.some(100)

    total = jnp.zeros((det, det), f32)
    for p in range(count):
        row, _, block, shift = place(p)
        back = lax.rem(det - shift, det)
        for c in range(2):
            first = pltpu.roll(ext[c, block, pl.ds(row, det), :], back, 1)
            second = pltpu.roll(ext[c, block + 1, pl.ds(row, det), :], back, 1)
            patch[p, c] = jnp.where(lanes < det - shift, first, second)
        patch_light = patch[p, 0] * patch[p, 0] + patch[p, 1] * patch[p, 1]
        light[...] = light[...] + patch_light
        total = total + patch_light * power[...]
        factor[p] = jnp.zeros((det, det), f32)
    some = pl.ds(0, 2 * count * det)

    def forward(q, carry):
        columns = pl.ds(pl.multiple_of(q * 2 * det, 2 * det), 2 * det)
        for p in range(count):
            patch_re, patch_im = patch[p, 0], patch[p, 1]
            for m in range(2):
                at = pl.ds((2 * p + m) * det, det)
                pr, pi = probe[q + m * groups, 0], probe[q + m * groups, 1]
                for c, value in enumerate((pr * patch_re - pi * patch_im, pr * patch_im + pi * patch_re)):
                    high, low = halves(value)
                    deep[at, pl.ds(c * det, det)] = high
                    deep[at, pl.ds((2 + c) * det, det)] = high
                    deep[at, pl.ds((4 + c) * det, det)] = low
        half[some, :] = jnp.dot(deep[some, :], right_f[...], preferred_element_type=f32)
        for p in range(count):
            first, second = [half[pl.ds((2 * p + m) * det, det), :] for m in range(2)]
            paired = jnp.concatenate(
                [
                    jnp.concatenate([first[:, :det], second[:, :det]], axis=1),
                    jnp.concatenate([first[:, det:], second[:, det:]], axis=1),
                ],
                axis=0,
            )
            high, low = halves(paired)
            stacked = jnp.concatenate([high, high, low], axis=0)
            out = jnp.dot(left_f[...], stacked, preferred_element_type=f32)
            far[p, :, columns] = out
            squares = out * out
            both = squares[:det] + squares[det:]
            factor[p] = factor[p] + (both[:, :det] + both[:, det:])
        return carry

    lax.fori_loop(0, groups, forward, 0)
    for p in range(count):
        factor[p] = jnp.sqrt(patterns[p]) / jnp.sqrt(jnp.maximum(factor[p], light_floor)) - 1.0
    measured = jnp.zeros((det, det), f32)
    for p in range(count):
        measured = measured + patterns[p]
    totals[0] = jnp.sum(measured.reshape(det // 8, 8, det), axis=0)
    totals[1] = jnp.sum(total.reshape(det // 8, 8, det), axis=0)
    spread_shape = slab_sizes + (rows, det)
    for h in range(2):
        r["packed_light"][h, :, :, :, 0] = light[...].reshape(spread_shape)

    home = tuple(mine)

    def flips_of(stage):
        flips = [()]
        for i in range(3):
            flips = [f + (d,) for f in flips for d in range(slab_sizes[i] if i in stage else 1)]
        return flips[1:]

    def spot_of(known, flips=(0, 0, 0)):
        return tuple(flipped(mine[i], slab_sizes[i], flips[i]) if i in known else slice(None) for i in range(3))

    def moves_of(flips):
        return list(zip(slab_dims, flips))

    two_steps, one_step = ((0, 1), (2,)), ((0, 1, 2),)

    class Sum:
        def __init__(self, stages, source, land0, acc, lands, landx):
            self.stages, self.source, self.acc = stages, source, acc
            self.land0, self.lands, self.landx = land0, lands, landx
            self.swap = remote(source.at[1 - core], land0, [(core_dim, 1)])
            self.batches = [Batch(land) for land in lands]

        def known(self, step):
            return [i for stage in self.stages[: step + 1] for i in stage]

        def send(self, step):
            for n, flips in enumerate(flips_of(self.stages[step])):
                source = self.acc.at[spot_of(self.known(step), flips)]
                self.batches[step].send(source, self.lands[step].at[n], moves_of(flips))

        def swapped(self):
            self.swap.wait()
            self.acc[...] = self.source[core] + self.land0[...]
            self.send(0)

        def reduced(self, step):
            self.batches[step].wait()
            land = self.lands[step]
            spot = spot_of(self.known(step))
            value = self.acc[spot]
            for d in range(land.shape[0]):
                value = value + land[d]
            self.acc[spot] = value
            if step < len(self.lands) - 1:
                self.send(step + 1)
                return
            for e, dim in enumerate(extra):
                item = remote(self.acc.at[home], self.landx.at[e], [(dim, 1)])
                item.start()
                item.wait()
                self.acc[home] = self.acc[home] + self.landx[e]

    light_sum = Sum(
        two_steps, r["packed_light"], r["land0_light"], r["acc_light"],
        [r["land1_light"], r["land2_light"]], r["landx_light"],
    )
    sums = []
    for q in range(groups):
        direct = q in direct_sums
        sums.append(
            Sum(
                one_step if direct else two_steps, packed.at[q], land0.at[q], acc.at[q],
                [land_all.at[q]] if direct else [land1.at[q], land2.at[q]], landx.at[q],
            )
        )
    total_swap = remote(totals, total_land, [(core_dim, 1)])

    def at_group(n):
        if n == 0:
            light_sum.swap.start()
            total_swap.start()
            return
        sums[n - 1].swap.start()
        if n == 2:
            light_sum.swapped()
        if n >= 3:
            sums[n - 3].swapped()

    def backward(q, carry):
        for n in range(groups):
            @pl.when(q == n)
            def _():
                at_group(n)

        columns = pl.ds(pl.multiple_of(q * 2 * det, 2 * det), 2 * det)
        for p in range(count):
            wide = jnp.concatenate([factor[p], factor[p]], axis=1)
            wide = jnp.concatenate([wide, wide], axis=0)
            high, low = halves(far[p, :, columns] * wide)
            stacked = jnp.concatenate([high, high, low], axis=0)
            out = jnp.dot(left_b[...], stacked, preferred_element_type=f32)
            high, low = halves(out)
            for m in range(2):
                at = pl.ds((2 * p + m) * det, det)
                for c in range(2):
                    part_h = high[c * det : (c + 1) * det, m * det : (m + 1) * det]
                    part_l = low[c * det : (c + 1) * det, m * det : (m + 1) * det]
                    deep[at, pl.ds(c * det, det)] = part_h
                    deep[at, pl.ds((2 + c) * det, det)] = part_h
                    deep[at, pl.ds((4 + c) * det, det)] = part_l
        half[some, :] = jnp.dot(deep[some, :], right_b[...], preferred_element_type=f32)
        for m in range(2):
            pr, pi = probe[q + m * groups, 0], probe[q + m * groups, 1]
            grad_re = jnp.zeros((det, det), f32)
            grad_im = jnp.zeros((det, det), f32)
            for p in range(count):
                at = pl.ds((2 * p + m) * det, det)
                cr, ci = half[at, :det], half[at, det:]
                patch_re, patch_im = patch[p, 0], patch[p, 1]
                grad_re = grad_re + patch_re * cr + patch_im * ci
                grad_im = grad_im + patch_re * ci - patch_im * cr
                num[p, 0] = num[p, 0] + (pr * cr + pi * ci)
                num[p, 1] = num[p, 1] + (pr * ci - pi * cr)
            packed[q, m, :, :, :, 0] = grad_re.reshape(spread_shape)
            packed[q, m, :, :, :, 1] = grad_im.reshape(spread_shape)
        return carry

    lax.fori_loop(0, groups, backward, 0)

    tile = mine[0]
    for i in range(1, 3):
        tile = tile * slab_sizes[i] + mine[i]
    strip = pl.ds(pl.multiple_of(tile * rows, rows), rows)
    own = Batch(full.at[(slice(None), core) + home])

    class Gather:
        def __init__(self, q):
            self.q = q
            self.view = full.at[q, core]
            if q in direct_gathers:
                self.stages = one_step
                self.batches = [Batch(land_all.at[0])]
            else:
                self.stages = two_steps[::-1]
                self.batches = [Batch(land2.at[0]), Batch(land1.at[0])]
            self.passing = Batch(land_all.at[0])

        def both(self, batch, spot, moves):
            batch.send(self.view.at[spot], self.view.at[spot], moves)

        def left(self, step):
            return [i for stage in self.stages[step:] for i in stage]

        def send(self, step):
            for flips in flips_of(self.stages[step]):
                self.both(self.batches[step], spot_of(self.left(step)), moves_of(flips))

        def begin(self):
            q = self.q
            for c in range(2):
                value = probe[core * groups + q, c, strip, :] + acc[(q,) + home + (c,)] * scale
                full[(q, core) + home + (c,)] = value
            self.both(own, home, [(core_dim, 1)])
            self.send(0)

        def got(self, step):
            self.batches[step].wait()
            if step < len(self.stages) - 1:
                self.send(step + 1)
            for flips in flips_of(self.stages[step]):
                self.both(self.passing, spot_of(self.left(step), flips), [(core_dim, 1)])

    gathers = [Gather(q) for q in range(groups)]

    at_group(groups)
    for p in range(count):
        shift = place(p)[3]
        for c in range(2):
            pads[p, c, pad_at, :] = pltpu.roll(num[p, c], shift, 1)
    build_frame(frame_num, 2)
    sums[groups - 2].swapped()
    sums[groups - 1].swapped()
    light_sum.reduced(0)
    num_fold = Fold(frame_num, num_slots, 0)
    for q in range(groups - 1):
        sums[q].reduced(0)
        num_fold.some(2)
    light_sum.reduced(1)
    scale = 1.0 / (r["acc_light"][home + (0,)] + probe_reg)
    for q in range(groups):
        if q not in direct_sums:
            sums[q].reduced(1)
            num_fold.some(2)
    sums[groups - 1].reduced(0)
    for q in range(groups):
        gathers[q].begin()
    num_fold.some(2)

    def slab_rows(spot):
        values = []
        for n in range(planes):
            c, k = n // modes, n % modes
            values.append(full[(k % groups, k // groups) + spot + (c,)])
        return jnp.concatenate(values, axis=0)

    tall = planes * rows
    up = lax.broadcasted_iota(jnp.int32, (tall, tall), 0)
    across = lax.broadcasted_iota(jnp.int32, (tall, tall), 1)
    same = jnp.where(((up - across) & (rows - 1)) == 0, 1.0, 0.0).astype(f32)
    plane = lax.broadcasted_iota(jnp.int32, (planes, tall), 0) * rows
    entry = lax.broadcasted_iota(jnp.int32, (planes, tall), 1)
    pick = jnp.where((entry >= plane) & (entry < plane + rows), 1.0, 0.0).astype(f32)
    plane = lax.broadcasted_iota(jnp.int32, (tall, det), 1) * rows
    entry = lax.broadcasted_iota(jnp.int32, (tall, det), 0)
    settled = jnp.where((entry >= plane) & (entry < plane + rows), 1.0, 0.0).astype(f32)

    own.wait()
    held = slab_rows(home)
    turned = jnp.concatenate([-held[tall // 2 :], held[: tall // 2]], axis=0)
    wide = jnp.concatenate([held, turned], axis=1)
    pairs = lax.dot_general(
        wide, wide, (((1,), (1,)), ((), ())), precision=highest, preferred_element_type=f32
    )
    gram = full_dot(full_dot(pick, pairs * same), settled)
    total_swap.wait()
    both = [jnp.sum(totals[i] + total_land[i]) for i in range(2)]
    sheet_lanes = lax.broadcasted_iota(jnp.int32, (8, det), 1)
    first = lax.broadcasted_iota(jnp.int32, (8, det), 0) == 0
    at_measured = first & (sheet_lanes == det - 2)
    at_modelled = first & (sheet_lanes == det - 1)
    sheet = jnp.where(at_measured, both[0], jnp.where(at_modelled, both[1], 0.0))
    for part in range(planes // 8):
        piece = gram[part * 8 : (part + 1) * 8]
        sheet = sheet + (pltpu.roll(piece, part * 32, 1) if part else piece)
    gram_out[...] = sheet
    spread = Batch(gram_land)
    for slot in range(1, slab_count):
        spread.send(gram_out, gram_land.at[slot - 1], list(zip(slab_dims, slab_coords(slot))))
    for q in range(groups):
        if q not in direct_gathers:
            gathers[q].got(0)
            num_fold.some(2)
    num_fold.some(100)
    spread.wait()
    sheet = gram_out[...]
    for i in range(slab_count - 1):
        sheet = sheet + gram_land[i]
    for e, dim in enumerate(extra):
        gram_x[2 * e] = sheet
        item = remote(gram_x.at[2 * e], gram_x.at[2 * e + 1], [(dim, 1)])
        item.start()
        item.wait()
        sheet = sheet + gram_x[2 * e + 1]
    measured = jnp.sum(jnp.where(at_measured, sheet, 0.0))
    modelled = jnp.sum(jnp.where(at_modelled, sheet, 0.0))
    ratio = measured / (modelled + total_eps)
    parts = [sheet[:, part * 32 : part * 32 + planes] for part in range(planes // 8)]
    embedded = jnp.concatenate(parts, axis=0)
    eye = jnp.where(
        lax.broadcasted_iota(jnp.int32, (planes, planes), 0) == lax.broadcasted_iota(jnp.int32, (planes, planes), 1),
        1.0, 0.0,
    ).astype(f32)
    frobenius = jnp.sqrt(jnp.sum(embedded * embedded, keepdims=True))
    current = embedded / frobenius
    inverse = eye
    for repeat in range(NS_STEPS):
        scaled = 1.5 * eye - 0.5 * full_dot(inverse, current)
        current = full_dot(current, scaled)
        inverse = full_dot(scaled, inverse)
    weight = jnp.sqrt(ratio * jnp.sum(embedded * eye, axis=1, keepdims=True))
    mix = weight * (inverse / jnp.sqrt(frobenius))
    mix = lax.dot_general(
        pick, full_dot(mix, pick), (((0,), (0,)), ((), ())), precision=highest, preferred_element_type=f32
    )
    high, low = halves(mix * same)
    mixer = jnp.concatenate([high, low, high], axis=1)
    for q in range(groups):
        gathers[q].got(0 if q in direct_gathers else 1)

    interior[0:2] = frame_num[:, det : det + block_rows, det : det + block_cols]
    interior[2] = frame_light[0, det : det + block_rows, det : det + block_cols]
    light_fold.end()
    num_fold.end()
    new_specimen[...] = specimen[...] + interior[0:2] / (interior[2] + object_reg)[None]

    for item in gathers:
        item.passing.wait()
    for t in range(0, slab_count, 2):
        sides = [slab_rows(slab_coords(s)) for s in (t, t + 1)]
        high, low = halves(jnp.concatenate(sides, axis=1))
        out = jnp.dot(mixer, jnp.concatenate([high, high, low], axis=0), preferred_element_type=f32)
        for n in range(planes):
            for s in range(2):
                new_probe[n % modes, n // modes, (t + s) * rows : (t + s + 1) * rows, :] = out[
                    n * rows : (n + 1) * rows, s * det : (s + 1) * det
                ]


def emit_kernel(*refs):
    sources, targets, held = refs[:2], refs[2:4], refs[4:6]
    come, gone = refs[6:]
    steps = []
    for source, target, buffer in zip(sources, targets, held):
        rows = max(source.shape[0] // 6, 1)
        for low in range(0, source.shape[0], rows):
            at = pl.ds(low, rows)
            n = len(steps)
            steps.append(
                (
                    pltpu.make_async_copy(source.at[at], buffer.at[at], come.at[n]),
                    pltpu.make_async_copy(buffer.at[at], target.at[at], gone.at[n]),
                )
            )
    for arrive, _ in steps:
        arrive.start()
    for arrive, leave in steps:
        arrive.wait()
        leave.start()
    for _, leave in steps:
        leave.wait()


def emit(probe, specimen):
    anywhere = pl.BlockSpec(memory_space=pl.ANY)
    return pl.pallas_call(
        emit_kernel,
        name="emit",
        out_shape=tuple(jax.ShapeDtypeStruct(x.shape, x.dtype) for x in (probe, specimen)),
        in_specs=[anywhere] * 2,
        out_specs=(anywhere,) * 2,
        scratch_shapes=[
            pltpu.VMEM(probe.shape, probe.dtype),
            pltpu.VMEM(specimen.shape, specimen.dtype),
            pltpu.SemaphoreType.DMA((8,)),
            pltpu.SemaphoreType.DMA((8,)),
        ],
        compiler_params=pltpu.CompilerParams(vmem_limit_bytes=56 * 1024 * 1024),
    )(probe, specimen)


def body(probe_modes, patterns, specimen, offsets):
    f32 = jnp.float32
    modes, _, det, _ = probe_modes.shape
    count = patterns.shape[0]
    block_rows, block_cols = specimen.shape[1:]
    col_blocks = block_cols // det + 2
    ext_rows = block_rows + 2 * det
    ext_cols = block_cols + 2 * det
    extra = extra_bits()
    more = max(len(extra), 1)
    rows = det // slab_count
    groups = modes // 2
    bf16 = jnp.bfloat16
    tables = [jnp.asarray(t) for t in dft_tables(det)]
    sems = 70 + (groups + 2) * len(extra)
    scratch = {
        "probe": pltpu.VMEM(probe_modes.shape, f32),
        "patterns": pltpu.VMEM(patterns.shape, f32),
        "specimen": pltpu.VMEM(specimen.shape, f32),
        **{f"table{n}": pltpu.VMEM(t.shape, bf16) for n, t in enumerate(tables)},
        "ext": pltpu.VMEM((2, col_blocks + 1, ext_rows, det), f32),
        "pads": pltpu.VMEM((count, 2, 2 * (ext_rows - det) + det, det), f32),
        "frame_num": pltpu.VMEM((2, ext_rows, ext_cols), f32),
        "frame_light": pltpu.VMEM((1, ext_rows, ext_cols), f32),
        "deep": pltpu.VMEM((2 * count * det, 6 * det), bf16),
        "half": pltpu.VMEM((2 * count * det, 2 * det), f32),
        "far": pltpu.VMEM((count, 2 * det, modes * det), f32),
        "patch": pltpu.VMEM((count, 2, det, det), f32),
        "factor": pltpu.VMEM((count, det, det), f32),
        "num": pltpu.VMEM((count, 2, det, det), f32),
        "power": pltpu.VMEM((det, det), f32),
        "light": pltpu.VMEM((det, det), f32),
        "totals": pltpu.VMEM((2, 8, det), f32),
        "total_land": pltpu.VMEM((2, 8, det), f32),
        "gram_out": pltpu.VMEM((8, det), f32),
        "gram_land": pltpu.VMEM((slab_count - 1, 8, det), f32),
        "gram_x": pltpu.VMEM((2 * more, 8, det), f32),
        "interior": pltpu.VMEM((3, block_rows, block_cols), f32),
        "send_sem": pltpu.SemaphoreType.DMA((sems,)),
        "recv_sem": pltpu.SemaphoreType.DMA((sems,)),
        "local_sem": pltpu.SemaphoreType.DMA((9,)),
    }
    for end, lead, planes in (("", (groups,), 2), ("_light", (), 1)):
        tile = (planes, rows, det)
        scratch["packed" + end] = pltpu.VMEM(lead + (2,) + slab_sizes + tile, f32)
        scratch["land0" + end] = pltpu.VMEM(lead + slab_sizes + tile, f32)
        scratch["acc" + end] = pltpu.VMEM(lead + slab_sizes + tile, f32)
        scratch["land1" + end] = pltpu.VMEM(lead + (slab_sizes[0] * slab_sizes[1] - 1, slab_sizes[2]) + tile, f32)
        scratch["land2" + end] = pltpu.VMEM(lead + (slab_sizes[2] - 1,) + tile, f32)
        scratch["landx" + end] = pltpu.VMEM(lead + (more,) + tile, f32)
    scratch["land_all"] = pltpu.VMEM((groups, slab_count - 1, 2, rows, det), f32)
    scratch["full"] = pltpu.VMEM((groups, 2) + slab_sizes + (2, rows, det), f32)
    for index, (i, j) in enumerate(directions()):
        shape = (det if i else block_rows, det if j else block_cols)
        scratch[f"num_slot{index}"] = pltpu.VMEM((2,) + shape, f32)
        scratch[f"light_slot{index}"] = pltpu.VMEM((1,) + shape, f32)
    names = ["offs", "probe_in", "patterns_in", "specimen_in"]
    names += [f"table_in{n}" for n in range(4)] + ["new_probe", "new_specimen"] + list(scratch)

    def kernel(*refs):
        update_kernel(extra, names, *refs)

    vmem = pl.BlockSpec(memory_space=pltpu.VMEM)
    results = pl.pallas_call(
        kernel,
        name="update",
        out_shape=(
            jax.ShapeDtypeStruct(probe_modes.shape, f32),
            jax.ShapeDtypeStruct(specimen.shape, f32),
        ),
        in_specs=[pl.BlockSpec(memory_space=pltpu.SMEM)] + [pl.BlockSpec(memory_space=pl.ANY)] * 7,
        out_specs=(vmem, vmem),
        scratch_shapes=list(scratch.values()),
        compiler_params=pltpu.CompilerParams(has_side_effects=True, vmem_limit_bytes=56 * 1024 * 1024),
    )(offsets.T, probe_modes, patterns, specimen, *tables)
    return emit(*results)


def solution(mesh):
    return jax.shard_map(
        body,
        mesh=mesh,
        in_specs=(
            P(),
            P(("scan", "tile"), None, None),
            P(None, "scan", "tile"),
            P(("scan", "tile"), None),
        ),
        out_specs=(P(), P(None, "scan", "tile")),
        check_vma=False,
    )
```
